8 devices in a mesh: dp: 2 (over z, y), tp: 4 (over x, core).
Axes of the slice: x: 2, y: 2, z: 1, core: 2. Of those that a mesh axis runs over, the one named last changes fastest.
Arguments:
- x: bfloat16 [512, 2048], P(('dp', 'tp')), parts along dimension 0
- grad_y: bfloat16 [512, 2048], P(('dp', 'tp')), parts along dimension 0
- gain_attn: float32 [3, 2048], replicated
- gain_mlp: float32 [3, 2048], replicated
- w_qkv: bfloat16 [3, 2048, 6144], P(None, None, 'tp')
- w_out: bfloat16 [3, 2048, 2048], P(None, 'tp')
- w_gate: bfloat16 [3, 2048, 8192], P(None, None, 'tp')
- w_up: bfloat16 [3, 2048, 8192], P(None, None, 'tp')
- w_down: bfloat16 [3, 8192, 2048], P(None, 'tp')
Outputs:
- output 1: bfloat16 [512, 2048], P(('dp', 'tp')), parts along dimension 0
- output 2: bfloat16 [512, 2048], P(('dp', 'tp')), parts along dimension 0
- output 3: bfloat16 [6, 2048, 6144], P('dp', None, 'tp'), parts along dimension 0
- output 4: bfloat16 [6, 2048, 2048], P('dp', 'tp'), parts along dimension 0
- output 5: bfloat16 [6, 2048, 8192], P('dp', None, 'tp'), parts along dimension 0
- output 6: bfloat16 [6, 2048, 8192], P('dp', None, 'tp'), parts along dimension 0
- output 7: bfloat16 [6, 8192, 2048], P('dp', 'tp'), parts along dimension 0
- output 8: float32 [6, 2048], P('dp'), parts along dimension 0
- output 9: float32 [6, 2048], P('dp'), parts along dimension 0
There are 2 independent parts. The reference program is written for one: setup_inputs(seed, part) draws one part's arguments, and reference() takes and returns one part's arrays. A program takes and returns all parts, laid end to end along the dimension named above; an argument that names none is the same for every part.
All inputs are finite; a program needn't handle non-finite values.
Results may differ from the reference program's by a relative error of at most 0.02.
Values are sent between devices in bfloat16 or wider.
A program may use at most 1 GiB of HBM per device.

```python
import jax
import jax.numpy as jnp
from jax import lax

D = 2048
FF = 8192
HEADS = 16
KV_HEADS = 16
HEAD = 128
LAYERS = 3
SEQ_LEN = 256
NORM_EPS = 1e-5
GROUP_SIZE = HEADS // KV_HEADS
QKV_COLS = (HEADS + 2 * KV_HEADS) * HEAD


def setup_inputs(seed: int = 0, part: int = 0) -> dict:
    part_key = jax.random.fold_in(jax.random.key(seed), part)
    act_keys = jax.random.split(part_key, 4)
    weight_keys = jax.random.split(jax.random.key(seed + 1), 7)
    x_mean = jax.random.normal(act_keys[0], (1, D), jnp.float32)
    x = jax.random.normal(act_keys[1], (SEQ_LEN, D), jnp.float32) + x_mean
    grad_mean = jax.random.normal(act_keys[2], (1, D), jnp.float32)
    grad_y = jax.random.normal(act_keys[3], (SEQ_LEN, D), jnp.float32) + grad_mean
    gain_attn = 1.0 + 0.3 * jax.random.normal(weight_keys[0], (LAYERS, D), jnp.float32)
    gain_mlp = 1.0 + 0.3 * jax.random.normal(weight_keys[1], (LAYERS, D), jnp.float32)
    w_qkv = jax.random.normal(weight_keys[2], (LAYERS, D, QKV_COLS), jnp.float32) * D ** -0.5
    w_out = jax.random.normal(weight_keys[3], (LAYERS, HEADS * HEAD, D), jnp.float32) * (HEADS * HEAD) ** -0.5
    w_gate = jax.random.normal(weight_keys[4], (LAYERS, D, FF), jnp.float32) * D ** -0.5
    w_up = jax.random.normal(weight_keys[5], (LAYERS, D, FF), jnp.float32) * D ** -0.5
    w_down = jax.random.normal(weight_keys[6], (LAYERS, FF, D), jnp.float32) * FF ** -0.5
    return {'x': x.astype(jnp.bfloat16), 'grad_y': grad_y.astype(jnp.bfloat16), 'gain_attn': gain_attn, 'gain_mlp': gain_mlp, 'w_qkv': w_qkv.astype(jnp.bfloat16), 'w_out': w_out.astype(jnp.bfloat16), 'w_gate': w_gate.astype(jnp.bfloat16), 'w_up': w_up.astype(jnp.bfloat16), 'w_down': w_down.astype(jnp.bfloat16)}


def rms_norm(hidden_in, gain_vec):
    hidden_f = hidden_in.astype(jnp.float32)
    inv_rms = lax.rsqrt(jnp.mean(hidden_f * hidden_f, axis=-1, keepdims=True) + NORM_EPS)
    return (hidden_f * inv_rms * gain_vec).astype(jnp.bfloat16)


def attention(qkv_out):
    positions = jnp.arange(SEQ_LEN)
    causal = positions[:, None] >= positions[None, :]

    def one_group(group_block):
        queries = group_block[:, :GROUP_SIZE].astype(jnp.float32)
        key_rows = group_block[:, GROUP_SIZE].astype(jnp.float32)
        value_rows = group_block[:, GROUP_SIZE + 1].astype(jnp.float32)
        scores = jnp.einsum('iqh,jh->qij', queries, key_rows) * HEAD ** -0.5
        prob_low = jax.nn.softmax(jnp.where(causal, scores, -1e30), axis=-1).astype(jnp.bfloat16)
        heads_out = jnp.einsum('qij,jh->iqh', prob_low.astype(jnp.float32), value_rows)
        return heads_out.astype(jnp.bfloat16)

    blocks = jnp.moveaxis(qkv_out.reshape(SEQ_LEN, KV_HEADS, GROUP_SIZE + 2, HEAD), 1, 0)
    heads_out = lax.map(jax.checkpoint(one_group), blocks)
    return jnp.moveaxis(heads_out, 0, 1).reshape(SEQ_LEN, HEADS * HEAD)


def decoder_layer(hidden_in, params):
    gain_attn, gain_mlp, w_qkv, w_out, w_gate, w_up, w_down = params
    normed = rms_norm(hidden_in, gain_attn)
    qkv_out = jnp.dot(normed, w_qkv, preferred_element_type=jnp.float32).astype(jnp.bfloat16)
    heads_out = attention(qkv_out)
    hidden_mid = hidden_in + jnp.dot(heads_out, w_out, preferred_element_type=jnp.float32).astype(jnp.bfloat16)
    normed_mid = rms_norm(hidden_mid, gain_mlp)
    gate_act = jnp.dot(normed_mid, w_gate, preferred_element_type=jnp.float32).astype(jnp.bfloat16)
    up_act = jnp.dot(normed_mid, w_up, preferred_element_type=jnp.float32).astype(jnp.bfloat16)
    gated_act = (jax.nn.silu(gate_act.astype(jnp.float32)) * up_act.astype(jnp.float32)).astype(jnp.bfloat16)
    return hidden_mid + jnp.dot(gated_act, w_down, preferred_element_type=jnp.float32).astype(jnp.bfloat16)


def stack_forward(x, params):
    def scan_body(hidden_carry, layer_params):
        return decoder_layer(hidden_carry, layer_params), None
    hidden_out, _ = lax.scan(scan_body, x, params)
    return hidden_out


def reference(x, grad_y, gain_attn, gain_mlp, w_qkv, w_out, w_gate, w_up, w_down):
    params = (gain_attn, gain_mlp, w_qkv, w_out, w_gate, w_up, w_down)
    y, pullback = jax.vjp(stack_forward, x, params)
    grad_x, grad_params = pullback(grad_y)
    return (y, grad_x, grad_params[2], grad_params[3], grad_params[4], grad_params[5], grad_params[6], grad_params[0], grad_params[1])
```

```python
import functools

import jax
import jax.numpy as jnp
from jax import lax
from jax.experimental import pallas as pl
from jax.experimental.pallas import tpu as pltpu
from jax.sharding import PartitionSpec as P

HEAD = 128
EPS = 1e-5
MESH = pl.DeviceIdType.MESH
F32 = jnp.float32
BF16 = jnp.bfloat16
VMEM_LIMIT = 66_000_000

D = 2048
S = 256
R = 64
NQ = 1536
NO = 512
NF = 2048
HEADS = 4
LAYERS = 3

AC = 4
AW = D // AC
RC = 4
RW = D // RC


def dot(a, b):
    return jnp.dot(a, b, preferred_element_type=F32)


def dot_nt(a, b):
    return lax.dot_general(a, b, (((1,), (1,)), ((), ())), preferred_element_type=F32)


def dot_tn(a, b):
    return lax.dot_general(a, b, (((0,), (0,)), ((), ())), preferred_element_type=F32)


def ds(i, n):
    return pl.ds(i * n if isinstance(i, int) else pl.multiple_of(i * n, n), n)


def loop(n, body):
    lax.fori_loop(0, n, lambda i, c: (body(i), c)[1], 0)


class Peers:
    def __init__(self):
        self.me = lax.axis_index("tp")
        core, chip = lax.rem(self.me, 2), self.me // 2
        self.sib = chip * 2 + (1 - core)
        self.cross = (1 - chip) * 2 + core
        self.diag = (1 - chip) * 2 + (1 - core)

    def barrier(self):
        sem = pltpu.get_barrier_semaphore()
        for peer in (self.sib, self.cross):
            pl.semaphore_signal(sem, inc=1, device_id={"tp": peer}, device_id_type=MESH)
        pl.semaphore_wait(sem, 2)


def remote(src, dst, send, recv, peer):
    return pltpu.make_async_remote_copy(
        src_ref=src, dst_ref=dst, send_sem=send, recv_sem=recv, device_id={"tp": peer}, device_id_type=MESH
    )


class Gather:
    def __init__(self, p, buf, send, recv, which):
        self.p, self.buf, self.send, self.recv, self.which = p, buf, send, recv, which

    def _copy(self, kind, chunk, owner, peer):
        part = self.buf.at[ds(owner, R), ds(chunk, AW)]
        return remote(part, part, self.send.at[self.which, kind, chunk], self.recv.at[self.which, kind, chunk], peer)

    def to_cross(self, chunk):
        self._copy(0, chunk, self.p.me, self.p.cross).start()

    def to_sib(self, chunk):
        self._copy(1, chunk, self.p.me, self.p.sib).start()

    def relay(self, chunk):
        self._copy(0, chunk, self.p.cross, self.p.cross).wait_recv()
        self._copy(2, chunk, self.p.cross, self.p.sib).start()

    def arrived(self, chunk):
        self._copy(1, chunk, self.p.sib, self.p.sib).wait_recv()
        self._copy(2, chunk, self.p.diag, self.p.sib).wait_recv()

    def start(self):
        for chunk in range(AC):
            self.to_cross(chunk)
        for chunk in range(AC):
            self.to_sib(chunk)

    def each(self, body):
        for chunk in range(AC + 1):
            if chunk < AC:
                self.relay(chunk)
            if chunk > 0:
                self.arrived(chunk - 1)
                body(chunk - 1)

    def finish(self):
        for chunk in range(AC):
            self._copy(0, chunk, self.p.me, self.p.cross).wait_send()
            self._copy(1, chunk, self.p.me, self.p.sib).wait_send()
            self._copy(2, chunk, self.p.cross, self.p.sib).wait_send()


class Scatter:
    def __init__(self, p, part, near, out, far, send, recv):
        self.p, self.part, self.near, self.out, self.far, self.send, self.recv = p, part, near, out, far, send, recv

    def _near(self, kind, chunk):
        owner = self.p.diag if kind == 0 else self.p.sib
        return remote(
            self.part.at[ds(owner, R), ds(chunk, RW)],
            self.near.at[kind, :, ds(chunk, RW)],
            self.send.at[kind, chunk],
            self.recv.at[kind, chunk],
            self.p.sib,
        )

    def _far(self, chunk):
        return remote(
            self.out.at[:, ds(chunk, RW)],
            self.far.at[:, ds(chunk, RW)],
            self.send.at[2, chunk],
            self.recv.at[2, chunk],
            self.p.cross,
        )

    def _mid(self, chunk):
        self._near(0, chunk).wait_recv()
        cols = ds(chunk, RW)
        self.out[:, cols] = (self.part[ds(self.p.cross, R), cols] + self.near[0, :, cols]).astype(BF16)
        self._far(chunk).start()

    def run(self, compute):
        def step(chunk):
            self.part[:, ds(chunk, RW)] = compute(chunk)
            self._near(0, chunk).start()
            self._near(1, chunk).start()

            @pl.when(chunk > 0)
            def _():
                self._mid(chunk - 1)

        loop(RC, step)
        self._mid(RC - 1)

    def result(self):
        for chunk in range(RC):
            self._near(1, chunk).wait_recv()
            self._far(chunk).wait_recv()
        total = self.part[ds(self.p.me, R), :] + self.near[1] + self.far[...].astype(F32)
        for chunk in range(RC):
            self._near(0, chunk).wait_send()
            self._near(1, chunk).wait_send()
            self._far(chunk).wait_send()
        return total.astype(BF16)


def norm(h, gain):
    hf = h.astype(F32)
    inv = lax.rsqrt(jnp.mean(hf * hf, axis=-1, keepdims=True) + EPS)
    return (hf * inv * gain).astype(BF16)


def norm_back(h, gain, dy):
    hf, dyf = h.astype(F32), dy.astype(F32)
    inv = lax.rsqrt(jnp.mean(hf * hf, axis=-1, keepdims=True) + EPS)
    dgain = jnp.sum(dyf * (hf * inv), axis=0, keepdims=True)
    dn = dyf * gain
    slope = jnp.sum(dn * hf, axis=-1, keepdims=True) * (inv * inv * inv) / D
    return (dn * inv - hf * slope).astype(BF16), dgain


def softmax_scores(q, k):
    scores = dot_nt(q, k) * HEAD**-0.5
    rows = lax.broadcasted_iota(jnp.int32, (S, S), 0)
    cols = lax.broadcasted_iota(jnp.int32, (S, S), 1)
    scores = jnp.where(rows >= cols, scores, -1e30)
    e = jnp.exp(scores - jnp.max(scores, axis=-1, keepdims=True))
    return e / jnp.sum(e, axis=-1, keepdims=True)


def head_cols(head, which):
    return pl.ds(pl.multiple_of(head * 3 * HEAD + which * HEAD, HEAD), HEAD)


def attention(qkv, o, probs=None):
    def one(head):
        prob = softmax_scores(qkv[:, head_cols(head, 0)], qkv[:, head_cols(head, 1)])
        if probs is not None:
            probs[head] = prob
        o[:, ds(head, HEAD)] = dot(prob.astype(BF16), qkv[:, head_cols(head, 2)]).astype(BF16)

    loop(HEADS, one)


def qkv_chunk(u, wq, acc, qkv, tile=768):
    def body(chunk):
        def one(j):
            cols = ds(j, tile)
            part = dot(u[:, ds(chunk, AW)], wq[ds(chunk, AW), cols])
            if chunk > 0:
                part = part + acc[:, cols]
            if chunk < AC - 1:
                acc[:, cols] = part
            else:
                qkv[:, cols] = part.astype(BF16)

        loop(NQ // tile, one)

    return body


def mlp_chunk(n, wg, wu, acc1, acc3, last, tile=512):
    def body(chunk):
        def one(j):
            cols = ds(j, tile)
            z1 = dot(n[:, ds(chunk, AW)], wg[ds(chunk, AW), cols])
            z3 = dot(n[:, ds(chunk, AW)], wu[ds(chunk, AW), cols])
            if chunk > 0:
                z1, z3 = z1 + acc1[:, cols], z3 + acc3[:, cols]
            if chunk < AC - 1:
                acc1[:, cols] = z1
                acc3[:, cols] = z3
            else:
                last(cols, z1.astype(BF16).astype(F32), z3.astype(BF16).astype(F32))

        loop(NF // tile, one)

    return body


def forward_kernel(x, ga, gm, wq_h, wo_h, wg_h, wu_h, wd_h, hs,
                   wq, wo, wg, wu, wd, h, u, n, acc1, acc3, qkv, o, m, part, near, out, far,
                   wsem, gsend, grecv, ssend, srecv):
    p = Peers()
    pairs = ((wq_h, wq), (wo_h, wo), (wg_h, wg), (wu_h, wu), (wd_h, wd))

    def load(i, layer):
        return pltpu.make_async_copy(pairs[i][0].at[layer], pairs[i][1], wsem.at[i])

    for i in range(5):
        load(i, 0).start()
    h[...] = x[...]
    p.barrier()
    mine = ds(p.me, R)

    def layer_step(layer):
        def refill(i):
            @pl.when(layer < LAYERS - 1)
            def _():
                load(i, layer + 1).start()

        u[mine, :] = norm(h[...], ga[pl.ds(layer, 1), :])
        gather = Gather(p, u, gsend, grecv, 0)
        gather.start()
        load(0, layer).wait()
        gather.each(qkv_chunk(u, wq, acc1, qkv))
        gather.finish()
        refill(0)
        attention(qkv, o)
        load(1, layer).wait()
        scatter = Scatter(p, part, near, out, far, ssend, srecv)
        scatter.run(lambda c: dot(o[...], wo[:, ds(c, RW)]))
        refill(1)
        h[...] = h[...] + scatter.result()

        n[mine, :] = norm(h[...], gm[pl.ds(layer, 1), :])
        gather = Gather(p, n, gsend, grecv, 0)
        gather.start()
        load(2, layer).wait()
        load(3, layer).wait()

        def last(cols, z1, z3):
            m[:, cols] = (z1 * jax.nn.sigmoid(z1) * z3).astype(BF16)

        gather.each(mlp_chunk(n, wg, wu, acc1, acc3, last))
        gather.finish()
        refill(2)
        refill(3)
        load(4, layer).wait()
        scatter.run(lambda c: dot(m[...], wd[:, ds(c, RW)]))
        refill(4)
        h[...] = h[...] + scatter.result()
        hs[layer] = h[...]

    loop(LAYERS, layer_step)


def backward_kernel(layer, hin, dy, gin, ga, gm, wq_h, wo_h, wg_h, wu_h, wd_h, *refs):
    last_call = layer == 0
    refs = list(refs)
    take = lambda k: [refs.pop(0) for _ in range(k)]
    (dx,) = take(1)
    gouts = take(2 if last_call else 1)
    saved_h = take(9)
    u, dqkv, o, da, n, dg, du, m, dd = saved = take(9)
    wq, wo, wg, wu, wd = take(5)
    hm, acc1, acc3, qkv, probs, dgated, dh, part, near, out, far, gbuf = take(12)
    gmid, gfar = take(2)
    wsem, osem, gsend, grecv, ssend, srecv, rsend, rrecv = take(8)

    p = Peers()
    pairs = ((wq_h, wq), (wo_h, wo), (wg_h, wg), (wu_h, wu), (wd_h, wd))
    loads = [pltpu.make_async_copy(src.at[layer], dst, wsem.at[i]) for i, (src, dst) in enumerate(pairs)]
    saves = [pltpu.make_async_copy(src, dst, osem.at[i]) for i, (src, dst) in enumerate(zip(saved, saved_h))]
    for i in (0, 1, 4, 2, 3):
        loads[i].start()
    mine = ds(p.me, R)
    h = hin[layer - 1] if layer > 0 else hin[...]
    gain_a, gain_m = ga[pl.ds(layer, 1), :], gm[pl.ds(layer, 1), :]
    u[mine, :] = norm(h, gain_a)
    dd[mine, :] = dy[...]
    p.barrier()
    gu = Gather(p, u, gsend, grecv, 0)
    gd = Gather(p, dd, gsend, grecv, 1)
    gu.start()
    for c in range(AC):
        gd.to_sib(c)
    for c in range(AC // 2):
        gd.to_cross(c)

    loads[0].wait()
    gu.each(qkv_chunk(u, wq, acc1, qkv))
    saves[0].start()
    attention(qkv, o, probs)
    saves[2].start()
    loads[1].wait()
    scatter = Scatter(p, part, near, out, far, ssend, srecv)
    scatter.run(lambda c: dot(o[...], wo[:, ds(c, RW)]))
    for c in range(AC // 2, AC):
        gd.to_cross(c)
    for c in range(AC // 2):
        gd.relay(c)
    h_mid = h + scatter.result()
    hm[...] = h_mid
    n[mine, :] = norm(h_mid, gain_m)
    gn = Gather(p, n, gsend, grecv, 2)
    gn.start()

    for c in range(AC // 2, AC):
        gd.relay(c)
    for c in range(AC):
        gd.arrived(c)
    saves[8].start()
    loads[4].wait()

    def gated(j):
        dgated[:, ds(j, 512)] = dot_nt(dd[...], wd[ds(j, 512), :]).astype(BF16)

    loop(NF // 512, gated)
    loads[2].wait()
    loads[3].wait()

    def last(cols, z1, z3):
        sig = jax.nn.sigmoid(z1)
        silu = z1 * sig
        dm = dgated[:, cols].astype(F32)
        m[:, cols] = (silu * z3).astype(BF16)
        du[:, cols] = (dm * silu).astype(BF16)
        dg[:, cols] = (dm * z3 * (sig + silu * (1.0 - sig))).astype(BF16)

    gn.each(mlp_chunk(n, wg, wu, acc1, acc3, last))
    for i in (4, 5, 6, 7):
        saves[i].start()

    scatter.run(lambda c: dot_nt(dg[...], wg[ds(c, RW), :]) + dot_nt(du[...], wu[ds(c, RW), :]))
    d_norm, dgain_m = norm_back(hm[...], gain_m, scatter.result())
    d_mid = dy[...] + d_norm
    da[mine, :] = d_mid
    ga_ = Gather(p, da, gsend, grecv, 3)
    ga_.start()
    gbuf[...] = gin[...]
    gbuf[pl.ds(LAYERS + layer, 1), :] = dgain_m

    def heads_chunk(chunk):
        part_h = dot_nt(da[:, ds(chunk, AW)], wo[:, ds(chunk, AW)])
        if chunk > 0:
            part_h = part_h + acc1[:, :NO]
        if chunk < AC - 1:
            acc1[:, :NO] = part_h
        else:
            dh[...] = part_h.astype(BF16)

    ga_.each(heads_chunk)
    saves[3].start()

    def back(head):
        prob = probs[head]
        d_o = dh[:, ds(head, HEAD)]
        q, k, v = (qkv[:, head_cols(head, i)] for i in range(3))
        d_prob = dot_nt(d_o, v)
        d_scores = (prob * (d_prob - jnp.sum(d_prob * prob, axis=-1, keepdims=True)) * HEAD**-0.5).astype(BF16)
        dqkv[:, head_cols(head, 0)] = dot(d_scores, k).astype(BF16)
        dqkv[:, head_cols(head, 1)] = dot_tn(d_scores, q).astype(BF16)
        dqkv[:, head_cols(head, 2)] = dot_tn(prob.astype(BF16), d_o).astype(BF16)

    loop(HEADS, back)
    saves[1].start()
    scatter.run(lambda c: dot_nt(dqkv[...], wq[ds(c, RW), :]))
    d_norm, dgain_a = norm_back(h, gain_a, scatter.result())
    dx[...] = da[mine, :] + d_norm
    gbuf[pl.ds(layer, 1), :] = dgain_a

    if last_call:
        near_g = remote(gbuf, gmid, rsend.at[0], rrecv.at[0], p.sib)
        near_g.start()
        near_g.wait()
        gbuf[...] = gbuf[...] + gmid[...]
        far_g = remote(gbuf, gfar, rsend.at[1], rrecv.at[1], p.cross)
        far_g.start()
        far_g.wait()
        total = gbuf[...] + gfar[...]
        gouts[0][...] = total[:LAYERS]
        gouts[1][...] = total[LAYERS:2 * LAYERS]
    else:
        gouts[0][...] = gbuf[...]
    for g in (gu, gd, gn, ga_):
        g.finish()
    for save in saves:
        save.wait()


def wgrad_kernel(layer, n_alias, u_h, dqkv_h, o_h, da_h, n_h, dg_h, du_h, m_h, dd_h, *refs):
    refs = list(refs[n_alias:])
    take = lambda k: [refs.pop(0) for _ in range(k)]
    outs = take(5)
    u, dqkv, o, da, n, dg, du, m, dd = acts = take(9)
    stages = take(5)
    isem, osem = take(2)
    loads = [pltpu.make_async_copy(src, dst, isem.at[i])
             for i, (src, dst) in enumerate(zip((u_h, dqkv_h, o_h, da_h, n_h, dg_h, du_h, m_h, dd_h), acts))]
    order = (0, 1, 4, 5, 6, 7, 8, 2, 3)
    for i in order:
        loads[i].start()
    work = ((0, 0, 1), (2, 4, 5), (3, 4, 6), (4, 7, 8), (1, 2, 3))
    waited = set()
    for out_i, a_i, b_i in work:
        for i in (a_i, b_i):
            if i not in waited:
                loads[i].wait()
                waited.add(i)
        a, b, out, stage = acts[a_i], acts[b_i], outs[out_i], stages[out_i]
        tiles, cols = a.shape[1] // S, b.shape[1]

        def copy(i, slot):
            return pltpu.make_async_copy(stage.at[slot], out.at[layer, ds(i, S), :], osem.at[out_i, slot])

        def step(i):
            slot = lax.rem(i, 2)

            @pl.when(i >= 2)
            def _():
                copy(i - 2, slot).wait()

            lhs = a[:, ds(i, S)].T
            for c in range(cols // 512):
                stage[slot, :, ds(c, 512)] = dot(lhs, b[:, ds(c, 512)]).astype(BF16)
            copy(i, slot).start()

        loop(tiles, step)
    for out_i, a_i, b_i in work:
        out, stage = outs[out_i], stages[out_i]
        tiles = acts[a_i].shape[1] // S
        for i in (tiles - 2, tiles - 1):
            pltpu.make_async_copy(stage.at[i % 2], out.at[layer, ds(i, S), :], osem.at[out_i, i % 2]).wait()


def vmem():
    return pl.BlockSpec(memory_space=pltpu.VMEM)


def hbm():
    return pl.BlockSpec(memory_space=pl.ANY)


WEIGHT_SCRATCH = [
    pltpu.VMEM((D, NQ), BF16),
    pltpu.VMEM((NO, D), BF16),
    pltpu.VMEM((D, NF), BF16),
    pltpu.VMEM((D, NF), BF16),
    pltpu.VMEM((NF, D), BF16),
]
SCATTER_SCRATCH = [
    pltpu.VMEM((S, D), F32),
    pltpu.VMEM((2, R, D), F32),
    pltpu.VMEM((R, D), BF16),
    pltpu.VMEM((R, D), BF16),
]
SAVED = [(S, D), (S, NQ), (S, NO), (S, D), (S, D), (S, NF), (S, NF), (S, NF), (S, D)]
GRADS = [(D, NQ), (NO, D), (D, NF), (D, NF), (NF, D)]


def run_forward(x, ga, gm, weights):
    dma = pltpu.SemaphoreType.DMA
    return pl.pallas_call(
        forward_kernel,
        name="forward",
        out_shape=jax.ShapeDtypeStruct((LAYERS, R, D), BF16),
        in_specs=[vmem()] * 3 + [hbm()] * 5,
        out_specs=vmem(),
        scratch_shapes=WEIGHT_SCRATCH
        + [
            pltpu.VMEM((R, D), BF16),
            pltpu.VMEM((S, D), BF16),
            pltpu.VMEM((S, D), BF16),
            pltpu.VMEM((S, NF), F32),
            pltpu.VMEM((S, NF), F32),
            pltpu.VMEM((S, NQ), BF16),
            pltpu.VMEM((S, NO), BF16),
            pltpu.VMEM((S, NF), BF16),
        ]
        + SCATTER_SCRATCH
        + [dma((5,)), dma((1, 3, AC)), dma((1, 3, AC)), dma((3, RC)), dma((3, RC))],
        compiler_params=pltpu.CompilerParams(collective_id=0, has_side_effects=True, vmem_limit_bytes=VMEM_LIMIT),
    )(x, ga, gm, *weights)


def run_backward(layer, hin, dy, gin, ga, gm, weights):
    dma = pltpu.SemaphoreType.DMA
    last_call = layer == 0
    gshape = [jax.ShapeDtypeStruct((LAYERS, D), F32)] * 2 if last_call else [jax.ShapeDtypeStruct((8, D), F32)]
    saved = [jax.ShapeDtypeStruct(shape, BF16) for shape in SAVED]
    outs = pl.pallas_call(
        functools.partial(backward_kernel, layer),
        name=f"backward{layer}",
        out_shape=[jax.ShapeDtypeStruct((R, D), BF16)] + gshape + saved,
        in_specs=[vmem()] * 5 + [hbm()] * 5,
        out_specs=[vmem()] * (1 + len(gshape)) + [hbm()] * 9,
        scratch_shapes=[pltpu.VMEM(shape, BF16) for shape in SAVED]
        + WEIGHT_SCRATCH
        + [
            pltpu.VMEM((R, D), BF16),
            pltpu.VMEM((S, NF), F32),
            pltpu.VMEM((S, NF), F32),
            pltpu.VMEM((S, NQ), BF16),
            pltpu.VMEM((HEADS, S, S), F32),
            pltpu.VMEM((S, NF), BF16),
            pltpu.VMEM((S, NO), BF16),
        ]
        + SCATTER_SCRATCH
        + [pltpu.VMEM((8, D), F32)] * 3
        + [dma((5,)), dma((9,)), dma((4, 3, AC)), dma((4, 3, AC)), dma((3, RC)), dma((3, RC)), dma((2,)), dma((2,))],
        compiler_params=pltpu.CompilerParams(
            collective_id=1 + layer, has_side_effects=True, vmem_limit_bytes=VMEM_LIMIT
        ),
    )(hin, dy, gin, ga, gm, *weights)
    return outs[0], outs[1 : 1 + len(gshape)], outs[1 + len(gshape) :]


def run_wgrad(layer, saved, grads):
    dma = pltpu.SemaphoreType.DMA
    n_alias = len(grads)
    return pl.pallas_call(
        functools.partial(wgrad_kernel, layer, n_alias),
        name=f"wgrad{layer}",
        out_shape=[jax.ShapeDtypeStruct((LAYERS, *shape), BF16) for shape in GRADS],
        in_specs=[hbm()] * (9 + n_alias),
        out_specs=[hbm()] * 5,
        input_output_aliases={9 + i: i for i in range(n_alias)},
        scratch_shapes=[pltpu.VMEM(shape, BF16) for shape in SAVED]
        + [pltpu.VMEM((2, S, shape[1]), BF16) for shape in GRADS]
        + [dma((9,)), dma((5, 2))],
        compiler_params=pltpu.CompilerParams(vmem_limit_bytes=VMEM_LIMIT),
        cost_estimate=pl.CostEstimate(flops=8_600_000_000, bytes_accessed=42_000_000, transcendentals=0),
    )(*saved, *grads)


def solution(mesh):
    row_spec = P(("dp", "tp"), None)
    col_spec = P(None, None, "tp")
    mid_spec = P(None, "tp", None)
    in_specs = (row_spec, row_spec, P(None, None), P(None, None), col_spec, mid_spec, col_spec, col_spec, mid_spec)
    out_specs = (
        row_spec, row_spec, P("dp", None, "tp"), P("dp", "tp", None), P("dp", None, "tp"), P("dp", None, "tp"),
        P("dp", "tp", None), P("dp", None), P("dp", None),
    )

    def device_step(x, grad_y, gain_attn, gain_mlp, w_qkv, w_out, w_gate, w_up, w_down):
        weights = (w_qkv, w_out, w_gate, w_up, w_down)
        hs = run_forward(x, gain_attn, gain_mlp, weights)
        d_hidden = grad_y
        gains = [jnp.zeros((8, D), F32)]
        grads = ()
        for layer in reversed(range(LAYERS)):
            d_hidden, gains, saved = run_backward(
                layer, hs if layer > 0 else x, d_hidden, gains[0], gain_attn, gain_mlp, weights
            )
            grads = run_wgrad(layer, saved, grads)
            if layer > 0:
                d_hidden, grads = lax.optimization_barrier((d_hidden, grads))
        return (hs[LAYERS - 1], d_hidden, *grads, *gains)

    return jax.shard_map(device_step, mesh=mesh, in_specs=in_specs, out_specs=out_specs, check_vma=False)
```

```python
import functools

import jax
import jax.numpy as jnp
from jax import lax
from jax.experimental import pallas as pl
from jax.experimental.pallas import tpu as pltpu
from jax.sharding import PartitionSpec as P

HEAD = 128
EPS = 1e-5
MESH = pl.DeviceIdType.MESH
F32 = jnp.float32
BF16 = jnp.bfloat16
VMEM_LIMIT = 66_000_000

D = 2048
S = 256
R = 64
NQ = 1536
NO = 512
NF = 2048
HEADS = 4
LAYERS = 3

AC = 4
AW = D // AC
RC = 4
RW = D // RC


def dot(a, b):
    return jnp.dot(a, b, preferred_element_type=F32)


def dot_nt(a, b):
    return lax.dot_general(a, b, (((1,), (1,)), ((), ())), preferred_element_type=F32)


def dot_tn(a, b):
    return lax.dot_general(a, b, (((0,), (0,)), ((), ())), preferred_element_type=F32)


def ds(i, n):
    return pl.ds(i * n if isinstance(i, int) else pl.multiple_of(i * n, n), n)


def loop(n, body):
    lax.fori_loop(0, n, lambda i, c: (body(i), c)[1], 0)


class Peers:
    def __init__(self):
        self.me = lax.axis_index("tp")
        core, chip = lax.rem(self.me, 2), self.me // 2
        self.sib = chip * 2 + (1 - core)
        self.cross = (1 - chip) * 2 + core
        self.diag = (1 - chip) * 2 + (1 - core)

    def barrier(self):
        sem = pltpu.get_barrier_semaphore()
        for peer in (self.sib, self.cross):
            pl.semaphore_signal(sem, inc=1, device_id={"tp": peer}, device_id_type=MESH)
        pl.semaphore_wait(sem, 2)


def remote(src, dst, send, recv, peer):
    return pltpu.make_async_remote_copy(
        src_ref=src, dst_ref=dst, send_sem=send, recv_sem=recv, device_id={"tp": peer}, device_id_type=MESH
    )


class Gather:
    def __init__(self, p, buf, send, recv, which):
        self.p, self.buf, self.send, self.recv, self.which = p, buf, send, recv, which

    def _copy(self, kind, chunk, owner, peer):
        part = self.buf.at[ds(owner, R), ds(chunk, AW)]
        return remote(part, part, self.send.at[self.which, kind, chunk], self.recv.at[self.which, kind, chunk], peer)

    def to_cross(self, chunk):
        self._copy(0, chunk, self.p.me, self.p.cross).start()

    def to_sib(self, chunk):
        self._copy(1, chunk, self.p.me, self.p.sib).start()

    def relay(self, chunk):
        self._copy(0, chunk, self.p.cross, self.p.cross).wait_recv()
        self._copy(2, chunk, self.p.cross, self.p.sib).start()

    def arrived(self, chunk):
        self._copy(1, chunk, self.p.sib, self.p.sib).wait_recv()
        self._copy(2, chunk, self.p.diag, self.p.sib).wait_recv()

    def start(self):
        for chunk in range(AC):
            self.to_cross(chunk)
        for chunk in range(AC):
            self.to_sib(chunk)

    def each(self, body):
        for chunk in range(AC + 1):
            if chunk < AC:
                self.relay(chunk)
            if chunk > 0:
                self.arrived(chunk - 1)
                body(chunk - 1)

    def finish(self):
        for chunk in range(AC):
            self._copy(0, chunk, self.p.me, self.p.cross).wait_send()
            self._copy(1, chunk, self.p.me, self.p.sib).wait_send()
            self._copy(2, chunk, self.p.cross, self.p.sib).wait_send()


class Scatter:
    def __init__(self, p, part, near, out, far, send, recv):
        self.p, self.part, self.near, self.out, self.far, self.send, self.recv = p, part, near, out, far, send, recv

    def _near(self, kind, chunk):
        owner = self.p.diag if kind == 0 else self.p.sib
        return remote(
            self.part.at[ds(owner, R), ds(chunk, RW)],
            self.near.at[kind, :, ds(chunk, RW)],
            self.send.at[kind, chunk],
            self.recv.at[kind, chunk],
            self.p.sib,
        )

    def _far(self, chunk):
        return remote(
            self.out.at[:, ds(chunk, RW)],
            self.far.at[:, ds(chunk, RW)],
            self.send.at[2, chunk],
            self.recv.at[2, chunk],
            self.p.cross,
        )

    def _mid(self, chunk):
        self._near(0, chunk).wait_recv()
        cols = ds(chunk, RW)
        self.out[:, cols] = (self.part[ds(self.p.cross, R), cols] + self.near[0, :, cols]).astype(BF16)
        self._far(chunk).start()

    def run(self, compute):
        def step(chunk):
            self.part[:, ds(chunk, RW)] = compute(chunk)
            self._near(0, chunk).start()
            self._near(1, chunk).start()

            @pl.when(chunk > 0)
            def _():
                self._mid(chunk - 1)

        loop(RC, step)
        self._mid(RC - 1)

    def result(self):
        for chunk in range(RC):
            self._near(1, chunk).wait_recv()
            self._far(chunk).wait_recv()
        total = self.part[ds(self.p.me, R), :] + self.near[1] + self.far[...].astype(F32)
        for chunk in range(RC):
            self._near(0, chunk).wait_send()
            self._near(1, chunk).wait_send()
            self._far(chunk).wait_send()
        return total.astype(BF16)


HR = R // 2
HS = S // 2
HA = 2
HAW = D // HA
HC = 4
HW = D // HC


def owned(owner, half):
    return ds(half * 4 + owner, HR)


class HalfGather(Gather):
    def _copy(self, kind, item, owner, peer):
        half, chunk = item
        part = self.buf.at[owned(owner, half), ds(chunk, HAW)]
        sems = (self.which, kind, half, chunk)
        return remote(part, part, self.send.at[sems], self.recv.at[sems], peer)

    def start(self, half):
        for chunk in range(HA):
            self.to_cross((half, chunk))
        for chunk in range(HA):
            self.to_sib((half, chunk))

    def finish(self):
        for half in range(2):
            for chunk in range(HA):
                self._copy(0, (half, chunk), self.p.me, self.p.cross).wait_send()
                self._copy(1, (half, chunk), self.p.me, self.p.sib).wait_send()
                self._copy(2, (half, chunk), self.p.cross, self.p.sib).wait_send()


class HalfScatter(Scatter):
    def _near(self, kind, half, chunk):
        owner = self.p.diag if kind == 0 else self.p.sib
        return remote(
            self.part.at[owned(owner, half), ds(chunk, HW)],
            self.near.at[kind, ds(half, HR), ds(chunk, HW)],
            self.send.at[kind, half, chunk],
            self.recv.at[kind, half, chunk],
            self.p.sib,
        )

    def _far(self, half, chunk):
        return remote(
            self.out.at[ds(half, HR), ds(chunk, HW)],
            self.far.at[ds(half, HR), ds(chunk, HW)],
            self.send.at[2, half, chunk],
            self.recv.at[2, half, chunk],
            self.p.cross,
        )

    def run(self, half, compute):
        def step(chunk):
            self.part[ds(half, HS), ds(chunk, HW)] = compute(chunk)
            self._near(0, half, chunk).start()
            self._near(1, half, chunk).start()

        def mid(chunk):
            self._near(0, half, chunk).wait_recv()
            cols = ds(chunk, HW)
            total = self.part[owned(self.p.cross, half), cols] + self.near[0, ds(half, HR), cols]
            self.out[ds(half, HR), cols] = total.astype(BF16)
            self._far(half, chunk).start()

        loop(HC, step)
        loop(HC, mid)

    def result(self, half):
        for chunk in range(HC):
            self._near(1, half, chunk).wait_recv()
            self._far(half, chunk).wait_recv()
        rows = ds(half, HR)
        total = self.part[owned(self.p.me, half), :] + self.near[1, rows, :] + self.far[rows, :].astype(F32)
        for chunk in range(HC):
            self._near(0, half, chunk).wait_send()
            self._near(1, half, chunk).wait_send()
            self._far(half, chunk).wait_send()
        return total.astype(BF16)


def true_position(row):
    return lax.rem(row, HS) // HR * R + row // HS * HR + lax.rem(row, HR)


def norm(h, gain):
    hf = h.astype(F32)
    inv = lax.rsqrt(jnp.mean(hf * hf, axis=-1, keepdims=True) + EPS)
    return (hf * inv * gain).astype(BF16)


def norm_back(h, gain, dy):
    hf, dyf = h.astype(F32), dy.astype(F32)
    inv = lax.rsqrt(jnp.mean(hf * hf, axis=-1, keepdims=True) + EPS)
    dgain = jnp.sum(dyf * (hf * inv), axis=0, keepdims=True)
    dn = dyf * gain
    slope = jnp.sum(dn * hf, axis=-1, keepdims=True) * (inv * inv * inv) / D
    return (dn * inv - hf * slope).astype(BF16), dgain


def softmax_scores(q, k, halves=False):
    scores = dot_nt(q, k) * HEAD**-0.5
    rows = lax.broadcasted_iota(jnp.int32, (S, S), 0)
    cols = lax.broadcasted_iota(jnp.int32, (S, S), 1)
    if halves:
        rows, cols = true_position(rows), true_position(cols)
    scores = jnp.where(rows >= cols, scores, -1e30)
    e = jnp.exp(scores - jnp.max(scores, axis=-1, keepdims=True))
    return e / jnp.sum(e, axis=-1, keepdims=True)


def head_cols(head, which):
    return pl.ds(pl.multiple_of(head * 3 * HEAD + which * HEAD, HEAD), HEAD)


def attention(qkv, o, probs=None, halves=False):
    def one(head):
        prob = softmax_scores(qkv[:, head_cols(head, 0)], qkv[:, head_cols(head, 1)], halves)
        if probs is not None:
            probs[head] = prob
        o[:, ds(head, HEAD)] = dot(prob.astype(BF16), qkv[:, head_cols(head, 2)]).astype(BF16)

    loop(HEADS, one)


def qkv_chunk(u, wq, acc, qkv, tile=768):
    def body(chunk):
        def one(j):
            cols = ds(j, tile)
            part = dot(u[:, ds(chunk, AW)], wq[ds(chunk, AW), cols])
            if chunk > 0:
                part = part + acc[:, cols]
            if chunk < AC - 1:
                acc[:, cols] = part
            else:
                qkv[:, cols] = part.astype(BF16)

        loop(NQ // tile, one)

    return body


def mlp_chunk(n, wg, wu, acc1, acc3, last, tile=512):
    def body(chunk):
        def one(j):
            cols = ds(j, tile)
            z1 = dot(n[:, ds(chunk, AW)], wg[ds(chunk, AW), cols])
            z3 = dot(n[:, ds(chunk, AW)], wu[ds(chunk, AW), cols])
            if chunk > 0:
                z1, z3 = z1 + acc1[:, cols], z3 + acc3[:, cols]
            if chunk < AC - 1:
                acc1[:, cols] = z1
                acc3[:, cols] = z3
            else:
                last(cols, z1.astype(BF16).astype(F32), z3.astype(BF16).astype(F32))

        loop(NF // tile, one)

    return body


def half_qkv(u, wq, acc, qkv, tile=768):
    def body(half, chunk):
        rows, deep = ds(half, HS), ds(chunk, HAW)

        def one(j):
            cols = ds(j, tile)
            part = dot(u[rows, deep], wq[deep, cols])
            if chunk > 0:
                part = part + acc[rows, cols]
            if chunk < HA - 1:
                acc[rows, cols] = part
            else:
                qkv[rows, cols] = part.astype(BF16)

        loop(NQ // tile, one)

    return body


def half_mlp(n, wg, wu, acc1, acc3, last, tile=512):
    def body(half, chunk):
        rows, deep = ds(half, HS), ds(chunk, HAW)

        def one(j):
            cols = ds(j, tile)
            z1 = dot(n[rows, deep], wg[deep, cols])
            z3 = dot(n[rows, deep], wu[deep, cols])
            if chunk > 0:
                z1, z3 = z1 + acc1[rows, cols], z3 + acc3[rows, cols]
            if chunk < HA - 1:
                acc1[rows, cols] = z1
                acc3[rows, cols] = z3
            else:
                last(rows, cols, z1.astype(BF16).astype(F32), z3.astype(BF16).astype(F32))

        loop(NF // tile, one)

    return body


ITEMS = [(half, chunk) for half in range(2) for chunk in range(HA)]


def in_order(gather, body):
    for i in range(len(ITEMS) + 1):
        if i < len(ITEMS):
            gather.relay(ITEMS[i])
        if i > 0:
            gather.arrived(ITEMS[i - 1])
            body(*ITEMS[i - 1])


def forward_kernel(x, ga, gm, wq_h, wo_h, wg_h, wu_h, wd_h, hs,
                   wq, wo, wg, wu, wd, h, u, n, acc1, acc3, qkv, o, m, part, near, out, far,
                   wsem, gsend, grecv, ssend, srecv):
    p = Peers()
    pairs = ((wq_h, wq), (wo_h, wo), (wg_h, wg), (wu_h, wu), (wd_h, wd))

    def load(i, layer):
        return pltpu.make_async_copy(pairs[i][0].at[layer], pairs[i][1], wsem.at[i])

    for i in range(5):
        load(i, 0).start()
    h[...] = x[...]
    p.barrier()
    gu = HalfGather(p, u, gsend, grecv, 0)
    gn = HalfGather(p, n, gsend, grecv, 1)
    scatter = HalfScatter(p, part, near, out, far, ssend, srecv)

    def enter(half, layer):
        u[owned(p.me, half), :] = norm(h[ds(half, HR), :], ga[pl.ds(layer, 1), :])
        gu.start(half)

    def add(half):
        rows = ds(half, HR)
        h[rows, :] = h[rows, :] + scatter.result(half)
        return h[rows, :]

    enter(0, 0)
    enter(1, 0)

    def layer_step(layer):
        more = layer < LAYERS - 1

        def refill(i):
            @pl.when(more)
            def _():
                load(i, layer + 1).start()

        load(0, layer).wait()
        in_order(gu, half_qkv(u, wq, acc1, qkv))
        refill(0)
        attention(qkv, o, halves=True)
        load(1, layer).wait()
        for half in range(2):
            scatter.run(half, lambda c: dot(o[ds(half, HS), :], wo[:, ds(c, HW)]))
        refill(1)
        gu.finish()
        for half in range(2):
            n[owned(p.me, half), :] = norm(add(half), gm[pl.ds(layer, 1), :])
            gn.start(half)

        def last(rows, cols, z1, z3):
            m[rows, cols] = (z1 * jax.nn.sigmoid(z1) * z3).astype(BF16)

        def leave(half):
            hs[layer, ds(half, HR), :] = add(half)

            @pl.when(more)
            def _():
                enter(half, layer + 1)

        gate_up = half_mlp(n, wg, wu, acc1, acc3, last)
        for i in (2, 3):
            load(i, layer).wait()
        gn.relay((0, 0))
        gn.relay((0, 1))
        gn.arrived((0, 0))
        gate_up(0, 0)
        gn.relay((1, 0))
        gn.arrived((0, 1))
        gate_up(0, 1)
        gn.relay((1, 1))
        load(4, layer).wait()
        scatter.run(0, lambda c: dot(m[ds(0, HS), :], wd[:, ds(c, HW)]))
        gn.arrived((1, 0))
        gate_up(1, 0)
        gn.arrived((1, 1))
        gate_up(1, 1)
        refill(2)
        refill(3)
        leave(0)
        scatter.run(1, lambda c: dot(m[ds(1, HS), :], wd[:, ds(c, HW)]))
        refill(4)
        gn.finish()
        leave(1)

    loop(LAYERS, layer_step)


def backward_kernel(layer, hin, dy, gin, ga, gm, wq_h, wo_h, wg_h, wu_h, wd_h, *refs):
    last_call = layer == 0
    refs = list(refs)
    take = lambda k: [refs.pop(0) for _ in range(k)]
    (dx,) = take(1)
    gouts = take(2 if last_call else 1)
    saved_h = take(9)
    u, dqkv, o, da, n, dg, du, m, dd = saved = take(9)
    wq, wo, wg, wu, wd = take(5)
    hm, acc1, acc3, qkv, probs, dgated, dh, part, near, out, far, gbuf = take(12)
    gmid, gfar = take(2)
    wsem, osem, gsend, grecv, ssend, srecv, rsend, rrecv = take(8)

    p = Peers()
    pairs = ((wq_h, wq), (wo_h, wo), (wg_h, wg), (wu_h, wu), (wd_h, wd))
    loads = [pltpu.make_async_copy(src.at[layer], dst, wsem.at[i]) for i, (src, dst) in enumerate(pairs)]
    saves = [pltpu.make_async_copy(src, dst, osem.at[i]) for i, (src, dst) in enumerate(zip(saved, saved_h))]
    for i in (0, 1, 4, 2, 3):
        loads[i].start()
    mine = ds(p.me, R)
    h = hin[layer - 1] if layer > 0 else hin[...]
    gain_a, gain_m = ga[pl.ds(layer, 1), :], gm[pl.ds(layer, 1), :]
    u[mine, :] = norm(h, gain_a)
    dd[mine, :] = dy[...]
    p.barrier()
    gu = Gather(p, u, gsend, grecv, 0)
    gd = Gather(p, dd, gsend, grecv, 1)
    gu.start()
    for c in range(AC):
        gd.to_sib(c)
    for c in range(AC // 2):
        gd.to_cross(c)

    loads[0].wait()
    gu.each(qkv_chunk(u, wq, acc1, qkv))
    saves[0].start()
    attention(qkv, o, probs)
    saves[2].start()
    loads[1].wait()
    scatter = Scatter(p, part, near, out, far, ssend, srecv)
    scatter.run(lambda c: dot(o[...], wo[:, ds(c, RW)]))
    for c in range(AC // 2, AC):
        gd.to_cross(c)
    for c in range(AC // 2):
        gd.relay(c)
    h_mid = h + scatter.result()
    hm[...] = h_mid
    n[mine, :] = norm(h_mid, gain_m)
    gn = Gather(p, n, gsend, grecv, 2)
    gn.start()

    for c in range(AC // 2, AC):
        gd.relay(c)
    for c in range(AC):
        gd.arrived(c)
    saves[8].start()
    loads[4].wait()

    def gated(j):
        dgated[:, ds(j, 512)] = dot_nt(dd[...], wd[ds(j, 512), :]).astype(BF16)

    loop(NF // 512, gated)
    loads[2].wait()
    loads[3].wait()

    def last(cols, z1, z3):
        sig = jax.nn.sigmoid(z1)
        silu = z1 * sig
        dm = dgated[:, cols].astype(F32)
        m[:, cols] = (silu * z3).astype(BF16)
        du[:, cols] = (dm * silu).astype(BF16)
        dg[:, cols] = (dm * z3 * (sig + silu * (1.0 - sig))).astype(BF16)

    gn.each(mlp_chunk(n, wg, wu, acc1, acc3, last))
    for i in (4, 5, 6, 7):
        saves[i].start()

    scatter.run(lambda c: dot_nt(dg[...], wg[ds(c, RW), :]) + dot_nt(du[...], wu[ds(c, RW), :]))
    d_norm, dgain_m = norm_back(hm[...], gain_m, scatter.result())
    d_mid = dy[...] + d_norm
    da[mine, :] = d_mid
    ga_ = Gather(p, da, gsend, grecv, 3)
    ga_.start()
    gbuf[...] = gin[...]
    gbuf[pl.ds(LAYERS + layer, 1), :] = dgain_m

    def heads_chunk(chunk):
        part_h = dot_nt(da[:, ds(chunk, AW)], wo[:, ds(chunk, AW)])
        if chunk > 0:
            part_h = part_h + acc1[:, :NO]
        if chunk < AC - 1:
            acc1[:, :NO] = part_h
        else:
            dh[...] = part_h.astype(BF16)

    ga_.each(heads_chunk)
    saves[3].start()

    def back(head):
        prob = probs[head]
        d_o = dh[:, ds(head, HEAD)]
        q, k, v = (qkv[:, head_cols(head, i)] for i in range(3))
        d_prob = dot_nt(d_o, v)
        d_scores = (prob * (d_prob - jnp.sum(d_prob * prob, axis=-1, keepdims=True)) * HEAD**-0.5).astype(BF16)
        dqkv[:, head_cols(head, 0)] = dot(d_scores, k).astype(BF16)
        dqkv[:, head_cols(head, 1)] = dot_tn(d_scores, q).astype(BF16)
        dqkv[:, head_cols(head, 2)] = dot_tn(prob.astype(BF16), d_o).astype(BF16)

    loop(HEADS, back)
    saves[1].start()
    scatter.run(lambda c: dot_nt(dqkv[...], wq[ds(c, RW), :]))
    d_norm, dgain_a = norm_back(h, gain_a, scatter.result())
    dx[...] = da[mine, :] + d_norm
    gbuf[pl.ds(layer, 1), :] = dgain_a

    if last_call:
        near_g = remote(gbuf, gmid, rsend.at[0], rrecv.at[0], p.sib)
        near_g.start()
        near_g.wait()
        gbuf[...] = gbuf[...] + gmid[...]
        far_g = remote(gbuf, gfar, rsend.at[1], rrecv.at[1], p.cross)
        far_g.start()
        far_g.wait()
        total = gbuf[...] + gfar[...]
        gouts[0][...] = total[:LAYERS]
        gouts[1][...] = total[LAYERS:2 * LAYERS]
    else:
        gouts[0][...] = gbuf[...]
    for g in (gu, gd, gn, ga_):
        g.finish()
    for save in saves:
        save.wait()


def wgrad_kernel(layer, n_alias, u_h, dqkv_h, o_h, da_h, n_h, dg_h, du_h, m_h, dd_h, *refs):
    refs = list(refs[n_alias:])
    take = lambda k: [refs.pop(0) for _ in range(k)]
    outs = take(5)
    u, dqkv, o, da, n, dg, du, m, dd = acts = take(9)
    stages = take(5)
    isem, osem = take(2)
    loads = [pltpu.make_async_copy(src, dst, isem.at[i])
             for i, (src, dst) in enumerate(zip((u_h, dqkv_h, o_h, da_h, n_h, dg_h, du_h, m_h, dd_h), acts))]
    order = (0, 1, 4, 5, 6, 7, 8, 2, 3)
    for i in order:
        loads[i].start()
    work = ((0, 0, 1), (2, 4, 5), (3, 4, 6), (4, 7, 8), (1, 2, 3))
    waited, copies = set(), []
    for out_i, a_i, b_i in work:
        for i in (a_i, b_i):
            if i not in waited:
                loads[i].wait()
                waited.add(i)
        a, b, out, stage = acts[a_i], acts[b_i], outs[out_i], stages[out_i]
        tiles, cols = a.shape[1] // S, b.shape[1]

        def copy(i):
            rows = ds(i, S)
            return pltpu.make_async_copy(stage.at[rows, :], out.at[layer, rows, :], osem.at[out_i, i])

        def step(i):
            lhs = a[:, ds(i, S)].T
            for c in range(cols // 512):
                stage[ds(i, S), ds(c, 512)] = dot(lhs, b[:, ds(c, 512)]).astype(BF16)
            copy(i).start()

        loop(tiles, step)
        copies += [copy(i) for i in range(tiles)]
    for each in copies:
        each.wait()


def vmem():
    return pl.BlockSpec(memory_space=pltpu.VMEM)


def hbm():
    return pl.BlockSpec(memory_space=pl.ANY)


WEIGHT_SCRATCH = [
    pltpu.VMEM((D, NQ), BF16),
    pltpu.VMEM((NO, D), BF16),
    pltpu.VMEM((D, NF), BF16),
    pltpu.VMEM((D, NF), BF16),
    pltpu.VMEM((NF, D), BF16),
]
SCATTER_SCRATCH = [
    pltpu.VMEM((S, D), F32),
    pltpu.VMEM((2, R, D), F32),
    pltpu.VMEM((R, D), BF16),
    pltpu.VMEM((R, D), BF16),
]
SAVED = [(S, D), (S, NQ), (S, NO), (S, D), (S, D), (S, NF), (S, NF), (S, NF), (S, D)]
GRADS = [(D, NQ), (NO, D), (D, NF), (D, NF), (NF, D)]


def run_forward(x, ga, gm, weights):
    dma = pltpu.SemaphoreType.DMA
    return pl.pallas_call(
        forward_kernel,
        name="forward",
        out_shape=jax.ShapeDtypeStruct((LAYERS, R, D), BF16),
        in_specs=[vmem()] * 3 + [hbm()] * 5,
        out_specs=vmem(),
        scratch_shapes=WEIGHT_SCRATCH
        + [
            pltpu.VMEM((R, D), BF16),
            pltpu.VMEM((S, D), BF16),
            pltpu.VMEM((S, D), BF16),
            pltpu.VMEM((S, NF), F32),
            pltpu.VMEM((S, NF), F32),
            pltpu.VMEM((S, NQ), BF16),
            pltpu.VMEM((S, NO), BF16),
            pltpu.VMEM((S, NF), BF16),
        ]
        + SCATTER_SCRATCH
        + [dma((5,)), dma((2, 3, 2, HA)), dma((2, 3, 2, HA)), dma((3, 2, HC)), dma((3, 2, HC))],
        compiler_params=pltpu.CompilerParams(collective_id=0, has_side_effects=True, vmem_limit_bytes=VMEM_LIMIT),
    )(x, ga, gm, *weights)


def run_backward(layer, hin, dy, gin, ga, gm, weights):
    dma = pltpu.SemaphoreType.DMA
    last_call = layer == 0
    gshape = [jax.ShapeDtypeStruct((LAYERS, D), F32)] * 2 if last_call else [jax.ShapeDtypeStruct((8, D), F32)]
    saved = [jax.ShapeDtypeStruct(shape, BF16) for shape in SAVED]
    outs = pl.pallas_call(
        functools.partial(backward_kernel, layer),
        name=f"backward{layer}",
        out_shape=[jax.ShapeDtypeStruct((R, D), BF16)] + gshape + saved,
        in_specs=[vmem()] * 5 + [hbm()] * 5,
        out_specs=[vmem()] * (1 + len(gshape)) + [hbm()] * 9,
        scratch_shapes=[pltpu.VMEM(shape, BF16) for shape in SAVED]
        + WEIGHT_SCRATCH
        + [
            pltpu.VMEM((R, D), BF16),
            pltpu.VMEM((S, NF), F32),
            pltpu.VMEM((S, NF), F32),
            pltpu.VMEM((S, NQ), BF16),
            pltpu.VMEM((HEADS, S, S), F32),
            pltpu.VMEM((S, NF), BF16),
            pltpu.VMEM((S, NO), BF16),
        ]
        + SCATTER_SCRATCH
        + [pltpu.VMEM((8, D), F32)] * 3
        + [dma((5,)), dma((9,)), dma((4, 3, AC)), dma((4, 3, AC)), dma((3, RC)), dma((3, RC)), dma((2,)), dma((2,))],
        compiler_params=pltpu.CompilerParams(
            collective_id=1 + layer, has_side_effects=True, vmem_limit_bytes=VMEM_LIMIT
        ),
    )(hin, dy, gin, ga, gm, *weights)
    return outs[0], outs[1 : 1 + len(gshape)], outs[1 + len(gshape) :]


def run_wgrad(layer, saved, grads):
    dma = pltpu.SemaphoreType.DMA
    n_alias = len(grads)
    return pl.pallas_call(
        functools.partial(wgrad_kernel, layer, n_alias),
        name=f"wgrad{layer}",
        out_shape=[jax.ShapeDtypeStruct((LAYERS, *shape), BF16) for shape in GRADS],
        in_specs=[hbm()] * (9 + n_alias),
        out_specs=[hbm()] * 5,
        input_output_aliases={9 + i: i for i in range(n_alias)},
        scratch_shapes=[pltpu.VMEM(shape, BF16) for shape in SAVED]
        + [pltpu.VMEM(shape, BF16) for shape in GRADS]
        + [dma((9,)), dma((5, 8))],
        compiler_params=pltpu.CompilerParams(vmem_limit_bytes=VMEM_LIMIT),
        cost_estimate=pl.CostEstimate(flops=8_600_000_000, bytes_accessed=42_000_000, transcendentals=0),
    )(*saved, *grads)


def solution(mesh):
    row_spec = P(("dp", "tp"), None)
    col_spec = P(None, None, "tp")
    mid_spec = P(None, "tp", None)
    in_specs = (row_spec, row_spec, P(None, None), P(None, None), col_spec, mid_spec, col_spec, col_spec, mid_spec)
    out_specs = (
        row_spec, row_spec, P("dp", None, "tp"), P("dp", "tp", None), P("dp", None, "tp"), P("dp", None, "tp"),
        P("dp", "tp", None), P("dp", None), P("dp", None),
    )

    def device_step(x, grad_y, gain_attn, gain_mlp, w_qkv, w_out, w_gate, w_up, w_down):
        weights = (w_qkv, w_out, w_gate, w_up, w_down)
        hs = run_forward(x, gain_attn, gain_mlp, weights)
        d_hidden = grad_y
        gains = [jnp.zeros((8, D), F32)]
        grads = ()
        for layer in reversed(range(LAYERS)):
            d_hidden, gains, saved = run_backward(
                layer, hs if layer > 0 else x, d_hidden, gains[0], gain_attn, gain_mlp, weights
            )
            grads = run_wgrad(layer, saved, grads)
            if layer > 0:
                d_hidden, grads = lax.optimization_barrier((d_hidden, grads))
        return (hs[LAYERS - 1], d_hidden, *grads, *gains)

    return jax.shard_map(device_step, mesh=mesh, in_specs=in_specs, out_specs=out_specs, check_vma=False)
```

```python
import functools

import jax
import jax.numpy as jnp
from jax import lax
from jax.experimental import pallas as pl
from jax.experimental.pallas import tpu as pltpu
from jax.sharding import PartitionSpec as P

HEAD = 128
EPS = 1e-5
MESH = pl.DeviceIdType.MESH
F32 = jnp.float32
BF16 = jnp.bfloat16
VMEM_LIMIT = 66_000_000

D = 2048
S = 256
R = 64
NQ = 1536
NO = 512
NF = 2048
HEADS = 4
LAYERS = 3

AC = 4
AW = D // AC
RC = 4
RW = D // RC


def dot(a, b):
    return jnp.dot(a, b, preferred_element_type=F32)


def dot_nt(a, b):
    return lax.dot_general(a, b, (((1,), (1,)), ((), ())), preferred_element_type=F32)


def dot_tn(a, b):
    return lax.dot_general(a, b, (((0,), (0,)), ((), ())), preferred_element_type=F32)


def ds(i, n):
    return pl.ds(i * n if isinstance(i, int) else pl.multiple_of(i * n, n), n)


def loop(n, body):
    lax.fori_loop(0, n, lambda i, c: (body(i), c)[1], 0)


class Peers:
    def __init__(self):
        self.me = lax.axis_index("tp")
        core, chip = lax.rem(self.me, 2), self.me // 2
        self.sib = chip * 2 + (1 - core)
        self.cross = (1 - chip) * 2 + core
        self.diag = (1 - chip) * 2 + (1 - core)

    def barrier(self):
        sem = pltpu.get_barrier_semaphore()
        for peer in (self.sib, self.cross):
            pl.semaphore_signal(sem, inc=1, device_id={"tp": peer}, device_id_type=MESH)
        pl.semaphore_wait(sem, 2)


def remote(src, dst, send, recv, peer):
    return pltpu.make_async_remote_copy(
        src_ref=src, dst_ref=dst, send_sem=send, recv_sem=recv, device_id={"tp": peer}, device_id_type=MESH
    )


class Gather:
    def __init__(self, p, buf, send, recv, which):
        self.p, self.buf, self.send, self.recv, self.which = p, buf, send, recv, which

    def _copy(self, kind, chunk, owner, peer):
        part = self.buf.at[ds(owner, R), ds(chunk, AW)]
        return remote(part, part, self.send.at[self.which, kind, chunk], self.recv.at[self.which, kind, chunk], peer)

    def to_cross(self, chunk):
        self._copy(0, chunk, self.p.me, self.p.cross).start()

    def to_sib(self, chunk):
        self._copy(1, chunk, self.p.me, self.p.sib).start()

    def relay(self, chunk):
        self._copy(0, chunk, self.p.cross, self.p.cross).wait_recv()
        self._copy(2, chunk, self.p.cross, self.p.sib).start()

    def arrived(self, chunk):
        self._copy(1, chunk, self.p.sib, self.p.sib).wait_recv()
        self._copy(2, chunk, self.p.diag, self.p.sib).wait_recv()

    def start(self):
        for chunk in range(AC):
            self.to_cross(chunk)
        for chunk in range(AC):
            self.to_sib(chunk)

    def each(self, body):
        for chunk in range(AC + 1):
            if chunk < AC:
                self.relay(chunk)
            if chunk > 0:
                self.arrived(chunk - 1)
                body(chunk - 1)

    def finish(self):
        for chunk in range(AC):
            self._copy(0, chunk, self.p.me, self.p.cross).wait_send()
            self._copy(1, chunk, self.p.me, self.p.sib).wait_send()
            self._copy(2, chunk, self.p.cross, self.p.sib).wait_send()


class Scatter:
    def __init__(self, p, part, near, out, far, send, recv):
        self.p, self.part, self.near, self.out, self.far, self.send, self.recv = p, part, near, out, far, send, recv

    def _near(self, kind, chunk):
        owner = self.p.diag if kind == 0 else self.p.sib
        return remote(
            self.part.at[ds(owner, R), ds(chunk, RW)],
            self.near.at[kind, :, ds(chunk, RW)],
            self.send.at[kind, chunk],
            self.recv.at[kind, chunk],
            self.p.sib,
        )

    def _far(self, chunk):
        return remote(
            self.out.at[:, ds(chunk, RW)],
            self.far.at[:, ds(chunk, RW)],
            self.send.at[2, chunk],
            self.recv.at[2, chunk],
            self.p.cross,
        )

    def _mid(self, chunk):
        self._near(0, chunk).wait_recv()
        cols = ds(chunk, RW)
        self.out[:, cols] = (self.part[ds(self.p.cross, R), cols] + self.near[0, :, cols]).astype(BF16)
        self._far(chunk).start()

    def run(self, compute):
        def step(chunk):
            self.part[:, ds(chunk, RW)] = compute(chunk)
            self._near(0, chunk).start()
            self._near(1, chunk).start()

            @pl.when(chunk > 0)
            def _():
                self._mid(chunk - 1)

        loop(RC, step)
        self._mid(RC - 1)

    def result(self):
        for chunk in range(RC):
            self._near(1, chunk).wait_recv()
            self._far(chunk).wait_recv()
        total = self.part[ds(self.p.me, R), :] + self.near[1] + self.far[...].astype(F32)
        for chunk in range(RC):
            self._near(0, chunk).wait_send()
            self._near(1, chunk).wait_send()
            self._far(chunk).wait_send()
        return total.astype(BF16)


HR = R // 2
HS = S // 2
HA = 4
HAW = D // HA
HC = 4
HW = D // HC


def owned(owner, half):
    return ds(half * 4 + owner, HR)


class HalfGather(Gather):
    def _copy(self, kind, item, owner, peer):
        half, chunk = item
        part = self.buf.at[owned(owner, half), ds(chunk, HAW)]
        sems = (self.which, kind, half, chunk)
        return remote(part, part, self.send.at[sems], self.recv.at[sems], peer)

    def start(self, half):
        for chunk in range(HA):
            self.to_cross((half, chunk))
        for chunk in range(HA):
            self.to_sib((half, chunk))

    def finish(self):
        for half in range(2):
            for chunk in range(HA):
                self._copy(0, (half, chunk), self.p.me, self.p.cross).wait_send()
                self._copy(1, (half, chunk), self.p.me, self.p.sib).wait_send()
                self._copy(2, (half, chunk), self.p.cross, self.p.sib).wait_send()


class HalfScatter(Scatter):
    def _near(self, kind, half, chunk):
        owner = self.p.diag if kind == 0 else self.p.sib
        return remote(
            self.part.at[owned(owner, half), ds(chunk, HW)],
            self.near.at[kind, ds(half, HR), ds(chunk, HW)],
            self.send.at[kind, half, chunk],
            self.recv.at[kind, half, chunk],
            self.p.sib,
        )

    def _far(self, half, chunk):
        return remote(
            self.out.at[ds(half, HR), ds(chunk, HW)],
            self.far.at[ds(half, HR), ds(chunk, HW)],
            self.send.at[2, half, chunk],
            self.recv.at[2, half, chunk],
            self.p.cross,
        )

    def run(self, half, compute):
        def step(chunk):
            self.part[ds(half, HS), ds(chunk, HW)] = compute(chunk)
            self._near(0, half, chunk).start()
            self._near(1, half, chunk).start()

        def mid(chunk):
            self._near(0, half, chunk).wait_recv()
            cols = ds(chunk, HW)
            total = self.part[owned(self.p.cross, half), cols] + self.near[0, ds(half, HR), cols]
            self.out[ds(half, HR), cols] = total.astype(BF16)
            self._far(half, chunk).start()

        loop(HC, step)
        loop(HC, mid)

    def result(self, half):
        for chunk in range(HC):
            self._near(1, half, chunk).wait_recv()
            self._far(half, chunk).wait_recv()
        rows = ds(half, HR)
        total = self.part[owned(self.p.me, half), :] + self.near[1, rows, :] + self.far[rows, :].astype(F32)
        for chunk in range(HC):
            self._near(0, half, chunk).wait_send()
            self._near(1, half, chunk).wait_send()
            self._far(half, chunk).wait_send()
        return total.astype(BF16)


def true_position(row):
    return lax.rem(row, HS) // HR * R + row // HS * HR + lax.rem(row, HR)


def norm(h, gain):
    hf = h.astype(F32)
    inv = lax.rsqrt(jnp.mean(hf * hf, axis=-1, keepdims=True) + EPS)
    return (hf * inv * gain).astype(BF16)


def norm_back(h, gain, dy):
    hf, dyf = h.astype(F32), dy.astype(F32)
    inv = lax.rsqrt(jnp.mean(hf * hf, axis=-1, keepdims=True) + EPS)
    dgain = jnp.sum(dyf * (hf * inv), axis=0, keepdims=True)
    dn = dyf * gain
    slope = jnp.sum(dn * hf, axis=-1, keepdims=True) * (inv * inv * inv) / D
    return (dn * inv - hf * slope).astype(BF16), dgain


def softmax_scores(q, k, halves=False):
    scores = dot_nt(q, k) * HEAD**-0.5
    rows = lax.broadcasted_iota(jnp.int32, (S, S), 0)
    cols = lax.broadcasted_iota(jnp.int32, (S, S), 1)
    if halves:
        rows, cols = true_position(rows), true_position(cols)
    scores = jnp.where(rows >= cols, scores, -1e30)
    e = jnp.exp(scores - jnp.max(scores, axis=-1, keepdims=True))
    return e / jnp.sum(e, axis=-1, keepdims=True)


def head_cols(head, which):
    return pl.ds(pl.multiple_of(head * 3 * HEAD + which * HEAD, HEAD), HEAD)


def attention(qkv, o, probs=None, halves=False):
    def one(head):
        prob = softmax_scores(qkv[:, head_cols(head, 0)], qkv[:, head_cols(head, 1)], halves)
        if probs is not None:
            probs[head] = prob
        o[:, ds(head, HEAD)] = dot(prob.astype(BF16), qkv[:, head_cols(head, 2)]).astype(BF16)

    loop(HEADS, one)


def qkv_chunk(u, wq, acc, qkv, tile=768):
    def body(chunk):
        def one(j):
            cols = ds(j, tile)
            part = dot(u[:, ds(chunk, AW)], wq[ds(chunk, AW), cols])
            if chunk > 0:
                part = part + acc[:, cols]
            if chunk < AC - 1:
                acc[:, cols] = part
            else:
                qkv[:, cols] = part.astype(BF16)

        loop(NQ // tile, one)

    return body


def mlp_chunk(n, wg, wu, acc1, acc3, last, tile=512):
    def body(chunk):
        def one(j):
            cols = ds(j, tile)
            z1 = dot(n[:, ds(chunk, AW)], wg[ds(chunk, AW), cols])
            z3 = dot(n[:, ds(chunk, AW)], wu[ds(chunk, AW), cols])
            if chunk > 0:
                z1, z3 = z1 + acc1[:, cols], z3 + acc3[:, cols]
            if chunk < AC - 1:
                acc1[:, cols] = z1
                acc3[:, cols] = z3
            else:
                last(cols, z1.astype(BF16).astype(F32), z3.astype(BF16).astype(F32))

        loop(NF // tile, one)

    return body


def half_qkv(u, wq, acc, qkv, tile=768):
    def body(half, chunk):
        rows, deep = ds(half, HS), ds(chunk, HAW)

        def one(j):
            cols = ds(j, tile)
            part = dot(u[rows, deep], wq[deep, cols])
            if chunk > 0:
                part = part + acc[rows, cols]
            if chunk < HA - 1:
                acc[rows, cols] = part
            else:
                qkv[rows, cols] = part.astype(BF16)

        loop(NQ // tile, one)

    return body


def half_mlp(n, wg, wu, acc1, acc3, last, tile=512):
    def body(half, chunk):
        rows, deep = ds(half, HS), ds(chunk, HAW)

        def one(j):
            cols = ds(j, tile)
            z1 = dot(n[rows, deep], wg[deep, cols])
            z3 = dot(n[rows, deep], wu[deep, cols])
            if chunk > 0:
                z1, z3 = z1 + acc1[rows, cols], z3 + acc3[rows, cols]
            if chunk < HA - 1:
                acc1[rows, cols] = z1
                acc3[rows, cols] = z3
            else:
                last(rows, cols, z1.astype(BF16).astype(F32), z3.astype(BF16).astype(F32))

        loop(NF // tile, one)

    return body


ITEMS = [(half, chunk) for half in range(2) for chunk in range(HA)]


def in_order(gather, body):
    for i in range(len(ITEMS) + 1):
        if i < len(ITEMS):
            gather.relay(ITEMS[i])
        if i > 0:
            gather.arrived(ITEMS[i - 1])
            body(*ITEMS[i - 1])


def forward_kernel(x, ga, gm, wq_h, wo_h, wg_h, wu_h, wd_h, hs, y,
                   wq, wo, wg, wu, wd, h, u, n, acc1, acc3, qkv, o, m, part, near, out, far,
                   wsem, gsend, grecv, ssend, srecv):
    p = Peers()
    pairs = ((wq_h, wq), (wo_h, wo), (wg_h, wg), (wu_h, wu), (wd_h, wd))

    def load(i, layer):
        return pltpu.make_async_copy(pairs[i][0].at[layer], pairs[i][1], wsem.at[i])

    for i in range(5):
        load(i, 0).start()
    h[...] = x[...]
    p.barrier()
    gu = HalfGather(p, u, gsend, grecv, 0)
    gn = HalfGather(p, n, gsend, grecv, 1)
    scatter = HalfScatter(p, part, near, out, far, ssend, srecv)

    def enter(half, layer):
        u[owned(p.me, half), :] = norm(h[ds(half, HR), :], ga[pl.ds(layer, 1), :])
        gu.start(half)

    def add(half):
        rows = ds(half, HR)
        h[rows, :] = h[rows, :] + scatter.result(half)
        return h[rows, :]

    enter(0, 0)
    enter(1, 0)

    def layer_step(layer):
        more = layer < LAYERS - 1

        def refill(i):
            @pl.when(more)
            def _():
                load(i, layer + 1).start()

        load(0, layer).wait()
        in_order(gu, half_qkv(u, wq, acc1, qkv))
        refill(0)
        attention(qkv, o, halves=True)
        load(1, layer).wait()
        for half in range(2):
            scatter.run(half, lambda c: dot(o[ds(half, HS), :], wo[:, ds(c, HW)]))
        refill(1)
        gu.finish()
        for half in range(2):
            n[owned(p.me, half), :] = norm(add(half), gm[pl.ds(layer, 1), :])
            gn.start(half)

        def last(rows, cols, z1, z3):
            m[rows, cols] = (z1 * jax.nn.sigmoid(z1) * z3).astype(BF16)

        def leave(half):
            total = add(half)

            @pl.when(more)
            def _():
                hs[layer, ds(half, HR), :] = total
                enter(half, layer + 1)

            @pl.when(jnp.logical_not(more))
            def _():
                y[ds(half, HR), :] = total

        gate_up = half_mlp(n, wg, wu, acc1, acc3, last)
        for i in (2, 3):
            load(i, layer).wait()
        for i, item in enumerate(ITEMS):
            if i == 0:
                gn.relay(item)
            if i == HA:
                load(4, layer).wait()
                scatter.run(0, lambda c: dot(m[ds(0, HS), :], wd[:, ds(c, HW)]))
            if i + 1 < len(ITEMS):
                gn.relay(ITEMS[i + 1])
            gn.arrived(item)
            gate_up(*item)
        refill(2)
        refill(3)
        scatter.run(1, lambda c: dot(m[ds(1, HS), :], wd[:, ds(c, HW)]))
        refill(4)
        leave(0)
        gn.finish()
        leave(1)

    loop(LAYERS, layer_step)


def backward_kernel(layer, hin, dy, *refs):
    first_call, last_call = layer == LAYERS - 1, layer == 0
    refs = list(refs)
    take = lambda k: [refs.pop(0) for _ in range(k)]
    gin = None if first_call else take(1)[0]
    ga, gm, wq_h, wo_h, wg_h, wu_h, wd_h = take(7)
    (dx,) = take(1)
    gouts = take(2 if last_call else 1)
    saved_h = take(9)
    u, dqkv, o, da, n, dg, du, m, dd = saved = take(9)
    wq, wo, wg, wu, wd = take(5)
    hm, acc1, acc3, qkv, probs, dgated, dh, part, near, out, far, gbuf = take(12)
    gmid, gfar = take(2)
    wsem, osem, gsend, grecv, ssend, srecv, rsend, rrecv = take(8)

    p = Peers()
    pairs = ((wq_h, wq), (wo_h, wo), (wg_h, wg), (wu_h, wu), (wd_h, wd))
    loads = [pltpu.make_async_copy(src.at[layer], dst, wsem.at[i]) for i, (src, dst) in enumerate(pairs)]
    saves = [pltpu.make_async_copy(src, dst, osem.at[i]) for i, (src, dst) in enumerate(zip(saved, saved_h))]
    for i in (0, 1, 4, 2, 3):
        loads[i].start()
    mine = ds(p.me, R)
    h = hin[layer - 1] if layer > 0 else hin[...]
    gain_a, gain_m = ga[pl.ds(layer, 1), :], gm[pl.ds(layer, 1), :]
    u[mine, :] = norm(h, gain_a)
    dd[mine, :] = dy[...]
    p.barrier()
    gu = Gather(p, u, gsend, grecv, 0)
    gd = Gather(p, dd, gsend, grecv, 1)
    gu.start()
    for c in range(AC):
        gd.to_sib(c)
    for c in range(AC // 2):
        gd.to_cross(c)

    loads[0].wait()
    gu.each(qkv_chunk(u, wq, acc1, qkv))
    saves[0].start()
    attention(qkv, o, probs)
    saves[2].start()
    loads[1].wait()
    scatter = Scatter(p, part, near, out, far, ssend, srecv)
    scatter.run(lambda c: dot(o[...], wo[:, ds(c, RW)]))
    for c in range(AC // 2, AC):
        gd.to_cross(c)
    for c in range(AC // 2):
        gd.relay(c)
    h_mid = h + scatter.result()
    hm[...] = h_mid
    n[mine, :] = norm(h_mid, gain_m)
    gn = Gather(p, n, gsend, grecv, 2)
    gn.start()

    for c in range(AC // 2, AC):
        gd.relay(c)
    for c in range(AC):
        gd.arrived(c)
    saves[8].start()
    loads[4].wait()

    def gated(j):
        dgated[:, ds(j, 512)] = dot_nt(dd[...], wd[ds(j, 512), :]).astype(BF16)

    loop(NF // 512, gated)
    loads[2].wait()
    loads[3].wait()

    def last(cols, z1, z3):
        sig = jax.nn.sigmoid(z1)
        silu = z1 * sig
        dm = dgated[:, cols].astype(F32)
        m[:, cols] = (silu * z3).astype(BF16)
        du[:, cols] = (dm * silu).astype(BF16)
        dg[:, cols] = (dm * z3 * (sig + silu * (1.0 - sig))).astype(BF16)

    gn.each(mlp_chunk(n, wg, wu, acc1, acc3, last))
    for i in (4, 5, 6, 7):
        saves[i].start()

    scatter.run(lambda c: dot_nt(dg[...], wg[ds(c, RW), :]) + dot_nt(du[...], wu[ds(c, RW), :]))
    d_norm, dgain_m = norm_back(hm[...], gain_m, scatter.result())
    d_mid = dy[...] + d_norm
    da[mine, :] = d_mid
    ga_ = Gather(p, da, gsend, grecv, 3)
    ga_.start()
    gbuf[...] = jnp.zeros_like(gbuf) if first_call else gin[...]
    gbuf[pl.ds(LAYERS + layer, 1), :] = dgain_m

    def heads_chunk(chunk):
        part_h = dot_nt(da[:, ds(chunk, AW)], wo[:, ds(chunk, AW)])
        if chunk > 0:
            part_h = part_h + acc1[:, :NO]
        if chunk < AC - 1:
            acc1[:, :NO] = part_h
        else:
            dh[...] = part_h.astype(BF16)

    ga_.each(heads_chunk)
    saves[3].start()

    def back(head):
        prob = probs[head]
        d_o = dh[:, ds(head, HEAD)]
        q, k, v = (qkv[:, head_cols(head, i)] for i in range(3))
        d_prob = dot_nt(d_o, v)
        d_scores = (prob * (d_prob - jnp.sum(d_prob * prob, axis=-1, keepdims=True)) * HEAD**-0.5).astype(BF16)
        dqkv[:, head_cols(head, 0)] = dot(d_scores, k).astype(BF16)
        dqkv[:, head_cols(head, 1)] = dot_tn(d_scores, q).astype(BF16)
        dqkv[:, head_cols(head, 2)] = dot_tn(prob.astype(BF16), d_o).astype(BF16)

    loop(HEADS, back)
    saves[1].start()
    scatter.run(lambda c: dot_nt(dqkv[...], wq[ds(c, RW), :]))
    d_norm, dgain_a = norm_back(h, gain_a, scatter.result())
    dx[...] = da[mine, :] + d_norm
    gbuf[pl.ds(layer, 1), :] = dgain_a

    if last_call:
        near_g = remote(gbuf, gmid, rsend.at[0], rrecv.at[0], p.sib)
        near_g.start()
        near_g.wait()
        gbuf[...] = gbuf[...] + gmid[...]
        far_g = remote(gbuf, gfar, rsend.at[1], rrecv.at[1], p.cross)
        far_g.start()
        far_g.wait()
        total = gbuf[...] + gfar[...]
        gouts[0][...] = total[:LAYERS]
        gouts[1][...] = total[LAYERS:2 * LAYERS]
    else:
        gouts[0][...] = gbuf[...]
    for g in (gu, gd, gn, ga_):
        g.finish()
    for save in saves:
        save.wait()


def wgrad_kernel(layer, n_alias, u_h, dqkv_h, o_h, da_h, n_h, dg_h, du_h, m_h, dd_h, *refs):
    refs = list(refs[n_alias:])
    take = lambda k: [refs.pop(0) for _ in range(k)]
    outs = take(5)
    u, dqkv, o, da, n, dg, du, m, dd = acts = take(9)
    stages = take(5)
    isem, osem = take(2)
    loads = [pltpu.make_async_copy(src, dst, isem.at[i])
             for i, (src, dst) in enumerate(zip((u_h, dqkv_h, o_h, da_h, n_h, dg_h, du_h, m_h, dd_h), acts))]
    work = ((2, 4, 5), (3, 4, 6), (4, 7, 8), (0, 0, 1), (1, 2, 3))
    started, waited, copies = set(), set(), []
    for number, (out_i, a_i, b_i) in enumerate(work):
        for _, *pair in work[: number + 2]:
            for i in pair:
                if i not in started:
                    loads[i].start()
                    started.add(i)
        for i in (a_i, b_i):
            if i not in waited:
                loads[i].wait()
                waited.add(i)
        a, b, out, stage = acts[a_i], acts[b_i], outs[out_i], stages[out_i]
        tiles, cols = a.shape[1] // S, b.shape[1]

        def copy(i):
            rows = ds(i, S)
            return pltpu.make_async_copy(stage.at[rows, :], out.at[layer, rows, :], osem.at[out_i, i])

        def step(i):
            lhs = a[:, ds(i, S)].T
            for c in range(cols // 512):
                stage[ds(i, S), ds(c, 512)] = dot(lhs, b[:, ds(c, 512)]).astype(BF16)
            copy(i).start()

        loop(tiles, step)
        copies += [copy(i) for i in range(tiles)]
    for each in copies:
        each.wait()


def vmem():
    return pl.BlockSpec(memory_space=pltpu.VMEM)


def hbm():
    return pl.BlockSpec(memory_space=pl.ANY)


WEIGHT_SCRATCH = [
    pltpu.VMEM((D, NQ), BF16),
    pltpu.VMEM((NO, D), BF16),
    pltpu.VMEM((D, NF), BF16),
    pltpu.VMEM((D, NF), BF16),
    pltpu.VMEM((NF, D), BF16),
]
SCATTER_SCRATCH = [
    pltpu.VMEM((S, D), F32),
    pltpu.VMEM((2, R, D), F32),
    pltpu.VMEM((R, D), BF16),
    pltpu.VMEM((R, D), BF16),
]
SAVED = [(S, D), (S, NQ), (S, NO), (S, D), (S, D), (S, NF), (S, NF), (S, NF), (S, D)]
GRADS = [(D, NQ), (NO, D), (D, NF), (D, NF), (NF, D)]


def run_forward(x, ga, gm, weights):
    dma = pltpu.SemaphoreType.DMA
    return pl.pallas_call(
        forward_kernel,
        name="forward",
        out_shape=[jax.ShapeDtypeStruct((LAYERS - 1, R, D), BF16), jax.ShapeDtypeStruct((R, D), BF16)],
        in_specs=[vmem()] * 3 + [hbm()] * 5,
        out_specs=[vmem()] * 2,
        scratch_shapes=WEIGHT_SCRATCH
        + [
            pltpu.VMEM((R, D), BF16),
            pltpu.VMEM((S, D), BF16),
            pltpu.VMEM((S, D), BF16),
            pltpu.VMEM((S, NF), F32),
            pltpu.VMEM((S, NF), F32),
            pltpu.VMEM((S, NQ), BF16),
            pltpu.VMEM((S, NO), BF16),
            pltpu.VMEM((S, NF), BF16),
        ]
        + SCATTER_SCRATCH
        + [dma((5,)), dma((2, 3, 2, HA)), dma((2, 3, 2, HA)), dma((3, 2, HC)), dma((3, 2, HC))],
        compiler_params=pltpu.CompilerParams(collective_id=0, has_side_effects=True, vmem_limit_bytes=VMEM_LIMIT),
    )(x, ga, gm, *weights)


def run_backward(layer, hin, dy, gin, ga, gm, weights):
    dma = pltpu.SemaphoreType.DMA
    last_call = layer == 0
    gshape = [jax.ShapeDtypeStruct((LAYERS, D), F32)] * 2 if last_call else [jax.ShapeDtypeStruct((8, D), F32)]
    saved = [jax.ShapeDtypeStruct(shape, BF16) for shape in SAVED]
    outs = pl.pallas_call(
        functools.partial(backward_kernel, layer),
        name=f"backward{layer}",
        out_shape=[jax.ShapeDtypeStruct((R, D), BF16)] + gshape + saved,
        in_specs=[vmem()] * (4 + len(gin)) + [hbm()] * 5,
        out_specs=[vmem()] * (1 + len(gshape)) + [hbm()] * 9,
        scratch_shapes=[pltpu.VMEM(shape, BF16) for shape in SAVED]
        + WEIGHT_SCRATCH
        + [
            pltpu.VMEM((R, D), BF16),
            pltpu.VMEM((S, NF), F32),
            pltpu.VMEM((S, NF), F32),
            pltpu.VMEM((S, NQ), BF16),
            pltpu.VMEM((HEADS, S, S), F32),
            pltpu.VMEM((S, NF), BF16),
            pltpu.VMEM((S, NO), BF16),
        ]
        + SCATTER_SCRATCH
        + [pltpu.VMEM((8, D), F32)] * 3
        + [dma((5,)), dma((9,)), dma((4, 3, AC)), dma((4, 3, AC)), dma((3, RC)), dma((3, RC)), dma((2,)), dma((2,))],
        compiler_params=pltpu.CompilerParams(
            collective_id=1 + layer, has_side_effects=True, vmem_limit_bytes=VMEM_LIMIT
        ),
    )(hin, dy, *gin, ga, gm, *weights)
    return outs[0], outs[1 : 1 + len(gshape)], outs[1 + len(gshape) :]


def run_wgrad(layer, saved, grads):
    dma = pltpu.SemaphoreType.DMA
    n_alias = len(grads)
    return pl.pallas_call(
        functools.partial(wgrad_kernel, layer, n_alias),
        name=f"wgrad{layer}",
        out_shape=[jax.ShapeDtypeStruct((LAYERS, *shape), BF16) for shape in GRADS],
        in_specs=[hbm()] * (9 + n_alias),
        out_specs=[hbm()] * 5,
        input_output_aliases={9 + i: i for i in range(n_alias)},
        scratch_shapes=[pltpu.VMEM(shape, BF16) for shape in SAVED]
        + [pltpu.VMEM(shape, BF16) for shape in GRADS]
        + [dma((9,)), dma((5, 8))],
        compiler_params=pltpu.CompilerParams(vmem_limit_bytes=VMEM_LIMIT),
        cost_estimate=pl.CostEstimate(flops=8_600_000_000, bytes_accessed=42_000_000, transcendentals=0),
    )(*saved, *grads)


def solution(mesh):
    row_spec = P(("dp", "tp"), None)
    col_spec = P(None, None, "tp")
    mid_spec = P(None, "tp", None)
    in_specs = (row_spec, row_spec, P(None, None), P(None, None), col_spec, mid_spec, col_spec, col_spec, mid_spec)
    out_specs = (
        row_spec, row_spec, P("dp", None, "tp"), P("dp", "tp", None), P("dp", None, "tp"), P("dp", None, "tp"),
        P("dp", "tp", None), P("dp", None), P("dp", None),
    )

    def device_step(x, grad_y, gain_attn, gain_mlp, w_qkv, w_out, w_gate, w_up, w_down):
        weights = (w_qkv, w_out, w_gate, w_up, w_down)
        hs, y = run_forward(x, gain_attn, gain_mlp, weights)
        d_hidden = grad_y
        gains = []
        grads = ()
        for layer in reversed(range(LAYERS)):
            d_hidden, gains, saved = run_backward(
                layer, hs if layer > 0 else x, d_hidden, gains, gain_attn, gain_mlp, weights
            )
            grads = run_wgrad(layer, saved, grads)
            if layer > 0:
                d_hidden, grads = lax.optimization_barrier((d_hidden, grads))
        return (y, d_hidden, *grads, *gains)

    return jax.shard_map(device_step, mesh=mesh, in_specs=in_specs, out_specs=out_specs, check_vma=False)
```

```python
import functools

import jax
import jax.numpy as jnp
from jax import lax
from jax.experimental import pallas as pl
from jax.experimental.pallas import tpu as pltpu
from jax.sharding import PartitionSpec as P

HEAD = 128
EPS = 1e-5
MESH = pl.DeviceIdType.MESH
F32 = jnp.float32
BF16 = jnp.bfloat16
VMEM_LIMIT = 66_000_000

D = 2048
S = 256
R = 64
NQ = 1536
NO = 512
NF = 2048
HEADS = 4
LAYERS = 3

AC = 4
AW = D // AC
RC = 4
RW = D // RC


def dot(a, b):
    return jnp.dot(a, b, preferred_element_type=F32)


def dot_nt(a, b):
    return lax.dot_general(a, b, (((1,), (1,)), ((), ())), preferred_element_type=F32)


def dot_tn(a, b):
    return lax.dot_general(a, b, (((0,), (0,)), ((), ())), preferred_element_type=F32)


def ds(i, n):
    return pl.ds(i * n if isinstance(i, int) else pl.multiple_of(i * n, n), n)


def loop(n, body):
    lax.fori_loop(0, n, lambda i, c: (body(i), c)[1], 0)


class Peers:
    def __init__(self):
        self.me = lax.axis_index("tp")
        core, chip = lax.rem(self.me, 2), self.me // 2
        self.sib = chip * 2 + (1 - core)
        self.cross = (1 - chip) * 2 + core
        self.diag = (1 - chip) * 2 + (1 - core)

    def barrier(self):
        sem = pltpu.get_barrier_semaphore()
        for peer in (self.sib, self.cross):
            pl.semaphore_signal(sem, inc=1, device_id={"tp": peer}, device_id_type=MESH)
        pl.semaphore_wait(sem, 2)


def remote(src, dst, send, recv, peer):
    return pltpu.make_async_remote_copy(
        src_ref=src, dst_ref=dst, send_sem=send, recv_sem=recv, device_id={"tp": peer}, device_id_type=MESH
    )


class Gather:
    def __init__(self, p, buf, send, recv, which, ac=AC):
        self.p, self.buf, self.send, self.recv, self.which, self.ac = p, buf, send, recv, which, ac

    def _copy(self, kind, chunk, owner, peer):
        part = self.buf.at[ds(owner, R), ds(chunk, D // self.ac)]
        return remote(part, part, self.send.at[self.which, kind, chunk], self.recv.at[self.which, kind, chunk], peer)

    def to_cross(self, chunk):
        self._copy(0, chunk, self.p.me, self.p.cross).start()

    def to_sib(self, chunk):
        self._copy(1, chunk, self.p.me, self.p.sib).start()

    def relay(self, chunk):
        self._copy(0, chunk, self.p.cross, self.p.cross).wait_recv()
        self._copy(2, chunk, self.p.cross, self.p.sib).start()

    def arrived(self, chunk):
        self._copy(1, chunk, self.p.sib, self.p.sib).wait_recv()
        self._copy(2, chunk, self.p.diag, self.p.sib).wait_recv()

    def start(self):
        for chunk in range(self.ac):
            self.to_cross(chunk)
        for chunk in range(self.ac):
            self.to_sib(chunk)

    def each(self, body):
        for chunk in range(self.ac + 1):
            if chunk < self.ac:
                self.relay(chunk)
            if chunk > 0:
                self.arrived(chunk - 1)
                body(chunk - 1)

    def finish(self):
        for chunk in range(self.ac):
            self._copy(0, chunk, self.p.me, self.p.cross).wait_send()
            self._copy(1, chunk, self.p.me, self.p.sib).wait_send()
            self._copy(2, chunk, self.p.cross, self.p.sib).wait_send()


class Scatter:
    def __init__(self, p, part, near, out, far, send, recv, rc=RC):
        self.rc = rc
        self.p, self.part, self.near, self.out, self.far, self.send, self.recv = p, part, near, out, far, send, recv

    def _near(self, kind, chunk):
        owner = self.p.diag if kind == 0 else self.p.sib
        return remote(
            self.part.at[ds(owner, R), ds(chunk, D // self.rc)],
            self.near.at[kind, :, ds(chunk, D // self.rc)],
            self.send.at[kind, chunk],
            self.recv.at[kind, chunk],
            self.p.sib,
        )

    def _far(self, chunk):
        return remote(
            self.out.at[:, ds(chunk, D // self.rc)],
            self.far.at[:, ds(chunk, D // self.rc)],
            self.send.at[2, chunk],
            self.recv.at[2, chunk],
            self.p.cross,
        )

    def _mid(self, chunk):
        self._near(0, chunk).wait_recv()
        cols = ds(chunk, D // self.rc)
        self.out[:, cols] = (self.part[ds(self.p.cross, R), cols] + self.near[0, :, cols]).astype(BF16)
        self._far(chunk).start()

    def run(self, compute):
        def step(chunk):
            self.part[:, ds(chunk, D // self.rc)] = compute(chunk)
            self._near(0, chunk).start()
            self._near(1, chunk).start()

            @pl.when(chunk > 0)
            def _():
                self._mid(chunk - 1)

        loop(self.rc, step)
        self._mid(self.rc - 1)

    def result(self):
        for chunk in range(self.rc):
            self._near(1, chunk).wait_recv()
            self._far(chunk).wait_recv()
        total = self.part[ds(self.p.me, R), :] + self.near[1] + self.far[...].astype(F32)
        for chunk in range(self.rc):
            self._near(0, chunk).wait_send()
            self._near(1, chunk).wait_send()
            self._far(chunk).wait_send()
        return total.astype(BF16)


HR = R // 2
HS = S // 2
HA = 1
HAW = D // HA
HC = 2
HW = D // HC


def owned(owner, half):
    return ds(half * 4 + owner, HR)


class HalfGather(Gather):
    def _copy(self, kind, item, owner, peer):
        half, chunk = item
        part = self.buf.at[owned(owner, half), ds(chunk, HAW)]
        sems = (self.which, kind, half, chunk)
        return remote(part, part, self.send.at[sems], self.recv.at[sems], peer)

    def start(self, half):
        for chunk in range(HA):
            self.to_cross((half, chunk))
        for chunk in range(HA):
            self.to_sib((half, chunk))

    def finish(self):
        for half in range(2):
            for chunk in range(HA):
                self._copy(0, (half, chunk), self.p.me, self.p.cross).wait_send()
                self._copy(1, (half, chunk), self.p.me, self.p.sib).wait_send()
                self._copy(2, (half, chunk), self.p.cross, self.p.sib).wait_send()


class HalfScatter(Scatter):
    def _near(self, kind, half, chunk):
        owner = self.p.diag if kind == 0 else self.p.sib
        return remote(
            self.part.at[owned(owner, half), ds(chunk, HW)],
            self.near.at[kind, ds(half, HR), ds(chunk, HW)],
            self.send.at[kind, half, chunk],
            self.recv.at[kind, half, chunk],
            self.p.sib,
        )

    def _far(self, half, chunk):
        return remote(
            self.out.at[ds(half, HR), ds(chunk, HW)],
            self.far.at[ds(half, HR), ds(chunk, HW)],
            self.send.at[2, half, chunk],
            self.recv.at[2, half, chunk],
            self.p.cross,
        )

    def run(self, half, compute):
        def step(chunk):
            self.part[ds(half, HS), ds(chunk, HW)] = compute(chunk)
            self._near(0, half, chunk).start()
            self._near(1, half, chunk).start()

        def mid(chunk):
            self._near(0, half, chunk).wait_recv()
            cols = ds(chunk, HW)
            total = self.part[owned(self.p.cross, half), cols] + self.near[0, ds(half, HR), cols]
            self.out[ds(half, HR), cols] = total.astype(BF16)
            self._far(half, chunk).start()

        loop(HC, step)
        loop(HC, mid)

    def result(self, half):
        for chunk in range(HC):
            self._near(1, half, chunk).wait_recv()
            self._far(half, chunk).wait_recv()
        rows = ds(half, HR)
        total = self.part[owned(self.p.me, half), :] + self.near[1, rows, :] + self.far[rows, :].astype(F32)
        for chunk in range(HC):
            self._near(0, half, chunk).wait_send()
            self._near(1, half, chunk).wait_send()
            self._far(half, chunk).wait_send()
        return total.astype(BF16)


def true_position(row):
    return lax.rem(row, HS) // HR * R + row // HS * HR + lax.rem(row, HR)


def norm(h, gain):
    hf = h.astype(F32)
    inv = lax.rsqrt(jnp.mean(hf * hf, axis=-1, keepdims=True) + EPS)
    return (hf * inv * gain).astype(BF16)


def norm_back(h, gain, dy):
    hf, dyf = h.astype(F32), dy.astype(F32)
    inv = lax.rsqrt(jnp.mean(hf * hf, axis=-1, keepdims=True) + EPS)
    dgain = jnp.sum(dyf * (hf * inv), axis=0, keepdims=True)
    dn = dyf * gain
    slope = jnp.sum(dn * hf, axis=-1, keepdims=True) * (inv * inv * inv) / D
    return (dn * inv - hf * slope).astype(BF16), dgain


def softmax_scores(q, k, halves=False):
    scores = dot_nt(q, k) * HEAD**-0.5
    rows = lax.broadcasted_iota(jnp.int32, (S, S), 0)
    cols = lax.broadcasted_iota(jnp.int32, (S, S), 1)
    if halves:
        rows, cols = true_position(rows), true_position(cols)
    scores = jnp.where(rows >= cols, scores, -1e30)
    e = jnp.exp(scores - jnp.max(scores, axis=-1, keepdims=True))
    return e / jnp.sum(e, axis=-1, keepdims=True)


def head_cols(head, which):
    return pl.ds(pl.multiple_of(head * 3 * HEAD + which * HEAD, HEAD), HEAD)


def attention(qkv, o, probs=None, halves=False):
    def one(head):
        prob = softmax_scores(qkv[:, head_cols(head, 0)], qkv[:, head_cols(head, 1)], halves)
        if probs is not None:
            probs[head] = prob
        o[:, ds(head, HEAD)] = dot(prob.astype(BF16), qkv[:, head_cols(head, 2)]).astype(BF16)

    loop(HEADS, one)


def qkv_chunk(u, wq, acc, qkv, tile=768, ac=AC):
    AC, AW = ac, D // ac

    def body(chunk):
        def one(j):
            cols = ds(j, tile)
            part = dot(u[:, ds(chunk, AW)], wq[ds(chunk, AW), cols])
            if chunk > 0:
                part = part + acc[:, cols]
            if chunk < AC - 1:
                acc[:, cols] = part
            else:
                qkv[:, cols] = part.astype(BF16)

        loop(NQ // tile, one)

    return body


def mlp_chunk(n, wg, wu, acc1, acc3, last, tile=512, ac=AC):
    AC, AW = ac, D // ac

    def body(chunk):
        def one(j):
            cols = ds(j, tile)
            z1 = dot(n[:, ds(chunk, AW)], wg[ds(chunk, AW), cols])
            z3 = dot(n[:, ds(chunk, AW)], wu[ds(chunk, AW), cols])
            if chunk > 0:
                z1, z3 = z1 + acc1[:, cols], z3 + acc3[:, cols]
            if chunk < AC - 1:
                acc1[:, cols] = z1
                acc3[:, cols] = z3
            else:
                last(cols, z1.astype(BF16).astype(F32), z3.astype(BF16).astype(F32))

        loop(NF // tile, one)

    return body


def half_qkv(u, wq, acc, qkv, tile=768):
    def body(half, chunk):
        rows, deep = ds(half, HS), ds(chunk, HAW)

        def one(j):
            cols = ds(j, tile)
            part = dot(u[rows, deep], wq[deep, cols])
            if chunk > 0:
                part = part + acc[rows, cols]
            if chunk < HA - 1:
                acc[rows, cols] = part
            else:
                qkv[rows, cols] = part.astype(BF16)

        loop(NQ // tile, one)

    return body


def half_mlp(n, wg, wu, acc1, acc3, last, tile=512):
    def body(half, chunk):
        rows, deep = ds(half, HS), ds(chunk, HAW)

        def one(j):
            cols = ds(j, tile)
            z1 = dot(n[rows, deep], wg[deep, cols])
            z3 = dot(n[rows, deep], wu[deep, cols])
            if chunk > 0:
                z1, z3 = z1 + acc1[rows, cols], z3 + acc3[rows, cols]
            if chunk < HA - 1:
                acc1[rows, cols] = z1
                acc3[rows, cols] = z3
            else:
                last(rows, cols, z1.astype(BF16).astype(F32), z3.astype(BF16).astype(F32))

        loop(NF // tile, one)

    return body


ITEMS = [(half, chunk) for half in range(2) for chunk in range(HA)]


def in_order(gather, body, between=None):
    for i, item in enumerate(ITEMS):
        gather.relay(item)
        if i == HA and between is not None:
            between()
        gather.arrived(item)
        body(*item)


def forward_kernel(x, ga, gm, wq_h, wo_h, wg_h, wu_h, wd_h, hs, y,
                   wq, wo, wg, wu, wd, h, u, n, acc1, acc3, qkv, o, m, part, near, out, far,
                   wsem, gsend, grecv, ssend, srecv):
    p = Peers()
    pairs = ((wq_h, wq), (wo_h, wo), (wg_h, wg), (wu_h, wu), (wd_h, wd))

    def load(i, layer):
        return pltpu.make_async_copy(pairs[i][0].at[layer], pairs[i][1], wsem.at[i])

    for i in range(5):
        load(i, 0).start()
    h[...] = x[...]
    p.barrier()
    gu = HalfGather(p, u, gsend, grecv, 0)
    gn = HalfGather(p, n, gsend, grecv, 1)
    scatter = HalfScatter(p, part, near, out, far, ssend, srecv)

    def enter(half, layer):
        u[owned(p.me, half), :] = norm(h[ds(half, HR), :], ga[pl.ds(layer, 1), :])
        gu.start(half)

    def add(half):
        rows = ds(half, HR)
        h[rows, :] = h[rows, :] + scatter.result(half)
        return h[rows, :]

    enter(0, 0)
    enter(1, 0)

    def layer_step(layer):
        more = layer < LAYERS - 1

        def refill(i):
            @pl.when(more)
            def _():
                load(i, layer + 1).start()

        load(0, layer).wait()
        in_order(gu, half_qkv(u, wq, acc1, qkv))
        refill(0)
        attention(qkv, o, halves=True)
        load(1, layer).wait()
        for half in range(2):
            scatter.run(half, lambda c: dot(o[ds(half, HS), :], wo[:, ds(c, HW)]))
        refill(1)
        gu.finish()
        for half in range(2):
            n[owned(p.me, half), :] = norm(add(half), gm[pl.ds(layer, 1), :])
            gn.start(half)

        def last(rows, cols, z1, z3):
            m[rows, cols] = (z1 * jax.nn.sigmoid(z1) * z3).astype(BF16)

        def leave(half):
            total = add(half)

            @pl.when(more)
            def _():
                hs[layer, ds(half, HR), :] = total
                enter(half, layer + 1)

            @pl.when(jnp.logical_not(more))
            def _():
                y[ds(half, HR), :] = total

        gate_up = half_mlp(n, wg, wu, acc1, acc3, last)
        for i in (2, 3):
            load(i, layer).wait()
        def down_a():
            load(4, layer).wait()
            scatter.run(0, lambda c: dot(m[ds(0, HS), :], wd[:, ds(c, HW)]))

        in_order(gn, gate_up, down_a)
        refill(2)
        refill(3)
        scatter.run(1, lambda c: dot(m[ds(1, HS), :], wd[:, ds(c, HW)]))
        refill(4)
        leave(0)
        gn.finish()
        leave(1)

    loop(LAYERS, layer_step)


def backward_kernel(layer, hin, dy, *refs):
    first_call, last_call = layer == LAYERS - 1, layer == 0
    refs = list(refs)
    take = lambda k: [refs.pop(0) for _ in range(k)]
    gin = None if first_call else take(1)[0]
    ga, gm, wq_h, wo_h, wg_h, wu_h, wd_h = take(7)
    (dx,) = take(1)
    gouts = take(2 if last_call else 1)
    saved_h = take(9)
    u, dqkv, o, da, n, dg, du, m, dd = saved = take(9)
    wq, wo, wg, wu, wd = take(5)
    hm, acc1, acc3, qkv, probs, dgated, dh, part, near, out, far, gbuf = take(12)
    gmid, gfar = take(2)
    wsem, osem, gsend, grecv, ssend, srecv, rsend, rrecv = take(8)

    ac, rc = {2: (4, 4), 1: (2, 4), 0: (4, 2)}[layer]
    p = Peers()
    pairs = ((wq_h, wq), (wo_h, wo), (wg_h, wg), (wu_h, wu), (wd_h, wd))
    loads = [pltpu.make_async_copy(src.at[layer], dst, wsem.at[i]) for i, (src, dst) in enumerate(pairs)]
    saves = [pltpu.make_async_copy(src, dst, osem.at[i]) for i, (src, dst) in enumerate(zip(saved, saved_h))]
    for i in (0, 1, 4, 2, 3):
        loads[i].start()
    mine = ds(p.me, R)
    h = hin[layer - 1] if layer > 0 else hin[...]
    gain_a, gain_m = ga[pl.ds(layer, 1), :], gm[pl.ds(layer, 1), :]
    u[mine, :] = norm(h, gain_a)
    dd[mine, :] = dy[...]
    p.barrier()
    gu = Gather(p, u, gsend, grecv, 0, ac)
    gd = Gather(p, dd, gsend, grecv, 1, ac)
    gu.start()
    for c in range(ac):
        gd.to_sib(c)
    for c in range(ac // 2):
        gd.to_cross(c)

    loads[0].wait()
    gu.each(qkv_chunk(u, wq, acc1, qkv, ac=ac))
    saves[0].start()
    attention(qkv, o, probs)
    saves[2].start()
    loads[1].wait()
    scatter = Scatter(p, part, near, out, far, ssend, srecv, rc)
    scatter.run(lambda c: dot(o[...], wo[:, ds(c, D // rc)]))
    for c in range(ac // 2, ac):
        gd.to_cross(c)
    for c in range(ac // 2):
        gd.relay(c)
    h_mid = h + scatter.result()
    hm[...] = h_mid
    n[mine, :] = norm(h_mid, gain_m)
    gn = Gather(p, n, gsend, grecv, 2, ac)
    gn.start()

    for c in range(ac // 2, ac):
        gd.relay(c)
    for c in range(ac):
        gd.arrived(c)
    saves[8].start()
    loads[4].wait()

    def gated(j):
        dgated[:, ds(j, 512)] = dot_nt(dd[...], wd[ds(j, 512), :]).astype(BF16)

    loop(NF // 512, gated)
    loads[2].wait()
    loads[3].wait()

    def last(cols, z1, z3):
        sig = jax.nn.sigmoid(z1)
        silu = z1 * sig
        dm = dgated[:, cols].astype(F32)
        m[:, cols] = (silu * z3).astype(BF16)
        du[:, cols] = (dm * silu).astype(BF16)
        dg[:, cols] = (dm * z3 * (sig + silu * (1.0 - sig))).astype(BF16)

    gn.each(mlp_chunk(n, wg, wu, acc1, acc3, last, ac=ac))
    for i in (4, 5, 6, 7):
        saves[i].start()

    scatter.run(lambda c: dot_nt(dg[...], wg[ds(c, D // rc), :]) + dot_nt(du[...], wu[ds(c, D // rc), :]))
    d_norm, dgain_m = norm_back(hm[...], gain_m, scatter.result())
    d_mid = dy[...] + d_norm
    da[mine, :] = d_mid
    ga_ = Gather(p, da, gsend, grecv, 3, ac)
    ga_.start()
    gbuf[...] = jnp.zeros_like(gbuf) if first_call else gin[...]
    gbuf[pl.ds(LAYERS + layer, 1), :] = dgain_m

    def heads_chunk(chunk):
        part_h = dot_nt(da[:, ds(chunk, D // ac)], wo[:, ds(chunk, D // ac)])
        if chunk > 0:
            part_h = part_h + acc1[:, :NO]
        if chunk < ac - 1:
            acc1[:, :NO] = part_h
        else:
            dh[...] = part_h.astype(BF16)

    ga_.each(heads_chunk)
    saves[3].start()

    def back(head):
        prob = probs[head]
        d_o = dh[:, ds(head, HEAD)]
        q, k, v = (qkv[:, head_cols(head, i)] for i in range(3))
        d_prob = dot_nt(d_o, v)
        d_scores = (prob * (d_prob - jnp.sum(d_prob * prob, axis=-1, keepdims=True)) * HEAD**-0.5).astype(BF16)
        dqkv[:, head_cols(head, 0)] = dot(d_scores, k).astype(BF16)
        dqkv[:, head_cols(head, 1)] = dot_tn(d_scores, q).astype(BF16)
        dqkv[:, head_cols(head, 2)] = dot_tn(prob.astype(BF16), d_o).astype(BF16)

    loop(HEADS, back)
    saves[1].start()
    scatter.run(lambda c: dot_nt(dqkv[...], wq[ds(c, D // rc), :]))
    d_norm, dgain_a = norm_back(h, gain_a, scatter.result())
    dx[...] = da[mine, :] + d_norm
    gbuf[pl.ds(layer, 1), :] = dgain_a

    if last_call:
        near_g = remote(gbuf, gmid, rsend.at[0], rrecv.at[0], p.sib)
        near_g.start()
        near_g.wait()
        gbuf[...] = gbuf[...] + gmid[...]
        far_g = remote(gbuf, gfar, rsend.at[1], rrecv.at[1], p.cross)
        far_g.start()
        far_g.wait()
        total = gbuf[...] + gfar[...]
        gouts[0][...] = total[:LAYERS]
        gouts[1][...] = total[LAYERS:2 * LAYERS]
    else:
        gouts[0][...] = gbuf[...]
    for g in (gu, gd, gn, ga_):
        g.finish()
    for save in saves:
        save.wait()


def wgrad_kernel(layer, n_alias, u_h, dqkv_h, o_h, da_h, n_h, dg_h, du_h, m_h, dd_h, *refs):
    refs = list(refs[n_alias:])
    take = lambda k: [refs.pop(0) for _ in range(k)]
    outs = take(5)
    u, dqkv, o, da, n, dg, du, m, dd = acts = take(9)
    stages = take(5)
    isem, osem = take(2)
    loads = [pltpu.make_async_copy(src, dst, isem.at[i])
             for i, (src, dst) in enumerate(zip((u_h, dqkv_h, o_h, da_h, n_h, dg_h, du_h, m_h, dd_h), acts))]
    work = ((2, 4, 5), (3, 4, 6), (4, 7, 8), (0, 0, 1), (1, 2, 3))
    started, waited, copies = set(), set(), []
    for number, (out_i, a_i, b_i) in enumerate(work):
        for _, *pair in work[: number + 2]:
            for i in pair:
                if i not in started:
                    loads[i].start()
                    started.add(i)
        for i in (a_i, b_i):
            if i not in waited:
                loads[i].wait()
                waited.add(i)
        a, b, out, stage = acts[a_i], acts[b_i], outs[out_i], stages[out_i]
        tiles, cols = a.shape[1] // S, b.shape[1]

        def copy(i):
            rows = ds(i, S)
            return pltpu.make_async_copy(stage.at[rows, :], out.at[layer, rows, :], osem.at[out_i, i])

        per = 2 if layer == 2 else 1

        def step(j):
            for i in [j * per + k for k in range(per)]:
                lhs = a[:, ds(i, S)].T
                for c in range(cols // 512):
                    stage[ds(i, S), ds(c, 512)] = dot(lhs, b[:, ds(c, 512)]).astype(BF16)
                if layer != 1:
                    copy(i).start()

        loop(tiles // per, step)
        if layer == 1:
            for i in range(tiles):
                copy(i).start()
        copies += [copy(i) for i in range(tiles)]
    for each in copies:
        each.wait()


def vmem():
    return pl.BlockSpec(memory_space=pltpu.VMEM)


def hbm():
    return pl.BlockSpec(memory_space=pl.ANY)


WEIGHT_SCRATCH = [
    pltpu.VMEM((D, NQ), BF16),
    pltpu.VMEM((NO, D), BF16),
    pltpu.VMEM((D, NF), BF16),
    pltpu.VMEM((D, NF), BF16),
    pltpu.VMEM((NF, D), BF16),
]
SCATTER_SCRATCH = [
    pltpu.VMEM((S, D), F32),
    pltpu.VMEM((2, R, D), F32),
    pltpu.VMEM((R, D), BF16),
    pltpu.VMEM((R, D), BF16),
]
SAVED = [(S, D), (S, NQ), (S, NO), (S, D), (S, D), (S, NF), (S, NF), (S, NF), (S, D)]
GRADS = [(D, NQ), (NO, D), (D, NF), (D, NF), (NF, D)]


def run_forward(x, ga, gm, weights):
    dma = pltpu.SemaphoreType.DMA
    return pl.pallas_call(
        forward_kernel,
        name="forward",
        out_shape=[jax.ShapeDtypeStruct((LAYERS - 1, R, D), BF16), jax.ShapeDtypeStruct((R, D), BF16)],
        in_specs=[vmem()] * 3 + [hbm()] * 5,
        out_specs=[vmem()] * 2,
        scratch_shapes=WEIGHT_SCRATCH
        + [
            pltpu.VMEM((R, D), BF16),
            pltpu.VMEM((S, D), BF16),
            pltpu.VMEM((S, D), BF16),
            pltpu.VMEM((S, NF), F32),
            pltpu.VMEM((S, NF), F32),
            pltpu.VMEM((S, NQ), BF16),
            pltpu.VMEM((S, NO), BF16),
            pltpu.VMEM((S, NF), BF16),
        ]
        + SCATTER_SCRATCH
        + [dma((5,)), dma((2, 3, 2, HA)), dma((2, 3, 2, HA)), dma((3, 2, HC)), dma((3, 2, HC))],
        compiler_params=pltpu.CompilerParams(collective_id=0, has_side_effects=True, vmem_limit_bytes=VMEM_LIMIT),
    )(x, ga, gm, *weights)


def run_backward(layer, hin, dy, gin, ga, gm, weights):
    dma = pltpu.SemaphoreType.DMA
    last_call = layer == 0
    gshape = [jax.ShapeDtypeStruct((LAYERS, D), F32)] * 2 if last_call else [jax.ShapeDtypeStruct((8, D), F32)]
    saved = [jax.ShapeDtypeStruct(shape, BF16) for shape in SAVED]
    outs = pl.pallas_call(
        functools.partial(backward_kernel, layer),
        name=f"backward{layer}",
        out_shape=[jax.ShapeDtypeStruct((R, D), BF16)] + gshape + saved,
        in_specs=[vmem()] * (4 + len(gin)) + [hbm()] * 5,
        out_specs=[vmem()] * (1 + len(gshape)) + [hbm()] * 9,
        scratch_shapes=[pltpu.VMEM(shape, BF16) for shape in SAVED]
        + WEIGHT_SCRATCH
        + [
            pltpu.VMEM((R, D), BF16),
            pltpu.VMEM((S, NF), F32),
            pltpu.VMEM((S, NF), F32),
            pltpu.VMEM((S, NQ), BF16),
            pltpu.VMEM((HEADS, S, S), F32),
            pltpu.VMEM((S, NF), BF16),
            pltpu.VMEM((S, NO), BF16),
        ]
        + SCATTER_SCRATCH
        + [pltpu.VMEM((8, D), F32)] * 3
        + [dma((5,)), dma((9,)), dma((4, 3, AC)), dma((4, 3, AC)), dma((3, RC)), dma((3, RC)), dma((2,)), dma((2,))],
        compiler_params=pltpu.CompilerParams(
            collective_id=1 + layer, has_side_effects=True, vmem_limit_bytes=VMEM_LIMIT
        ),
    )(hin, dy, *gin, ga, gm, *weights)
    return outs[0], outs[1 : 1 + len(gshape)], outs[1 + len(gshape) :]


def run_wgrad(layer, saved, grads):
    dma = pltpu.SemaphoreType.DMA
    n_alias = len(grads)
    return pl.pallas_call(
        functools.partial(wgrad_kernel, layer, n_alias),
        name=f"wgrad{layer}",
        out_shape=[jax.ShapeDtypeStruct((LAYERS, *shape), BF16) for shape in GRADS],
        in_specs=[hbm()] * (9 + n_alias),
        out_specs=[hbm()] * 5,
        input_output_aliases={9 + i: i for i in range(n_alias)},
        scratch_shapes=[pltpu.VMEM(shape, BF16) for shape in SAVED]
        + [pltpu.VMEM(shape, BF16) for shape in GRADS]
        + [dma((9,)), dma((5, 8))],
        compiler_params=pltpu.CompilerParams(vmem_limit_bytes=VMEM_LIMIT),
        cost_estimate=pl.CostEstimate(flops=8_600_000_000, bytes_accessed=42_000_000, transcendentals=0),
    )(*saved, *grads)


def solution(mesh):
    row_spec = P(("dp", "tp"), None)
    col_spec = P(None, None, "tp")
    mid_spec = P(None, "tp", None)
    in_specs = (row_spec, row_spec, P(None, None), P(None, None), col_spec, mid_spec, col_spec, col_spec, mid_spec)
    out_specs = (
        row_spec, row_spec, P("dp", None, "tp"), P("dp", "tp", None), P("dp", None, "tp"), P("dp", None, "tp"),
        P("dp", "tp", None), P("dp", None), P("dp", None),
    )

    def device_step(x, grad_y, gain_attn, gain_mlp, w_qkv, w_out, w_gate, w_up, w_down):
        weights = (w_qkv, w_out, w_gate, w_up, w_down)
        hs, y = run_forward(x, gain_attn, gain_mlp, weights)
        d_hidden = grad_y
        gains = []
        grads = ()
        for layer in reversed(range(LAYERS)):
            d_hidden, gains, saved = run_backward(
                layer, hs if layer > 0 else x, d_hidden, gains, gain_attn, gain_mlp, weights
            )
            grads = run_wgrad(layer, saved, grads)
            if layer > 0:
                d_hidden, grads = lax.optimization_barrier((d_hidden, grads))
        return (y, d_hidden, *grads, *gains)

    return jax.shard_map(device_step, mesh=mesh, in_specs=in_specs, out_specs=out_specs, check_vma=False)
```

```python
import functools

import jax
import jax.numpy as jnp
from jax import lax
from jax.experimental import pallas as pl
from jax.experimental.pallas import tpu as pltpu
from jax.sharding import PartitionSpec as P

HEAD = 128
EPS = 1e-5
MESH = pl.DeviceIdType.MESH
F32 = jnp.float32
BF16 = jnp.bfloat16
VMEM_LIMIT = 66_000_000

D = 2048
S = 256
R = 64
NQ = 1536
NO = 512
NF = 2048
HEADS = 4
LAYERS = 3

HR = R // 2
HS = S // 2


def dot(a, b):
    return jnp.dot(a, b, preferred_element_type=F32)


def dot_nt(a, b):
    return lax.dot_general(a, b, (((1,), (1,)), ((), ())), preferred_element_type=F32)


def dot_tn(a, b):
    return lax.dot_general(a, b, (((0,), (0,)), ((), ())), preferred_element_type=F32)


def ds(i, n):
    return pl.ds(i * n if isinstance(i, int) else pl.multiple_of(i * n, n), n)


def loop(n, body):
    lax.fori_loop(0, n, lambda i, c: (body(i), c)[1], 0)


class Peers:
    def __init__(self):
        self.me = lax.axis_index("tp")
        core, chip = lax.rem(self.me, 2), self.me // 2
        self.sib = chip * 2 + (1 - core)
        self.cross = (1 - chip) * 2 + core
        self.diag = (1 - chip) * 2 + (1 - core)

    def barrier(self):
        sem = pltpu.get_barrier_semaphore()
        for peer in (self.sib, self.cross):
            pl.semaphore_signal(sem, inc=1, device_id={"tp": peer}, device_id_type=MESH)
        pl.semaphore_wait(sem, 2)


def remote(src, dst, send, recv, peer):
    return pltpu.make_async_remote_copy(
        src_ref=src, dst_ref=dst, send_sem=send, recv_sem=recv, device_id={"tp": peer}, device_id_type=MESH
    )


def owned(owner, half):
    return ds(half * 4 + owner, HR)


def true_position(row):
    return lax.rem(row, HS) // HR * R + row // HS * HR + lax.rem(row, HR)


class Gather:
    def __init__(self, p, buf, send, recv, which):
        self.p, self.buf, self.send, self.recv, self.which = p, buf, send, recv, which

    def _copy(self, kind, half, owner, peer):
        part = self.buf.at[owned(owner, half), :]
        sems = (self.which, kind, half)
        return remote(part, part, self.send.at[sems], self.recv.at[sems], peer)

    def start(self, half):
        self._copy(0, half, self.p.me, self.p.cross).start()
        self._copy(1, half, self.p.me, self.p.sib).start()

    def relay(self, half):
        self._copy(0, half, self.p.cross, self.p.cross).wait_recv()
        self._copy(2, half, self.p.cross, self.p.sib).start()

    def arrived(self, half):
        self._copy(1, half, self.p.sib, self.p.sib).wait_recv()
        self._copy(2, half, self.p.diag, self.p.sib).wait_recv()

    def each(self, body):
        def one(half):
            self.relay(half)
            self.arrived(half)
            body(half)

        loop(2, one)

    def finish(self):
        def one(half):
            self._copy(0, half, self.p.me, self.p.cross).wait_send()
            self._copy(1, half, self.p.me, self.p.sib).wait_send()
            self._copy(2, half, self.p.cross, self.p.sib).wait_send()

        loop(2, one)


class Scatter:
    def __init__(self, p, part, near, out, far, send, recv, chunks):
        self.p, self.part, self.near, self.out, self.far, self.send, self.recv = p, part, near, out, far, send, recv
        self.chunks, self.width = chunks, D // chunks

    def _near(self, kind, half, chunk):
        owner = self.p.diag if kind == 0 else self.p.sib
        cols = ds(chunk, self.width)
        return remote(
            self.part.at[owned(owner, half), cols],
            self.near.at[kind, ds(half, HR), cols],
            self.send.at[kind, half, chunk],
            self.recv.at[kind, half, chunk],
            self.p.sib,
        )

    def _far(self, half, chunk):
        cols = ds(chunk, self.width)
        return remote(
            self.out.at[ds(half, HR), cols],
            self.far.at[ds(half, HR), cols],
            self.send.at[2, half, chunk],
            self.recv.at[2, half, chunk],
            self.p.cross,
        )

    def _mid(self, half, chunk):
        self._near(0, half, chunk).wait_recv()
        cols = ds(chunk, self.width)
        total = self.part[owned(self.p.cross, half), cols] + self.near[0, ds(half, HR), cols]
        self.out[ds(half, HR), cols] = total.astype(BF16)
        self._far(half, chunk).start()

    def run(self, half, compute):
        def step(chunk):
            cols = ds(chunk, self.width)
            self.part[ds(half, HS), cols] = compute(ds(half, HS), cols)
            self._near(0, half, chunk).start()
            self._near(1, half, chunk).start()

        loop(self.chunks, step)
        loop(self.chunks, lambda chunk: self._mid(half, chunk))

    def run_full(self, compute):
        def mids(chunk):
            self._mid(0, chunk)
            self._mid(1, chunk)

        def step(chunk):
            cols = ds(chunk, self.width)
            self.part[:, cols] = compute(cols)
            for kind in range(2):
                for half in range(2):
                    self._near(kind, half, chunk).start()

            @pl.when(chunk > 0)
            def _():
                mids(chunk - 1)

        loop(self.chunks, step)
        mids(self.chunks - 1)

    def result(self, half):
        def waits(chunk):
            self._near(1, half, chunk).wait_recv()
            self._far(half, chunk).wait_recv()

        def sent(chunk):
            self._near(0, half, chunk).wait_send()
            self._near(1, half, chunk).wait_send()
            self._far(half, chunk).wait_send()

        loop(self.chunks, waits)
        rows = ds(half, HR)
        total = self.part[owned(self.p.me, half), :] + self.near[1, rows, :] + self.far[rows, :].astype(F32)
        loop(self.chunks, sent)
        return total.astype(BF16)


def norm(h, gain):
    hf = h.astype(F32)
    inv = lax.rsqrt(jnp.mean(hf * hf, axis=-1, keepdims=True) + EPS)
    return (hf * inv * gain).astype(BF16)


def norm_back(h, gain, dy):
    hf, dyf = h.astype(F32), dy.astype(F32)
    inv = lax.rsqrt(jnp.mean(hf * hf, axis=-1, keepdims=True) + EPS)
    dgain = jnp.sum(dyf * (hf * inv), axis=0, keepdims=True)
    dn = dyf * gain
    slope = jnp.sum(dn * hf, axis=-1, keepdims=True) * (inv * inv * inv) / D
    return (dn * inv - hf * slope).astype(BF16), dgain


def softmax_scores(q, k):
    scores = dot_nt(q, k) * HEAD**-0.5
    rows = true_position(lax.broadcasted_iota(jnp.int32, (S, 1), 0))
    cols = true_position(lax.broadcasted_iota(jnp.int32, (1, S), 1))
    scores = jnp.where(rows >= cols, scores, -1e30)
    e = jnp.exp(scores - jnp.max(scores, axis=-1, keepdims=True))
    return e / jnp.sum(e, axis=-1, keepdims=True)


def head_cols(head, which):
    return ds(head * 3 + which, HEAD)


def per_head(one, together):
    def step(j):
        for i in range(together):
            one(j * together + i)

    loop(HEADS // together, step)


def attention(qkv, o, together, probs=None):
    def one(head):
        prob = softmax_scores(qkv[:, head_cols(head, 0)], qkv[:, head_cols(head, 1)])
        if probs is not None:
            probs[head] = prob
        o[:, ds(head, HEAD)] = dot(prob.astype(BF16), qkv[:, head_cols(head, 2)]).astype(BF16)

    per_head(one, together)


def half_qkv(u, wq, qkv):
    def body(half):
        rows = ds(half, HS)
        for j in range(NQ // 512):
            qkv[rows, ds(j, 512)] = dot(u[rows, :], wq[:, ds(j, 512)]).astype(BF16)

    return body


def half_mlp(n, wg, wu, last, tile):
    def body(half):
        rows = ds(half, HS)

        def one(j):
            for k in range(tile // 512):
                cols = ds(j * (tile // 512) + k, 512)
                z1 = dot(n[rows, :], wg[:, cols]).astype(BF16).astype(F32)
                z3 = dot(n[rows, :], wu[:, cols]).astype(BF16).astype(F32)
                last(rows, cols, z1, z3)

        loop(NF // tile, one)

    return body


def forward_kernel(x, ga, gm, wq_h, wo_h, wg_h, wu_h, wd_h, hs, y,
                   wq, wo, wg, wu, wd, h, u, n, qkv, o, m, part, near, out, far,
                   wsem, gsend, grecv, ssend, srecv):
    p = Peers()
    pairs = ((wq_h, wq), (wo_h, wo), (wg_h, wg), (wu_h, wu), (wd_h, wd))

    def load(i, layer):
        return pltpu.make_async_copy(pairs[i][0].at[layer], pairs[i][1], wsem.at[i])

    for i in range(5):
        load(i, 0).start()
    h[...] = x[...]
    p.barrier()
    gu = Gather(p, u, gsend, grecv, 0)
    gn = Gather(p, n, gsend, grecv, 1)
    scatter = Scatter(p, part, near, out, far, ssend, srecv, 2)

    def enter(half, layer):
        u[owned(p.me, half), :] = norm(h[ds(half, HR), :], ga[pl.ds(layer, 1), :])
        gu.start(half)

    def add(half):
        rows = ds(half, HR)
        total = h[rows, :] + scatter.result(half)
        h[rows, :] = total
        return total

    loop(2, lambda half: enter(half, 0))

    def layer_step(layer):
        more = layer < LAYERS - 1

        def refill(i):
            @pl.when(more)
            def _():
                load(i, layer + 1).start()

        load(0, layer).wait()
        gu.each(half_qkv(u, wq, qkv))
        refill(0)
        attention(qkv, o, 4)
        load(1, layer).wait()
        loop(2, lambda half: scatter.run(half, lambda rows, cols: dot(o[rows, :], wo[:, cols])))
        refill(1)
        gu.finish()

        def between(half):
            n[owned(p.me, half), :] = norm(add(half), gm[pl.ds(layer, 1), :])
            gn.start(half)

        loop(2, between)

        def last(rows, cols, z1, z3):
            m[rows, cols] = (z1 * jax.nn.sigmoid(z1) * z3).astype(BF16)

        gate_up = half_mlp(n, wg, wu, last, 1024)
        for i in (2, 3, 4):
            load(i, layer).wait()
        gn.relay(0)

        def mlp(half):
            gn.arrived(half)
            gate_up(half)

            @pl.when(half == 0)
            def _():
                gn.relay(1)

            scatter.run(half, lambda rows, cols: dot(m[rows, :], wd[:, cols]))

        loop(2, mlp)
        refill(2)
        refill(3)
        refill(4)
        gn.finish()

        def leave(half):
            total = add(half)

            @pl.when(more)
            def _():
                hs[layer, ds(half, HR), :] = total
                enter(half, layer + 1)

            @pl.when(jnp.logical_not(more))
            def _():
                y[ds(half, HR), :] = total

        loop(2, leave)

    loop(LAYERS, layer_step)


def backward_kernel(layer, hin, dy, *refs):
    first_call, last_call = layer == LAYERS - 1, layer == 0
    refs = list(refs)
    take = lambda k: [refs.pop(0) for _ in range(k)]
    gin = None if first_call else take(1)[0]
    ga, gm, wq_h, wo_h, wg_h, wu_h, wd_h = take(7)
    (dx,) = take(1)
    gouts = take(2 if last_call else 1)
    saved_h = take(9)
    u, dqkv, o, da, n, dg, du, m, dd = saved = take(9)
    wq, wo, wg, wu, wd = take(5)
    hm, qkv, probs, dgated, dh, part, near, out, far, gbuf, gmid, gfar = take(12)
    wsem, osem, gsend, grecv, ssend, srecv, rsend, rrecv = take(8)

    p = Peers()
    pairs = ((wq_h, wq), (wo_h, wo), (wg_h, wg), (wu_h, wu), (wd_h, wd))
    loads = [pltpu.make_async_copy(src.at[layer], dst, wsem.at[i]) for i, (src, dst) in enumerate(pairs)]
    saves = [pltpu.make_async_copy(src, dst, osem.at[i]) for i, (src, dst) in enumerate(zip(saved, saved_h))]
    for i in (0, 1, 4, 2, 3):
        loads[i].start()
    h = hin.at[layer - 1] if layer > 0 else hin
    gain_a, gain_m = ga[pl.ds(layer, 1), :], gm[pl.ds(layer, 1), :]
    gu, gd, gn, gda = (Gather(p, buf, gsend, grecv, i) for i, buf in enumerate((u, dd, n, da)))
    two = Scatter(p, part, near, out, far, ssend, srecv, 2)
    four = Scatter(p, part, near, out, far, ssend, srecv, 4)
    p.barrier()

    def enter(half):
        u[owned(p.me, half), :] = norm(h[ds(half, HR), :], gain_a)
        gu.start(half)

    def enter_d(half):
        dd[owned(p.me, half), :] = dy[ds(half, HR), :]
        gd.start(half)

    loop(2, enter)
    loop(2, enter_d)
    gbuf[...] = jnp.zeros_like(gbuf) if first_call else gin[...]

    loads[0].wait()
    gu.each(half_qkv(u, wq, qkv))
    saves[0].start()
    attention(qkv, o, 2, probs)
    saves[2].start()
    loads[1].wait()
    loop(2, lambda half: two.run(half, lambda rows, cols: dot(o[rows, :], wo[:, cols])))

    loop(2, gd.relay)
    loop(2, gd.arrived)
    saves[8].start()
    loads[4].wait()

    def gated(j):
        dgated[:, ds(j, 512)] = dot_nt(dd[...], wd[ds(j, 512), :]).astype(BF16)

    loop(NF // 512, gated)

    def between(half):
        rows = ds(half, HR)
        h_mid = h[rows, :] + two.result(half)
        hm[rows, :] = h_mid
        n[owned(p.me, half), :] = norm(h_mid, gain_m)
        gn.start(half)

    loop(2, between)
    loads[2].wait()
    loads[3].wait()

    def last(rows, cols, z1, z3):
        sig = jax.nn.sigmoid(z1)
        silu = z1 * sig
        dm = dgated[rows, cols].astype(F32)
        m[rows, cols] = (silu * z3).astype(BF16)
        du[rows, cols] = (dm * silu).astype(BF16)
        dg[rows, cols] = (dm * z3 * (sig + silu * (1.0 - sig))).astype(BF16)

    gn.each(half_mlp(n, wg, wu, last, 512))
    for i in (4, 5, 6, 7):
        saves[i].start()

    four.run_full(lambda cols: dot_nt(dg[...], wg[cols, :]) + dot_nt(du[...], wu[cols, :]))

    def mid_back(half):
        rows = ds(half, HR)
        d_norm, dgain = norm_back(hm[rows, :], gain_m, four.result(half))
        da[owned(p.me, half), :] = dy[rows, :] + d_norm
        gda.start(half)
        row = pl.ds(LAYERS + layer, 1)
        gbuf[row, :] = gbuf[row, :] + dgain

    loop(2, mid_back)

    def heads(half):
        rows = ds(half, HS)
        dh[rows, :] = dot_nt(da[rows, :], wo[...]).astype(BF16)

    gda.each(heads)
    saves[3].start()

    def back(head):
        prob = probs[head]
        d_o = dh[:, ds(head, HEAD)]
        q, k, v = (qkv[:, head_cols(head, i)] for i in range(3))
        d_prob = dot_nt(d_o, v)
        d_scores = (prob * (d_prob - jnp.sum(d_prob * prob, axis=-1, keepdims=True)) * HEAD**-0.5).astype(BF16)
        dqkv[:, head_cols(head, 0)] = dot(d_scores, k).astype(BF16)
        dqkv[:, head_cols(head, 1)] = dot_tn(d_scores, q).astype(BF16)
        dqkv[:, head_cols(head, 2)] = dot_tn(prob.astype(BF16), d_o).astype(BF16)

    per_head(back, 2)
    saves[1].start()
    four.run_full(lambda cols: dot_nt(dqkv[...], wq[cols, :]))

    def leave(half):
        rows = ds(half, HR)
        d_norm, dgain = norm_back(h[rows, :], gain_a, four.result(half))
        dx[rows, :] = da[owned(p.me, half), :] + d_norm
        row = pl.ds(layer, 1)
        gbuf[row, :] = gbuf[row, :] + dgain

    loop(2, leave)

    if last_call:
        near_g = remote(gbuf, gmid, rsend.at[0], rrecv.at[0], p.sib)
        near_g.start()
        near_g.wait()
        gbuf[...] = gbuf[...] + gmid[...]
        far_g = remote(gbuf, gfar, rsend.at[1], rrecv.at[1], p.cross)
        far_g.start()
        far_g.wait()
        total = gbuf[...] + gfar[...]
        gouts[0][...] = total[:LAYERS]
        gouts[1][...] = total[LAYERS:2 * LAYERS]
    else:
        gouts[0][...] = gbuf[...]
    for g in (gu, gd, gn, gda):
        g.finish()
    for save in saves:
        save.wait()


def wgrad_kernel(layer, n_alias, u_h, dqkv_h, o_h, da_h, n_h, dg_h, du_h, m_h, dd_h, *refs):
    refs = list(refs[n_alias:])
    take = lambda k: [refs.pop(0) for _ in range(k)]
    gqkv_h, gout_h, ggate_h, gup_h, gdown_h = take(5)
    u, dqkv, o, da, lhs, rhs, gqkv, gout, gmlp = take(9)
    isem, osem = take(2)
    sources = (n_h, dg_h, du_h, m_h, dd_h, u_h, dqkv_h, o_h, da_h)
    targets = (lhs.at[0], rhs.at[0], rhs.at[1], lhs.at[1], rhs.at[2], u, dqkv, o, da)
    loads = [pltpu.make_async_copy(src, dst, isem.at[i]) for i, (src, dst) in enumerate(zip(sources, targets))]
    for load in loads:
        load.start()

    def tiles(a, b, stage, first, count):
        for i in [first + k for k in range(count)]:
            left = a[:, ds(i, S)].T
            for c in range(b.shape[1] // 512):
                stage[ds(i, S), ds(c, 512)] = dot(left, b[:, ds(c, 512)]).astype(BF16)

    def copy(stage, out, i, sem):
        return pltpu.make_async_copy(stage.at[ds(i, 2 * S), :], out.at[layer, ds(i, 2 * S), :], sem)

    mlp_outs = (ggate_h, gup_h, gdown_h)
    loads[0].wait()
    loads[1].wait()

    def mlp(step):
        which, i = step // 4, lax.rem(step, 4)

        @pl.when(step == 4)
        def _():
            loads[2].wait()

        @pl.when(step == 8)
        def _():
            loads[3].wait()
            loads[4].wait()

        stage = gmlp.at[which]
        tiles(lhs.at[which // 2], rhs.at[which], stage, i * 2, 2)
        for k, out in enumerate(mlp_outs):
            @pl.when(which == k)
            def _():
                copy(stage, out, i, osem.at[k, i]).start()

    loop(12, mlp)
    for load in loads[5:]:
        load.wait()

    def qkv(i):
        tiles(u, dqkv, gqkv, i * 2, 2)
        copy(gqkv, gqkv_h, i, osem.at[3, i]).start()

    loop(4, qkv)
    tiles(o, da, gout, 0, 2)
    copy(gout, gout_h, 0, osem.at[4, 0]).start()
    for i in range(4):
        for k, out in enumerate(mlp_outs):
            copy(gmlp.at[k], out, i, osem.at[k, i]).wait()
        copy(gqkv, gqkv_h, i, osem.at[3, i]).wait()
    copy(gout, gout_h, 0, osem.at[4, 0]).wait()


def vmem():
    return pl.BlockSpec(memory_space=pltpu.VMEM)


def hbm():
    return pl.BlockSpec(memory_space=pl.ANY)


WEIGHT_SCRATCH = [
    pltpu.VMEM((D, NQ), BF16),
    pltpu.VMEM((NO, D), BF16),
    pltpu.VMEM((D, NF), BF16),
    pltpu.VMEM((D, NF), BF16),
    pltpu.VMEM((NF, D), BF16),
]
SCATTER_SCRATCH = [
    pltpu.VMEM((S, D), F32),
    pltpu.VMEM((2, R, D), F32),
    pltpu.VMEM((R, D), BF16),
    pltpu.VMEM((R, D), BF16),
]
SAVED = [(S, D), (S, NQ), (S, NO), (S, D), (S, D), (S, NF), (S, NF), (S, NF), (S, D)]
GRADS = [(D, NQ), (NO, D), (D, NF), (D, NF), (NF, D)]


def run_forward(x, ga, gm, weights):
    dma = pltpu.SemaphoreType.DMA
    return pl.pallas_call(
        forward_kernel,
        name="forward",
        out_shape=[jax.ShapeDtypeStruct((LAYERS - 1, R, D), BF16), jax.ShapeDtypeStruct((R, D), BF16)],
        in_specs=[vmem()] * 3 + [hbm()] * 5,
        out_specs=[vmem()] * 2,
        scratch_shapes=WEIGHT_SCRATCH
        + [
            pltpu.VMEM((R, D), BF16),
            pltpu.VMEM((S, D), BF16),
            pltpu.VMEM((S, D), BF16),
            pltpu.VMEM((S, NQ), BF16),
            pltpu.VMEM((S, NO), BF16),
            pltpu.VMEM((S, NF), BF16),
        ]
        + SCATTER_SCRATCH
        + [dma((5,)), dma((2, 3, 2)), dma((2, 3, 2)), dma((3, 2, 2)), dma((3, 2, 2))],
        compiler_params=pltpu.CompilerParams(collective_id=0, has_side_effects=True, vmem_limit_bytes=VMEM_LIMIT),
    )(x, ga, gm, *weights)


def run_backward(layer, hin, dy, gin, ga, gm, weights):
    dma = pltpu.SemaphoreType.DMA
    last_call = layer == 0
    gshape = [jax.ShapeDtypeStruct((LAYERS, D), F32)] * 2 if last_call else [jax.ShapeDtypeStruct((8, D), F32)]
    saved = [jax.ShapeDtypeStruct(shape, BF16) for shape in SAVED]
    outs = pl.pallas_call(
        functools.partial(backward_kernel, layer),
        name=f"backward{layer}",
        out_shape=[jax.ShapeDtypeStruct((R, D), BF16)] + gshape + saved,
        in_specs=[vmem()] * (4 + len(gin)) + [hbm()] * 5,
        out_specs=[vmem()] * (1 + len(gshape)) + [hbm()] * 9,
        scratch_shapes=[pltpu.VMEM(shape, BF16) for shape in SAVED]
        + WEIGHT_SCRATCH
        + [
            pltpu.VMEM((R, D), BF16),
            pltpu.VMEM((S, NQ), BF16),
            pltpu.VMEM((HEADS, S, S), F32),
            pltpu.VMEM((S, NF), BF16),
            pltpu.VMEM((S, NO), BF16),
        ]
        + SCATTER_SCRATCH
        + [pltpu.VMEM((8, D), F32)] * 3
        + [dma((5,)), dma((9,)), dma((4, 3, 2)), dma((4, 3, 2)), dma((3, 2, 4)), dma((3, 2, 4)), dma((2,)), dma((2,))],
        compiler_params=pltpu.CompilerParams(
            collective_id=1 + layer, has_side_effects=True, vmem_limit_bytes=VMEM_LIMIT
        ),
    )(hin, dy, *gin, ga, gm, *weights)
    return outs[0], outs[1 : 1 + len(gshape)], outs[1 + len(gshape) :]


def run_wgrad(layer, saved, grads):
    dma = pltpu.SemaphoreType.DMA
    n_alias = len(grads)
    return pl.pallas_call(
        functools.partial(wgrad_kernel, layer, n_alias),
        name=f"wgrad{layer}",
        out_shape=[jax.ShapeDtypeStruct((LAYERS, *shape), BF16) for shape in GRADS],
        in_specs=[hbm()] * (9 + n_alias),
        out_specs=[hbm()] * 5,
        input_output_aliases={9 + i: i for i in range(n_alias)},
        scratch_shapes=[pltpu.VMEM(shape, BF16) for shape in SAVED[:4]]
        + [pltpu.VMEM(shape, BF16) for shape in ((2, S, D), (3, S, D), GRADS[0], GRADS[1], (3, D, D))]
        + [dma((9,)), dma((5, 4))],
        compiler_params=pltpu.CompilerParams(vmem_limit_bytes=VMEM_LIMIT),
        cost_estimate=pl.CostEstimate(flops=8_600_000_000, bytes_accessed=42_000_000, transcendentals=0),
    )(*saved, *grads)


def solution(mesh):
    row_spec = P(("dp", "tp"), None)
    col_spec = P(None, None, "tp")
    mid_spec = P(None, "tp", None)
    in_specs = (row_spec, row_spec, P(None, None), P(None, None), col_spec, mid_spec, col_spec, col_spec, mid_spec)
    out_specs = (
        row_spec, row_spec, P("dp", None, "tp"), P("dp", "tp", None), P("dp", None, "tp"), P("dp", None, "tp"),
        P("dp", "tp", None), P("dp", None), P("dp", None),
    )

    def device_step(x, grad_y, gain_attn, gain_mlp, w_qkv, w_out, w_gate, w_up, w_down):
        weights = (w_qkv, w_out, w_gate, w_up, w_down)
        hs, y = run_forward(x, gain_attn, gain_mlp, weights)
        d_hidden = grad_y
        gains = []
        grads = ()
        for layer in reversed(range(LAYERS)):
            d_hidden, gains, saved = run_backward(
                layer, hs if layer > 0 else x, d_hidden, gains, gain_attn, gain_mlp, weights
            )
            grads = run_wgrad(layer, saved, grads)
            if layer > 0:
                d_hidden, grads = lax.optimization_barrier((d_hidden, grads))
        return (y, d_hidden, *grads, *gains)

    return jax.shard_map(device_step, mesh=mesh, in_specs=in_specs, out_specs=out_specs, check_vma=False)
```

```python
import functools

import jax
import jax.numpy as jnp
from jax import lax
from jax.experimental import pallas as pl
from jax.experimental.pallas import tpu as pltpu
from jax.sharding import PartitionSpec as P

HEAD = 128
EPS = 1e-5
MESH = pl.DeviceIdType.MESH
F32 = jnp.float32
BF16 = jnp.bfloat16
VMEM_LIMIT = 67_000_000

D = 2048
S = 256
R = 64
NQ = 1536
NO = 512
NF = 2048
HEADS = 4
LAYERS = 3

HR = R // 2
HS = S // 2


def dot(a, b):
    return jnp.dot(a, b, preferred_element_type=F32)


def dot_nt(a, b):
    return lax.dot_general(a, b, (((1,), (1,)), ((), ())), preferred_element_type=F32)


def dot_tn(a, b):
    return lax.dot_general(a, b, (((0,), (0,)), ((), ())), preferred_element_type=F32)


def ds(i, n):
    return pl.ds(i * n if isinstance(i, int) else pl.multiple_of(i * n, n), n)


def loop(n, body):
    lax.fori_loop(0, n, lambda i, c: (body(i), c)[1], 0)


class Peers:
    def __init__(self):
        self.me = lax.axis_index("tp")
        core, chip = lax.rem(self.me, 2), self.me // 2
        self.sib = chip * 2 + (1 - core)
        self.cross = (1 - chip) * 2 + core
        self.diag = (1 - chip) * 2 + (1 - core)

    def barrier(self, *more):
        sem = pltpu.get_barrier_semaphore()
        for peer in (self.sib, self.cross, *more):
            pl.semaphore_signal(sem, inc=1, device_id={"tp": peer}, device_id_type=MESH)
        pl.semaphore_wait(sem, 2 + len(more))


def remote(src, dst, send, recv, peer):
    return pltpu.make_async_remote_copy(
        src_ref=src, dst_ref=dst, send_sem=send, recv_sem=recv, device_id={"tp": peer}, device_id_type=MESH
    )


def owned(owner, half):
    return ds(half * 4 + owner, HR)


def true_position(row):
    return lax.rem(row, HS) // HR * R + row // HS * HR + lax.rem(row, HR)


class Gather:
    def __init__(self, p, buf, send, recv, which):
        self.p, self.buf, self.send, self.recv, self.which = p, buf, send, recv, which

    def _copy(self, kind, half, owner, peer):
        part = self.buf.at[owned(owner, half), :]
        sems = (self.which, kind, half)
        return remote(part, part, self.send.at[sems], self.recv.at[sems], peer)

    def start(self, half):
        self._copy(0, half, self.p.me, self.p.cross).start()
        self._copy(1, half, self.p.me, self.p.sib).start()

    def relay(self, half):
        self._copy(0, half, self.p.cross, self.p.cross).wait_recv()
        self._copy(2, half, self.p.cross, self.p.sib).start()

    def arrived(self, half):
        self._copy(1, half, self.p.sib, self.p.sib).wait_recv()
        self._copy(2, half, self.p.diag, self.p.sib).wait_recv()

    def each(self, body):
        def one(half):
            self.relay(half)
            self.arrived(half)
            body(half)

        loop(2, one)

    def finish(self):
        def one(half):
            self._copy(0, half, self.p.me, self.p.cross).wait_send()
            self._copy(1, half, self.p.me, self.p.sib).wait_send()
            self._copy(2, half, self.p.cross, self.p.sib).wait_send()

        loop(2, one)


class Scatter:
    def __init__(self, p, part, near, out, far, send, recv, chunks):
        self.p, self.part, self.near, self.out, self.far, self.send, self.recv = p, part, near, out, far, send, recv
        self.chunks, self.width = chunks, D // chunks

    def _near(self, kind, half, chunk):
        owner = self.p.diag if kind == 0 else self.p.sib
        cols = ds(chunk, self.width)
        return remote(
            self.part.at[owned(owner, half), cols],
            self.near.at[kind, ds(half, HR), cols],
            self.send.at[kind, half, chunk],
            self.recv.at[kind, half, chunk],
            self.p.sib,
        )

    def _far(self, half, chunk):
        cols = ds(chunk, self.width)
        return remote(
            self.out.at[ds(half, HR), cols],
            self.far.at[ds(half, HR), cols],
            self.send.at[2, half, chunk],
            self.recv.at[2, half, chunk],
            self.p.cross,
        )

    def _mid(self, half, chunk, send=True):
        self._near(0, half, chunk).wait_recv()
        cols = ds(chunk, self.width)
        total = self.part[owned(self.p.cross, half), cols] + self.near[0, ds(half, HR), cols]
        self.out[ds(half, HR), cols] = total.astype(BF16)
        if send:
            self._far(half, chunk).start()

    def mids(self, half):
        loop(self.chunks, lambda chunk: self._mid(half, chunk))

    def run(self, half, compute):
        def step(chunk):
            cols = ds(chunk, self.width)
            self.part[ds(half, HS), cols] = compute(ds(half, HS), cols)
            self._near(0, half, chunk).start()
            self._near(1, half, chunk).start()

        loop(self.chunks, step)

    def run_full(self, compute, send=True):
        def mids(chunk):
            self._mid(0, chunk, send)
            self._mid(1, chunk, send)

        def step(chunk):
            cols = ds(chunk, self.width)
            self.part[:, cols] = compute(cols)
            for kind in range(2):
                for half in range(2):
                    self._near(kind, half, chunk).start()

            @pl.when(chunk > 0)
            def _():
                mids(chunk - 1)

        loop(self.chunks, step)
        mids(self.chunks - 1)

    def result(self, half):
        def waits(chunk):
            self._near(1, half, chunk).wait_recv()
            self._far(half, chunk).wait_recv()

        def sent(chunk):
            self._near(0, half, chunk).wait_send()
            self._near(1, half, chunk).wait_send()
            self._far(half, chunk).wait_send()

        loop(self.chunks, waits)
        rows = ds(half, HR)
        total = self.part[owned(self.p.me, half), :] + self.near[1, rows, :] + self.far[rows, :].astype(F32)
        loop(self.chunks, sent)
        return total.astype(BF16)


    def own_sum(self, own):
        for half in range(2):
            for chunk in range(self.chunks):
                self._near(1, half, chunk).wait_recv()
            own[ds(half, HR), :] = self.part[owned(self.p.me, half), :] + self.near[1, ds(half, HR), :]
        for half in range(2):
            for chunk in range(self.chunks):
                for kind in range(2):
                    self._near(kind, half, chunk).wait_send()


def norm(h, gain):
    hf = h.astype(F32)
    inv = lax.rsqrt(jnp.mean(hf * hf, axis=-1, keepdims=True) + EPS)
    return (hf * inv * gain).astype(BF16)


def norm_back(h, gain, dy):
    hf, dyf = h.astype(F32), dy.astype(F32)
    inv = lax.rsqrt(jnp.mean(hf * hf, axis=-1, keepdims=True) + EPS)
    dgain = jnp.sum(dyf * (hf * inv), axis=0, keepdims=True)
    dn = dyf * gain
    slope = jnp.sum(dn * hf, axis=-1, keepdims=True) * (inv * inv * inv) / D
    return (dn * inv - hf * slope).astype(BF16), dgain


def softmax_scores(q, k):
    scores = dot_nt(q, k) * HEAD**-0.5
    rows = true_position(lax.broadcasted_iota(jnp.int32, (S, 1), 0))
    cols = true_position(lax.broadcasted_iota(jnp.int32, (1, S), 1))
    scores = jnp.where(rows >= cols, scores, -1e30)
    e = jnp.exp(scores - jnp.max(scores, axis=-1, keepdims=True))
    return e / jnp.sum(e, axis=-1, keepdims=True)


def head_cols(head, which):
    return ds(head * 3 + which, HEAD)


def per_head(one, together):
    def step(j):
        for i in range(together):
            one(j * together + i)

    loop(HEADS // together, step)


def attention(qkv, o, together, probs=None):
    def one(head):
        prob = softmax_scores(qkv[:, head_cols(head, 0)], qkv[:, head_cols(head, 1)])
        if probs is not None:
            probs[head] = prob
        o[:, ds(head, HEAD)] = dot(prob.astype(BF16), qkv[:, head_cols(head, 2)]).astype(BF16)

    per_head(one, together)


def half_qkv(u, wq, qkv):
    def body(half):
        rows = ds(half, HS)
        for j in range(NQ // 512):
            qkv[rows, ds(j, 512)] = dot(u[rows, :], wq[:, ds(j, 512)]).astype(BF16)

    return body


def half_mlp(n, wg, wu, last, tile, hook=None):
    def body(half):
        rows = ds(half, HS)

        def one(j):
            if hook is not None:
                hook(half, j)
            for k in range(tile // 512):
                cols = ds(j * (tile // 512) + k, 512)
                z1 = dot(n[rows, :], wg[:, cols]).astype(BF16).astype(F32)
                z3 = dot(n[rows, :], wu[:, cols]).astype(BF16).astype(F32)
                last(rows, cols, z1, z3)

        loop(NF // tile, one)

    return body


def forward_kernel(x, ga, gm, wq_h, wo_h, wg_h, wu_h, wd_h, hs, y,
                   wq, wo, wg, wu, wd, h, u, n, qkv, o, m, part, near, out, far,
                   wsem, gsend, grecv, ssend, srecv):
    p = Peers()
    pairs = ((wq_h, wq), (wo_h, wo), (wg_h, wg), (wu_h, wu), (wd_h, wd))

    def load(i, layer):
        return pltpu.make_async_copy(pairs[i][0].at[layer], pairs[i][1], wsem.at[i])

    for i in range(5):
        load(i, 0).start()
    h[...] = x[...]
    p.barrier()
    gu = Gather(p, u, gsend, grecv, 0)
    gn = Gather(p, n, gsend, grecv, 1)
    scatter = Scatter(p, part, near, out, far, ssend, srecv, 2)

    def enter(half, layer):
        u[owned(p.me, half), :] = norm(h[ds(half, HR), :], ga[pl.ds(layer, 1), :])
        gu.start(half)

    def add(half):
        rows = ds(half, HR)
        total = h[rows, :] + scatter.result(half)
        h[rows, :] = total
        return total

    loop(2, lambda half: enter(half, 0))

    def layer_step(layer):
        more = layer < LAYERS - 1

        def refill(i):
            @pl.when(more)
            def _():
                load(i, layer + 1).start()

        load(0, layer).wait()
        gu.each(half_qkv(u, wq, qkv))
        refill(0)
        attention(qkv, o, 4)
        load(1, layer).wait()

        def project(half):
            scatter.run(half, lambda rows, cols: dot(o[rows, :], wo[:, cols]))
            scatter.mids(half)

        loop(2, project)
        refill(1)
        gu.finish()

        def between(half):
            n[owned(p.me, half), :] = norm(add(half), gm[pl.ds(layer, 1), :])
            gn.start(half)

        loop(2, between)

        def last(rows, cols, z1, z3):
            m[rows, cols] = (z1 * jax.nn.sigmoid(z1) * z3).astype(BF16)

        def send_first(half, j):
            @pl.when((half == 1) & (j == 1))
            def _():
                scatter.mids(0)

        gate_up = half_mlp(n, wg, wu, last, 1024, send_first)
        for i in (2, 3, 4):
            load(i, layer).wait()
        gn.relay(0)

        def mlp(half):
            gn.arrived(half)
            gate_up(half)

            @pl.when(half == 0)
            def _():
                gn.relay(1)

            scatter.run(half, lambda rows, cols: dot(m[rows, :], wd[:, cols]))

        loop(2, mlp)
        scatter.mids(1)
        refill(2)
        refill(3)
        refill(4)
        gn.finish()

        def leave(half):
            total = add(half)

            @pl.when(more)
            def _():
                hs[layer, ds(half, HR), :] = total
                enter(half, layer + 1)

            @pl.when(jnp.logical_not(more))
            def _():
                y[ds(half, HR), :] = total

        loop(2, leave)

    loop(LAYERS, layer_step)


def finish_layer(h, gain, own, far, d_mid, rows):
    d_in = (own[rows, :] + far[rows, :].astype(F32)).astype(BF16)
    d_norm, dgain = norm_back(h[rows, :], gain, d_in)
    return d_mid[rows, :] + d_norm, dgain


def backward_kernel(layer, hin, *refs):
    first_call, last_call = layer == LAYERS - 1, layer == 0
    refs = list(refs)
    take = lambda k: [refs.pop(0) for _ in range(k)]
    if first_call:
        (dy,) = take(1)
    else:
        h_above, above_own, above_far, above_mid, gin = take(5)
    ga, gm, wq_h, wo_h, wg_h, wu_h, wd_h = take(7)
    own_out, far_out, mid_out, gout = take(4)
    saved_h = take(9)
    u, dqkv, o, da, n, dg, du, m, dd = saved = take(9)
    wq, wo, wg, wu, wd = take(5)
    hm, qkv, probs, dgated, dh, part, near, out, far, gbuf, gmid, gfar, dy_buf = take(13)
    wsem, osem, gsend, grecv, ssend, srecv, rsend, rrecv = take(8)

    p = Peers()
    pairs = ((wq_h, wq), (wo_h, wo), (wg_h, wg), (wu_h, wu), (wd_h, wd))
    loads = [pltpu.make_async_copy(src.at[layer], dst, wsem.at[i]) for i, (src, dst) in enumerate(pairs)]
    saves = [pltpu.make_async_copy(src, dst, osem.at[i]) for i, (src, dst) in enumerate(zip(saved, saved_h))]
    for i in (0, 1, 4, 2, 3):
        loads[i].start()
    h = hin.at[layer - 1] if layer > 0 else hin
    if not first_call:
        h_above = h_above.at[layer]
    gain_a, gain_m = ga[pl.ds(layer, 1), :], gm[pl.ds(layer, 1), :]
    gu, gd, gn, gda = (Gather(p, buf, gsend, grecv, i) for i, buf in enumerate((u, dd, n, da)))
    two = Scatter(p, part, near, out, far, ssend, srecv, 2)
    four = Scatter(p, part, near, out, far, ssend, srecv, 4)
    p.barrier()

    def enter(half):
        u[owned(p.me, half), :] = norm(h[ds(half, HR), :], gain_a)
        gu.start(half)

    if first_call:
        gbuf[...] = jnp.zeros_like(gbuf)
    else:
        dy = dy_buf
        gbuf[...] = gin[...]

    def enter_d(half):
        rows = ds(half, HR)
        if not first_call:
            above = layer + 1
            total, dgain = finish_layer(h_above, ga[above : above + 1, :], above_own, above_far, above_mid, rows)
            dy[rows, :] = total
            gbuf[above : above + 1, :] = gbuf[above : above + 1, :] + dgain
        dd[owned(p.me, half), :] = dy[rows, :]
        gd.start(half)

    loop(2, enter)
    loop(2, enter_d)

    loads[0].wait()
    gu.each(half_qkv(u, wq, qkv))
    saves[0].start()
    attention(qkv, o, 2, probs)
    saves[2].start()
    loads[1].wait()

    def project(half):
        two.run(half, lambda rows, cols: dot(o[rows, :], wo[:, cols]))
        two.mids(half)

    loop(2, project)

    loop(2, gd.relay)
    loop(2, gd.arrived)
    saves[8].start()
    loads[4].wait()

    def gated(j):
        dgated[:, ds(j, 512)] = dot_nt(dd[...], wd[ds(j, 512), :]).astype(BF16)

    loop(NF // 512, gated)

    def between(half):
        rows = ds(half, HR)
        h_mid = h[rows, :] + two.result(half)
        hm[rows, :] = h_mid
        n[owned(p.me, half), :] = norm(h_mid, gain_m)
        gn.start(half)

    loop(2, between)
    loads[2].wait()
    loads[3].wait()

    def last(rows, cols, z1, z3):
        sig = jax.nn.sigmoid(z1)
        silu = z1 * sig
        dm = dgated[rows, cols].astype(F32)
        m[rows, cols] = (silu * z3).astype(BF16)
        du[rows, cols] = (dm * silu).astype(BF16)
        dg[rows, cols] = (dm * z3 * (sig + silu * (1.0 - sig))).astype(BF16)

    gn.each(half_mlp(n, wg, wu, last, 1024))
    for i in (4, 5, 6, 7):
        saves[i].start()

    four.run_full(lambda cols: dot_nt(dg[...], wg[cols, :]) + dot_nt(du[...], wu[cols, :]))

    def mid_back(half):
        rows = ds(half, HR)
        d_norm, dgain = norm_back(hm[rows, :], gain_m, four.result(half))
        da[owned(p.me, half), :] = dy[rows, :] + d_norm
        gda.start(half)
        row = pl.ds(LAYERS + layer, 1)
        gbuf[row, :] = gbuf[row, :] + dgain

    loop(2, mid_back)
    if last_call:
        near_g = remote(gbuf, gmid, rsend.at[0], rrecv.at[0], p.sib)
        near_g.start()

    def heads(half):
        rows = ds(half, HS)
        dh[rows, :] = dot_nt(da[rows, :], wo[...]).astype(BF16)

    gda.each(heads)
    saves[3].start()

    def back(head):
        prob = probs[head]
        d_o = dh[:, ds(head, HEAD)]
        q, k, v = (qkv[:, head_cols(head, i)] for i in range(3))
        d_prob = dot_nt(d_o, v)
        d_scores = (prob * (d_prob - jnp.sum(d_prob * prob, axis=-1, keepdims=True)) * HEAD**-0.5).astype(BF16)
        dqkv[:, head_cols(head, 0)] = dot(d_scores, k).astype(BF16)
        dqkv[:, head_cols(head, 1)] = dot_tn(d_scores, q).astype(BF16)
        dqkv[:, head_cols(head, 2)] = dot_tn(prob.astype(BF16), d_o).astype(BF16)

    per_head(back, 4)
    saves[1].start()
    if last_call:
        near_g.wait()
        gbuf[...] = gbuf[...] + gmid[...]
        far_g = remote(gbuf, gfar, rsend.at[1], rrecv.at[1], p.cross)
        far_g.start()
    last_sum = Scatter(p, part, near, far_out, None, ssend, srecv, 4)
    last_sum.run_full(lambda cols: dot_nt(dqkv[...], wq[cols, :]), send=False)
    for half in range(2):
        mid_out[ds(half, HR), :] = da[owned(p.me, half), :]
    last_sum.own_sum(own_out)
    if last_call:
        far_g.wait()
        gout[...] = gbuf[...] + gfar[...]
    else:
        gout[...] = gbuf[...]
    for g in (gu, gd, gn, gda):
        g.finish()
    for save in saves:
        save.wait()


def closing_kernel(x, own, far, d_mid, gin, ga, dx, ga_out, gm_out, mine, others, send, recv):
    p = Peers()
    p.barrier(p.diag)
    mine[...] = jnp.zeros_like(mine)

    def finish(half):
        rows = ds(half, HR)
        total, dgain = finish_layer(x, ga[0:1, :], own, far, d_mid, rows)
        dx[rows, :] = total
        mine[0:1, :] = mine[0:1, :] + dgain

    loop(2, finish)
    copies = [
        remote(mine, others.at[i], send.at[i], recv.at[i], peer) for i, peer in enumerate((p.cross, p.diag, p.sib))
    ]
    for copy in copies:
        copy.start()
    ga_out[1:LAYERS, :] = gin[1:LAYERS, :]
    gm_out[...] = gin[LAYERS : 2 * LAYERS, :]
    for copy in copies:
        copy.wait()
    ga_out[0:1, :] = ((mine[...] + others[2]) + (others[0] + others[1]))[0:1, :]


def wgrad_kernel(layer, n_alias, u_h, dqkv_h, o_h, da_h, n_h, dg_h, du_h, m_h, dd_h, *refs):
    refs = list(refs)
    take = lambda k: [refs.pop(0) for _ in range(k)]
    take(n_alias)
    y_in = take(1) if n_alias == 0 else ()
    gqkv_h, gout_h, ggate_h, gup_h, gdown_h = take(5)
    y_out = take(1) if n_alias == 0 else ()
    u, dqkv, o, da, lhs, rhs, gqkv, gout, gmlp = take(9)
    isem, osem = take(2)
    for y, result in zip(y_in, y_out):
        result[...] = y[...]
    sources = (n_h, dg_h, du_h, m_h, dd_h, u_h, dqkv_h, o_h, da_h)
    targets = (lhs.at[0], rhs.at[0], rhs.at[1], lhs.at[1], rhs.at[2], u, dqkv, o, da)
    loads = [pltpu.make_async_copy(src, dst, isem.at[i]) for i, (src, dst) in enumerate(zip(sources, targets))]
    for load in loads:
        load.start()

    def tiles(a, b, stage, first, count):
        for i in [first + k for k in range(count)]:
            left = a[:, ds(i, S)].T
            for c in range(b.shape[1] // 512):
                stage[ds(i, S), ds(c, 512)] = dot(left, b[:, ds(c, 512)]).astype(BF16)

    def copy(stage, out, i, sem):
        return pltpu.make_async_copy(stage.at[ds(i, 2 * S), :], out.at[layer, ds(i, 2 * S), :], sem)

    mlp_outs = (ggate_h, gup_h, gdown_h)
    loads[0].wait()
    loads[1].wait()

    def mlp(step):
        which, i = step // 4, lax.rem(step, 4)

        @pl.when(step == 4)
        def _():
            loads[2].wait()

        @pl.when(step == 8)
        def _():
            loads[3].wait()
            loads[4].wait()

        stage = gmlp.at[which]
        tiles(lhs.at[which // 2], rhs.at[which], stage, i * 2, 2)
        for k, out in enumerate(mlp_outs):
            @pl.when(which == k)
            def _():
                copy(stage, out, i, osem.at[k, i]).start()

    loop(12, mlp)
    for load in loads[5:]:
        load.wait()

    def qkv(i):
        tiles(u, dqkv, gqkv, i * 2, 2)
        copy(gqkv, gqkv_h, i, osem.at[3, i]).start()

    loop(4, qkv)
    tiles(o, da, gout, 0, 2)
    copy(gout, gout_h, 0, osem.at[4, 0]).start()
    for i in range(4):
        for k, out in enumerate(mlp_outs):
            copy(gmlp.at[k], out, i, osem.at[k, i]).wait()
        copy(gqkv, gqkv_h, i, osem.at[3, i]).wait()
    copy(gout, gout_h, 0, osem.at[4, 0]).wait()


def vmem():
    return pl.BlockSpec(memory_space=pltpu.VMEM)


def hbm():
    return pl.BlockSpec(memory_space=pltpu.HBM)


WEIGHT_SCRATCH = [
    pltpu.VMEM((D, NQ), BF16),
    pltpu.VMEM((NO, D), BF16),
    pltpu.VMEM((D, NF), BF16),
    pltpu.VMEM((D, NF), BF16),
    pltpu.VMEM((NF, D), BF16),
]
SCATTER_SCRATCH = [
    pltpu.VMEM((S, D), F32),
    pltpu.VMEM((2, R, D), F32),
    pltpu.VMEM((R, D), BF16),
    pltpu.VMEM((R, D), BF16),
]
SAVED = [(S, D), (S, NQ), (S, NO), (S, D), (S, D), (S, NF), (S, NF), (S, NF), (S, D)]
GRADS = [(D, NQ), (NO, D), (D, NF), (D, NF), (NF, D)]


def run_forward(x, ga, gm, weights):
    dma = pltpu.SemaphoreType.DMA
    return pl.pallas_call(
        forward_kernel,
        name="forward",
        out_shape=[jax.ShapeDtypeStruct((LAYERS - 1, R, D), BF16), jax.ShapeDtypeStruct((R, D), BF16)],
        in_specs=[vmem()] * 3 + [hbm()] * 5,
        out_specs=[vmem()] * 2,
        scratch_shapes=WEIGHT_SCRATCH
        + [
            pltpu.VMEM((R, D), BF16),
            pltpu.VMEM((S, D), BF16),
            pltpu.VMEM((S, D), BF16),
            pltpu.VMEM((S, NQ), BF16),
            pltpu.VMEM((S, NO), BF16),
            pltpu.VMEM((S, NF), BF16),
        ]
        + SCATTER_SCRATCH
        + [dma((5,)), dma((2, 3, 2)), dma((2, 3, 2)), dma((3, 2, 2)), dma((3, 2, 2))],
        compiler_params=pltpu.CompilerParams(collective_id=0, has_side_effects=True, vmem_limit_bytes=VMEM_LIMIT),
    )(x, ga, gm, *weights)


def run_backward(layer, hin, above, ga, gm, weights):
    dma = pltpu.SemaphoreType.DMA
    results = [((R, D), F32), ((R, D), BF16), ((R, D), BF16), ((8, D), F32)] + [(shape, BF16) for shape in SAVED]
    outs = pl.pallas_call(
        functools.partial(backward_kernel, layer),
        name=f"backward{layer}",
        out_shape=[jax.ShapeDtypeStruct(*result) for result in results],
        in_specs=[vmem()] * (3 + len(above)) + [hbm()] * 5,
        out_specs=[vmem()] * 4 + [hbm()] * 9,
        scratch_shapes=[pltpu.VMEM(shape, BF16) for shape in SAVED]
        + WEIGHT_SCRATCH
        + [
            pltpu.VMEM((R, D), BF16),
            pltpu.VMEM((S, NQ), BF16),
            pltpu.VMEM((HEADS, S, S), F32),
            pltpu.VMEM((S, NF), BF16),
            pltpu.VMEM((S, NO), BF16),
        ]
        + SCATTER_SCRATCH
        + [pltpu.VMEM((8, D), F32)] * 3
        + [pltpu.VMEM((R, D), BF16)]
        + [dma((5,)), dma((9,)), dma((4, 3, 2)), dma((4, 3, 2)), dma((3, 2, 4)), dma((3, 2, 4)), dma((2,)), dma((2,))],
        compiler_params=pltpu.CompilerParams(
            collective_id=1 + layer, has_side_effects=True, vmem_limit_bytes=VMEM_LIMIT
        ),
    )(hin, *above, ga, gm, *weights)
    return outs[:4], outs[4:]


def run_closing(x, above, ga):
    dma = pltpu.SemaphoreType.DMA
    return pl.pallas_call(
        closing_kernel,
        name="closing",
        out_shape=[jax.ShapeDtypeStruct((R, D), BF16)] + [jax.ShapeDtypeStruct((LAYERS, D), F32)] * 2,
        in_specs=[vmem()] * 6,
        out_specs=[vmem()] * 3,
        scratch_shapes=[pltpu.VMEM((8, D), F32), pltpu.VMEM((3, 8, D), F32), dma((3,)), dma((3,))],
        compiler_params=pltpu.CompilerParams(
            collective_id=1 + LAYERS, has_side_effects=True, vmem_limit_bytes=VMEM_LIMIT
        ),
    )(x, *above, ga)


def run_wgrad(layer, saved, grads, y=()):
    dma = pltpu.SemaphoreType.DMA
    n_alias = len(grads)
    return pl.pallas_call(
        functools.partial(wgrad_kernel, layer, n_alias),
        name=f"wgrad{layer}",
        out_shape=[jax.ShapeDtypeStruct((LAYERS, *shape), BF16) for shape in GRADS]
        + [jax.ShapeDtypeStruct((R, D), BF16)] * len(y),
        in_specs=[hbm()] * (9 + n_alias) + [vmem()] * len(y),
        out_specs=[hbm()] * 5 + [vmem()] * len(y),
        input_output_aliases={9 + i: i for i in range(n_alias)},
        scratch_shapes=[pltpu.VMEM(shape, BF16) for shape in SAVED[:4]]
        + [pltpu.VMEM(shape, BF16) for shape in ((2, S, D), (3, S, D), GRADS[0], GRADS[1], (3, D, D))]
        + [dma((9,)), dma((5, 4))],
        compiler_params=pltpu.CompilerParams(vmem_limit_bytes=VMEM_LIMIT),
        cost_estimate=pl.CostEstimate(flops=8_600_000_000, bytes_accessed=42_000_000, transcendentals=0),
    )(*saved, *grads, *y)


def solution(mesh):
    row_spec = P(("dp", "tp"), None)
    col_spec = P(None, None, "tp")
    mid_spec = P(None, "tp", None)
    in_specs = (row_spec, row_spec, P(None, None), P(None, None), col_spec, mid_spec, col_spec, col_spec, mid_spec)
    out_specs = (
        row_spec, row_spec, P("dp", None, "tp"), P("dp", "tp", None), P("dp", None, "tp"), P("dp", None, "tp"),
        P("dp", "tp", None), P("dp", None), P("dp", None),
    )

    def device_step(x, grad_y, gain_attn, gain_mlp, w_qkv, w_out, w_gate, w_up, w_down):
        weights = (w_qkv, w_out, w_gate, w_up, w_down)
        hs, y = run_forward(x, gain_attn, gain_mlp, weights)
        above = (grad_y,)
        grads, y = (), (y,)
        for layer in reversed(range(LAYERS)):
            (own, chip_sum, d_mid, gains), saved = run_backward(
                layer, hs if layer > 0 else x, above, gain_attn, gain_mlp, weights
            )
            far = lax.ppermute(chip_sum, "tp", [(0, 2), (1, 3), (2, 0), (3, 1)])
            grads = run_wgrad(layer, saved, grads, y if layer == LAYERS - 1 else ())
            if layer == LAYERS - 1:
                *grads, y = grads
            far, grads = lax.optimization_barrier((far, tuple(grads)))
            above = (*((hs,) if layer > 0 else ()), own, far, d_mid, gains)
        grad_x, *gains = run_closing(x, above, gain_attn)
        return (y, grad_x, *grads, *gains)

    return jax.shard_map(device_step, mesh=mesh, in_specs=in_specs, out_specs=out_specs, check_vma=False)
```

```python
import functools

import jax
import jax.numpy as jnp
from jax import lax
from jax.experimental import pallas as pl
from jax.experimental.pallas import tpu as pltpu
from jax.sharding import PartitionSpec as P

HEAD = 128
EPS = 1e-5
MESH = pl.DeviceIdType.MESH
F32 = jnp.float32
BF16 = jnp.bfloat16
VMEM_LIMIT = 67_000_000

D = 2048
S = 256
R = 64
NQ = 1536
NO = 512
NF = 2048
HEADS = 4
LAYERS = 3

HR = R // 2
HS = S // 2


def dot(a, b):
    return jnp.dot(a, b, preferred_element_type=F32)


def dot_nt(a, b):
    return lax.dot_general(a, b, (((1,), (1,)), ((), ())), preferred_element_type=F32)


def dot_tn(a, b):
    return lax.dot_general(a, b, (((0,), (0,)), ((), ())), preferred_element_type=F32)


def ds(i, n):
    return pl.ds(i * n if isinstance(i, int) else pl.multiple_of(i * n, n), n)


def loop(n, body):
    lax.fori_loop(0, n, lambda i, c: (body(i), c)[1], 0)


class Peers:
    def __init__(self):
        self.me = lax.axis_index("tp")
        core, chip = lax.rem(self.me, 2), self.me // 2
        self.sib = chip * 2 + (1 - core)
        self.cross = (1 - chip) * 2 + core
        self.diag = (1 - chip) * 2 + (1 - core)

    def barrier(self, *more):
        sem = pltpu.get_barrier_semaphore()
        for peer in (self.sib, self.cross, *more):
            pl.semaphore_signal(sem, inc=1, device_id={"tp": peer}, device_id_type=MESH)
        pl.semaphore_wait(sem, 2 + len(more))


def remote(src, dst, send, recv, peer):
    return pltpu.make_async_remote_copy(
        src_ref=src, dst_ref=dst, send_sem=send, recv_sem=recv, device_id={"tp": peer}, device_id_type=MESH
    )


def owned(owner, half):
    return ds(half * 4 + owner, HR)


def true_position(row):
    return lax.rem(row, HS) // HR * R + row // HS * HR + lax.rem(row, HR)


class Gather:
    def __init__(self, p, buf, send, recv, which):
        self.p, self.buf, self.send, self.recv, self.which = p, buf, send, recv, which

    def _copy(self, kind, half, chunk, owner, peer):
        part = self.buf.at[owned(owner, half), ds(chunk, D // 2)]
        sems = (self.which, kind, half, chunk)
        return remote(part, part, self.send.at[sems], self.recv.at[sems], peer)

    def start(self, half):
        for chunk in range(2):
            self._copy(0, half, chunk, self.p.me, self.p.cross).start()
        for chunk in range(2):
            self._copy(1, half, chunk, self.p.me, self.p.sib).start()

    def relay(self, half, chunk):
        self._copy(0, half, chunk, self.p.cross, self.p.cross).wait_recv()
        self._copy(2, half, chunk, self.p.cross, self.p.sib).start()

    def arrived(self, half, chunk):
        self._copy(1, half, chunk, self.p.sib, self.p.sib).wait_recv()
        self._copy(2, half, chunk, self.p.diag, self.p.sib).wait_recv()

    def each(self, bodies, middle=None, after=None):
        self.relay(0, 0)

        def one(half):
            @pl.when(half == 0)
            def _():
                self.relay(0, 1)

            self.arrived(half, 0)
            bodies[0](half)

            @pl.when(half == 0)
            def _():
                self.relay(1, 0)

            if middle is not None:
                middle(half)
            self.arrived(half, 1)
            bodies[1](half)

            @pl.when(half == 0)
            def _():
                self.relay(1, 1)

            if after is not None:
                after(half)

        loop(2, one)

    def all(self):
        for half in range(2):
            for chunk in range(2):
                self.relay(half, chunk)
        for half in range(2):
            for chunk in range(2):
                self.arrived(half, chunk)

    def finish(self):
        def one(half):
            for chunk in range(2):
                self._copy(0, half, chunk, self.p.me, self.p.cross).wait_send()
                self._copy(1, half, chunk, self.p.me, self.p.sib).wait_send()
                self._copy(2, half, chunk, self.p.cross, self.p.sib).wait_send()

        loop(2, one)


class Scatter:
    def __init__(self, p, part, near, out, far, send, recv, chunks):
        self.p, self.part, self.near, self.out, self.far, self.send, self.recv = p, part, near, out, far, send, recv
        self.chunks, self.width = chunks, D // chunks

    def _near(self, kind, half, chunk):
        owner = self.p.diag if kind == 0 else self.p.sib
        cols = ds(chunk, self.width)
        return remote(
            self.part.at[owned(owner, half), cols],
            self.near.at[kind, ds(half, HR), cols],
            self.send.at[kind, half, chunk],
            self.recv.at[kind, half, chunk],
            self.p.sib,
        )

    def _far(self, half, chunk):
        cols = ds(chunk, self.width)
        return remote(
            self.out.at[ds(half, HR), cols],
            self.far.at[ds(half, HR), cols],
            self.send.at[2, half, chunk],
            self.recv.at[2, half, chunk],
            self.p.cross,
        )

    def _mid(self, half, chunk, send=True):
        self._near(0, half, chunk).wait_recv()
        cols = ds(chunk, self.width)
        total = self.part[owned(self.p.cross, half), cols] + self.near[0, ds(half, HR), cols]
        self.out[ds(half, HR), cols] = total.astype(BF16)
        if send:
            self._far(half, chunk).start()

    def mids(self, half):
        loop(self.chunks, lambda chunk: self._mid(half, chunk))

    def run(self, half, compute):
        def step(chunk):
            cols = ds(chunk, self.width)
            self.part[ds(half, HS), cols] = compute(ds(half, HS), cols)
            self._near(0, half, chunk).start()
            self._near(1, half, chunk).start()

        loop(self.chunks, step)

    def run_full(self, compute, send=True):
        def mids(chunk):
            self._mid(0, chunk, send)
            self._mid(1, chunk, send)

        def step(chunk):
            cols = ds(chunk, self.width)
            self.part[:, cols] = compute(cols)
            for kind in range(2):
                for half in range(2):
                    self._near(kind, half, chunk).start()

            @pl.when(chunk > 0)
            def _():
                mids(chunk - 1)

        loop(self.chunks, step)
        mids(self.chunks - 1)

    def result(self, half):
        def waits(chunk):
            self._near(1, half, chunk).wait_recv()
            self._far(half, chunk).wait_recv()

        def sent(chunk):
            self._near(0, half, chunk).wait_send()
            self._near(1, half, chunk).wait_send()
            self._far(half, chunk).wait_send()

        loop(self.chunks, waits)
        rows = ds(half, HR)
        total = self.part[owned(self.p.me, half), :] + self.near[1, rows, :] + self.far[rows, :].astype(F32)
        loop(self.chunks, sent)
        return total.astype(BF16)


    def own_sum(self, own):
        for half in range(2):
            for chunk in range(self.chunks):
                self._near(1, half, chunk).wait_recv()
            own[ds(half, HR), :] = self.part[owned(self.p.me, half), :] + self.near[1, ds(half, HR), :]
        for half in range(2):
            for chunk in range(self.chunks):
                for kind in range(2):
                    self._near(kind, half, chunk).wait_send()


def norm(h, gain):
    hf = h.astype(F32)
    inv = lax.rsqrt(jnp.mean(hf * hf, axis=-1, keepdims=True) + EPS)
    return (hf * inv * gain).astype(BF16)


def norm_back(h, gain, dy):
    hf, dyf = h.astype(F32), dy.astype(F32)
    inv = lax.rsqrt(jnp.mean(hf * hf, axis=-1, keepdims=True) + EPS)
    dgain = jnp.sum(dyf * (hf * inv), axis=0, keepdims=True)
    dn = dyf * gain
    slope = jnp.sum(dn * hf, axis=-1, keepdims=True) * (inv * inv * inv) / D
    return (dn * inv - hf * slope).astype(BF16), dgain


def softmax_scores(q, k):
    scores = dot_nt(q, k) * HEAD**-0.5
    rows = true_position(lax.broadcasted_iota(jnp.int32, (S, 1), 0))
    cols = true_position(lax.broadcasted_iota(jnp.int32, (1, S), 1))
    scores = jnp.where(rows >= cols, scores, -1e30)
    e = jnp.exp(scores - jnp.max(scores, axis=-1, keepdims=True))
    return e / jnp.sum(e, axis=-1, keepdims=True)


def head_cols(head, which):
    return ds(head * 3 + which, HEAD)


def per_head(one, together):
    def step(j):
        for i in range(together):
            one(j * together + i)

    loop(HEADS // together, step)


def attention(qkv, o, together, probs=None):
    def one(head):
        prob = softmax_scores(qkv[:, head_cols(head, 0)], qkv[:, head_cols(head, 1)])
        if probs is not None:
            probs[head] = prob
        o[:, ds(head, HEAD)] = dot(prob.astype(BF16), qkv[:, head_cols(head, 2)]).astype(BF16)

    per_head(one, together)


def half_qkv(u, wq, acc, qkv):
    def body(chunk, half):
        rows, deep = ds(half, HS), ds(chunk, D // 2)
        for j in range(NQ // 512):
            cols = ds(j, 512)
            part = dot(u[rows, deep], wq[deep, cols])
            if chunk == 0:
                acc[:, cols] = part
            else:
                qkv[rows, cols] = (acc[:, cols] + part).astype(BF16)

    return [functools.partial(body, chunk) for chunk in range(2)]


def half_mlp(n, wg, wu, acc1, acc3, last, tile):
    def body(chunk, half):
        rows, deep = ds(half, HS), ds(chunk, D // 2)

        def one(j):
            for k in range(tile // 512):
                cols = ds(j * (tile // 512) + k, 512)
                z1 = dot(n[rows, deep], wg[deep, cols])
                z3 = dot(n[rows, deep], wu[deep, cols])
                if chunk == 0:
                    acc1[:, cols] = z1
                    acc3[:, cols] = z3
                else:
                    z1 = (acc1[:, cols] + z1).astype(BF16).astype(F32)
                    z3 = (acc3[:, cols] + z3).astype(BF16).astype(F32)
                    last(rows, cols, z1, z3)

        loop(NF // tile, one)

    return [functools.partial(body, chunk) for chunk in range(2)]


def forward_kernel(x, ga, gm, wq_h, wo_h, wg_h, wu_h, wd_h, h1, h2, y,
                   wq, wo, wg, wu, wd, h, u, n, acc1, acc3, qkv, o, m, part, near, out, far,
                   wsem, gsend, grecv, ssend, srecv):
    p = Peers()
    pairs = ((wq_h, wq), (wo_h, wo), (wg_h, wg), (wu_h, wu), (wd_h, wd))

    def load(i, layer):
        return pltpu.make_async_copy(pairs[i][0].at[layer], pairs[i][1], wsem.at[i])

    for i in range(5):
        load(i, 0).start()
    h[...] = x[...]
    p.barrier()
    gu = Gather(p, u, gsend, grecv, 0)
    gn = Gather(p, n, gsend, grecv, 1)
    scatter = Scatter(p, part, near, out, far, ssend, srecv, 2)

    def enter(half, layer):
        u[owned(p.me, half), :] = norm(h[ds(half, HR), :], ga[pl.ds(layer, 1), :])
        gu.start(half)

    def add(half):
        rows = ds(half, HR)
        total = h[rows, :] + scatter.result(half)
        h[rows, :] = total
        return total

    loop(2, lambda half: enter(half, 0))

    def layer_step(layer):
        more = layer < LAYERS - 1

        def refill(i):
            @pl.when(more)
            def _():
                load(i, layer + 1).start()

        load(0, layer).wait()
        gu.each(half_qkv(u, wq, acc1, qkv))
        refill(0)
        attention(qkv, o, 4)
        load(1, layer).wait()

        def project(half):
            scatter.run(half, lambda rows, cols: dot(o[rows, :], wo[:, cols]))
            scatter.mids(half)

        loop(2, project)
        refill(1)
        gu.finish()

        def between(half):
            n[owned(p.me, half), :] = norm(add(half), gm[pl.ds(layer, 1), :])
            gn.start(half)

        loop(2, between)

        def last(rows, cols, z1, z3):
            m[rows, cols] = (z1 * jax.nn.sigmoid(z1) * z3).astype(BF16)

        for i in (2, 3, 4):
            load(i, layer).wait()

        def send_first(half):
            @pl.when(half == 1)
            def _():
                scatter.mids(0)

        gn.each(
            half_mlp(n, wg, wu, acc1, acc3, last, 1024),
            send_first,
            lambda half: scatter.run(half, lambda rows, cols: dot(m[rows, :], wd[:, cols])),
        )
        scatter.mids(1)
        refill(2)
        refill(3)
        refill(4)
        gn.finish()

        def leave(half):
            total = add(half)

            for i, kept in enumerate((h1, h2, y)):
                @pl.when(layer == i)
                def _():
                    kept[ds(half, HR), :] = total

            @pl.when(more)
            def _():
                enter(half, layer + 1)

        loop(2, leave)

    loop(LAYERS, layer_step)


def finish_layer(h, gain, own, far, d_mid, rows):
    d_in = (own[rows, :] + far[rows, :].astype(F32)).astype(BF16)
    d_norm, dgain = norm_back(h[rows, :], gain, d_in)
    return d_mid[rows, :] + d_norm, dgain


def backward_kernel(layer, hin, *refs):
    first_call, last_call = layer == LAYERS - 1, layer == 0
    refs = list(refs)
    take = lambda k: [refs.pop(0) for _ in range(k)]
    if first_call:
        (dy,) = take(1)
    else:
        h_above, above_own, above_far, above_mid, gin = take(5)
    ga, gm, wq_h, wo_h, wg_h, wu_h, wd_h = take(7)
    own_out, far_out, mid_out, gout = take(4)
    saved_h = take(9)
    u, dqkv, o, da, n, dg, du, m, dd = saved = take(9)
    wq, wo, wg, wu, wd = take(5)
    hm, acc1, acc3, qkv, probs, dgated, dh, part, near, out, far, gbuf, gmid, gfar, dy_buf = take(15)
    wsem, osem, gsend, grecv, ssend, srecv, rsend, rrecv = take(8)

    p = Peers()
    pairs = ((wq_h, wq), (wo_h, wo), (wg_h, wg), (wu_h, wu), (wd_h, wd))
    loads = [pltpu.make_async_copy(src.at[layer], dst, wsem.at[i]) for i, (src, dst) in enumerate(pairs)]
    saves = [pltpu.make_async_copy(src, dst, osem.at[i]) for i, (src, dst) in enumerate(zip(saved, saved_h))]
    for i in (0, 1, 4, 2, 3):
        loads[i].start()
    h = hin
    gain_a, gain_m = ga[pl.ds(layer, 1), :], gm[pl.ds(layer, 1), :]
    gu, gd, gn, gda = (Gather(p, buf, gsend, grecv, i) for i, buf in enumerate((u, dd, n, da)))
    two = Scatter(p, part, near, out, far, ssend, srecv, 2)
    four = Scatter(p, part, near, out, far, ssend, srecv, 4)
    p.barrier()

    def enter(half):
        u[owned(p.me, half), :] = norm(h[ds(half, HR), :], gain_a)
        gu.start(half)

    if first_call:
        gbuf[...] = jnp.zeros_like(gbuf)
    else:
        dy = dy_buf
        gbuf[...] = gin[...]

    def enter_d(half):
        rows = ds(half, HR)
        if not first_call:
            above = layer + 1
            total, dgain = finish_layer(h_above, ga[above : above + 1, :], above_own, above_far, above_mid, rows)
            dy[rows, :] = total
            gbuf[above : above + 1, :] = gbuf[above : above + 1, :] + dgain
        dd[owned(p.me, half), :] = dy[rows, :]
        gd.start(half)

    loop(2, enter)
    loop(2, enter_d)

    loads[0].wait()
    gu.each(half_qkv(u, wq, acc1, qkv))
    saves[0].start()
    attention(qkv, o, 2, probs)
    saves[2].start()
    loads[1].wait()

    def project(half):
        two.run(half, lambda rows, cols: dot(o[rows, :], wo[:, cols]))
        two.mids(half)

    loop(2, project)

    gd.all()
    saves[8].start()
    loads[4].wait()

    def gated(j):
        dgated[:, ds(j, 512)] = dot_nt(dd[...], wd[ds(j, 512), :]).astype(BF16)

    loop(NF // 512, gated)

    def between(half):
        rows = ds(half, HR)
        h_mid = h[rows, :] + two.result(half)
        hm[rows, :] = h_mid
        n[owned(p.me, half), :] = norm(h_mid, gain_m)
        gn.start(half)

    loop(2, between)
    loads[2].wait()
    loads[3].wait()

    def last(rows, cols, z1, z3):
        sig = jax.nn.sigmoid(z1)
        silu = z1 * sig
        dm = dgated[rows, cols].astype(F32)
        m[rows, cols] = (silu * z3).astype(BF16)
        du[rows, cols] = (dm * silu).astype(BF16)
        dg[rows, cols] = (dm * z3 * (sig + silu * (1.0 - sig))).astype(BF16)

    gn.each(half_mlp(n, wg, wu, acc1, acc3, last, 1024))
    for i in (4, 5, 6, 7):
        saves[i].start()

    four.run_full(lambda cols: dot_nt(dg[...], wg[cols, :]) + dot_nt(du[...], wu[cols, :]))

    def mid_back(half):
        rows = ds(half, HR)
        d_norm, dgain = norm_back(hm[rows, :], gain_m, four.result(half))
        da[owned(p.me, half), :] = dy[rows, :] + d_norm
        gda.start(half)
        row = pl.ds(LAYERS + layer, 1)
        gbuf[row, :] = gbuf[row, :] + dgain

    loop(2, mid_back)
    if last_call:
        near_g = remote(gbuf, gmid, rsend.at[0], rrecv.at[0], p.sib)
        near_g.start()

    def heads(chunk, half):
        rows, deep = ds(half, HS), ds(chunk, D // 2)
        part_h = dot_nt(da[rows, deep], wo[:, deep])
        if chunk == 0:
            acc1[:, :NO] = part_h
        else:
            dh[rows, :] = (acc1[:, :NO] + part_h).astype(BF16)

    gda.each([functools.partial(heads, chunk) for chunk in range(2)])
    saves[3].start()

    def back(head):
        prob = probs[head]
        d_o = dh[:, ds(head, HEAD)]
        q, k, v = (qkv[:, head_cols(head, i)] for i in range(3))
        d_prob = dot_nt(d_o, v)
        d_scores = (prob * (d_prob - jnp.sum(d_prob * prob, axis=-1, keepdims=True)) * HEAD**-0.5).astype(BF16)
        dqkv[:, head_cols(head, 0)] = dot(d_scores, k).astype(BF16)
        dqkv[:, head_cols(head, 1)] = dot_tn(d_scores, q).astype(BF16)
        dqkv[:, head_cols(head, 2)] = dot_tn(prob.astype(BF16), d_o).astype(BF16)

    per_head(back, 4)
    saves[1].start()
    if last_call:
        near_g.wait()
        gbuf[...] = gbuf[...] + gmid[...]
        far_g = remote(gbuf, gfar, rsend.at[1], rrecv.at[1], p.cross)
        far_g.start()
    last_sum = Scatter(p, part, near, far_out, None, ssend, srecv, 4)
    last_sum.run_full(lambda cols: dot_nt(dqkv[...], wq[cols, :]), send=False)
    for half in range(2):
        mid_out[ds(half, HR), :] = da[owned(p.me, half), :]
    last_sum.own_sum(own_out)
    if last_call:
        far_g.wait()
        gout[...] = gbuf[...] + gfar[...]
    else:
        gout[...] = gbuf[...]
    for g in (gu, gd, gn, gda):
        g.finish()
    for save in saves:
        save.wait()


def closing_kernel(x, own, far, d_mid, gin, ga, dx, ga_out, gm_out, mine, others, send, recv):
    p = Peers()
    p.barrier(p.diag)
    mine[...] = jnp.zeros_like(mine)

    def finish(half):
        rows = ds(half, HR)
        total, dgain = finish_layer(x, ga[0:1, :], own, far, d_mid, rows)
        dx[rows, :] = total
        mine[0:1, :] = mine[0:1, :] + dgain

    loop(2, finish)
    copies = [
        remote(mine, others.at[i], send.at[i], recv.at[i], peer) for i, peer in enumerate((p.cross, p.diag, p.sib))
    ]
    for copy in copies:
        copy.start()
    ga_out[1:LAYERS, :] = gin[1:LAYERS, :]
    gm_out[...] = gin[LAYERS : 2 * LAYERS, :]
    for copy in copies:
        copy.wait()
    ga_out[0:1, :] = ((mine[...] + others[2]) + (others[0] + others[1]))[0:1, :]


def wgrad_kernel(layer, n_alias, u_h, dqkv_h, o_h, da_h, n_h, dg_h, du_h, m_h, dd_h, *refs):
    refs = list(refs)
    take = lambda k: [refs.pop(0) for _ in range(k)]
    take(n_alias)
    gqkv_h, gout_h, ggate_h, gup_h, gdown_h = take(5)
    u, dqkv, o, da, lhs, rhs, gqkv, gout, gmlp = take(9)
    isem, osem = take(2)
    sources = (n_h, dg_h, du_h, m_h, dd_h, u_h, dqkv_h, o_h, da_h)
    targets = (lhs.at[0], rhs.at[0], rhs.at[1], lhs.at[1], rhs.at[2], u, dqkv, o, da)
    loads = [pltpu.make_async_copy(src, dst, isem.at[i]) for i, (src, dst) in enumerate(zip(sources, targets))]
    for load in loads:
        load.start()

    def tiles(a, b, stage, first, count):
        for i in [first + k for k in range(count)]:
            left = a[:, ds(i, S)].T
            for c in range(b.shape[1] // 512):
                stage[ds(i, S), ds(c, 512)] = dot(left, b[:, ds(c, 512)]).astype(BF16)

    def copy(stage, out, i, sem):
        return pltpu.make_async_copy(stage.at[ds(i, 2 * S), :], out.at[layer, ds(i, 2 * S), :], sem)

    mlp_outs = (ggate_h, gup_h, gdown_h)
    loads[0].wait()
    loads[1].wait()

    def mlp(step):
        which, i = step // 4, lax.rem(step, 4)

        @pl.when(step == 4)
        def _():
            loads[2].wait()

        @pl.when(step == 8)
        def _():
            loads[3].wait()
            loads[4].wait()

        stage = gmlp.at[which]
        tiles(lhs.at[which // 2], rhs.at[which], stage, i * 2, 2)
        for k, out in enumerate(mlp_outs):
            @pl.when(which == k)
            def _():
                copy(stage, out, i, osem.at[k, i]).start()

    loop(12, mlp)
    for load in loads[5:]:
        load.wait()

    def qkv(i):
        tiles(u, dqkv, gqkv, i * 2, 2)
        copy(gqkv, gqkv_h, i, osem.at[3, i]).start()

    loop(4, qkv)
    tiles(o, da, gout, 0, 2)
    copy(gout, gout_h, 0, osem.at[4, 0]).start()
    for i in range(4):
        for k, out in enumerate(mlp_outs):
            copy(gmlp.at[k], out, i, osem.at[k, i]).wait()
        copy(gqkv, gqkv_h, i, osem.at[3, i]).wait()
    copy(gout, gout_h, 0, osem.at[4, 0]).wait()


def vmem():
    return pl.BlockSpec(memory_space=pltpu.VMEM)


def hbm():
    return pl.BlockSpec(memory_space=pltpu.HBM)


WEIGHT_SCRATCH = [
    pltpu.VMEM((D, NQ), BF16),
    pltpu.VMEM((NO, D), BF16),
    pltpu.VMEM((D, NF), BF16),
    pltpu.VMEM((D, NF), BF16),
    pltpu.VMEM((NF, D), BF16),
]
SCATTER_SCRATCH = [
    pltpu.VMEM((S, D), F32),
    pltpu.VMEM((2, R, D), F32),
    pltpu.VMEM((R, D), BF16),
    pltpu.VMEM((R, D), BF16),
]
SAVED = [(S, D), (S, NQ), (S, NO), (S, D), (S, D), (S, NF), (S, NF), (S, NF), (S, D)]
GRADS = [(D, NQ), (NO, D), (D, NF), (D, NF), (NF, D)]


def run_forward(x, ga, gm, weights):
    dma = pltpu.SemaphoreType.DMA
    return pl.pallas_call(
        forward_kernel,
        name="forward",
        out_shape=[jax.ShapeDtypeStruct((R, D), BF16)] * 3,
        in_specs=[vmem()] * 3 + [hbm()] * 5,
        out_specs=[vmem()] * 3,
        scratch_shapes=WEIGHT_SCRATCH
        + [
            pltpu.VMEM((R, D), BF16),
            pltpu.VMEM((S, D), BF16),
            pltpu.VMEM((S, D), BF16),
            pltpu.VMEM((HS, NF), F32),
            pltpu.VMEM((HS, NF), F32),
            pltpu.VMEM((S, NQ), BF16),
            pltpu.VMEM((S, NO), BF16),
            pltpu.VMEM((S, NF), BF16),
        ]
        + SCATTER_SCRATCH
        + [dma((5,)), dma((2, 3, 2, 2)), dma((2, 3, 2, 2)), dma((3, 2, 2)), dma((3, 2, 2))],
        compiler_params=pltpu.CompilerParams(collective_id=0, has_side_effects=True, vmem_limit_bytes=VMEM_LIMIT),
    )(x, ga, gm, *weights)


def run_backward(layer, hin, above, ga, gm, weights):
    dma = pltpu.SemaphoreType.DMA
    results = [((R, D), F32), ((R, D), BF16), ((R, D), BF16), ((8, D), F32)] + [(shape, BF16) for shape in SAVED]
    outs = pl.pallas_call(
        functools.partial(backward_kernel, layer),
        name=f"backward{layer}",
        out_shape=[jax.ShapeDtypeStruct(*result) for result in results],
        in_specs=[vmem()] * (3 + len(above)) + [hbm()] * 5,
        out_specs=[vmem()] * 4 + [hbm()] * 9,
        scratch_shapes=[pltpu.VMEM(shape, BF16) for shape in SAVED]
        + WEIGHT_SCRATCH
        + [
            pltpu.VMEM((R, D), BF16),
            pltpu.VMEM((HS, NF), F32),
            pltpu.VMEM((HS, NF), F32),
            pltpu.VMEM((S, NQ), BF16),
            pltpu.VMEM((HEADS, S, S), F32),
            pltpu.VMEM((S, NF), BF16),
            pltpu.VMEM((S, NO), BF16),
        ]
        + SCATTER_SCRATCH
        + [pltpu.VMEM((8, D), F32)] * 3
        + [pltpu.VMEM((R, D), BF16)]
        + [dma((5,)), dma((9,)), dma((4, 3, 2, 2)), dma((4, 3, 2, 2)), dma((3, 2, 4)), dma((3, 2, 4)), dma((2,)), dma((2,))],
        compiler_params=pltpu.CompilerParams(
            collective_id=1 + layer, has_side_effects=True, vmem_limit_bytes=VMEM_LIMIT
        ),
    )(hin, *above, ga, gm, *weights)
    return outs[:4], outs[4:]


def run_closing(above, ga):
    dma = pltpu.SemaphoreType.DMA
    return pl.pallas_call(
        closing_kernel,
        name="closing",
        out_shape=[jax.ShapeDtypeStruct((R, D), BF16)] + [jax.ShapeDtypeStruct((LAYERS, D), F32)] * 2,
        in_specs=[vmem()] * 6,
        out_specs=[vmem()] * 3,
        scratch_shapes=[pltpu.VMEM((8, D), F32), pltpu.VMEM((3, 8, D), F32), dma((3,)), dma((3,))],
        compiler_params=pltpu.CompilerParams(
            collective_id=1 + LAYERS, has_side_effects=True, vmem_limit_bytes=8_000_000
        ),
    )(*above, ga)


def run_wgrad(layer, saved, grads):
    dma = pltpu.SemaphoreType.DMA
    n_alias = len(grads)
    return pl.pallas_call(
        functools.partial(wgrad_kernel, layer, n_alias),
        name=f"wgrad{layer}",
        out_shape=[jax.ShapeDtypeStruct((LAYERS, *shape), BF16) for shape in GRADS],
        in_specs=[hbm()] * (9 + n_alias),
        out_specs=[hbm()] * 5,
        input_output_aliases={9 + i: i for i in range(n_alias)},
        scratch_shapes=[pltpu.VMEM(shape, BF16) for shape in SAVED[:4]]
        + [pltpu.VMEM(shape, BF16) for shape in ((2, S, D), (3, S, D), GRADS[0], GRADS[1], (3, D, D))]
        + [dma((9,)), dma((5, 4))],
        compiler_params=pltpu.CompilerParams(vmem_limit_bytes=VMEM_LIMIT if layer > 0 else 66_200_000),
        cost_estimate=pl.CostEstimate(flops=8_600_000_000, bytes_accessed=42_000_000, transcendentals=0),
    )(*saved, *grads)


def solution(mesh):
    row_spec = P(("dp", "tp"), None)
    col_spec = P(None, None, "tp")
    mid_spec = P(None, "tp", None)
    in_specs = (row_spec, row_spec, P(None, None), P(None, None), col_spec, mid_spec, col_spec, col_spec, mid_spec)
    out_specs = (
        row_spec, row_spec, P("dp", None, "tp"), P("dp", "tp", None), P("dp", None, "tp"), P("dp", None, "tp"),
        P("dp", "tp", None), P("dp", None), P("dp", None),
    )

    def device_step(x, grad_y, gain_attn, gain_mlp, w_qkv, w_out, w_gate, w_up, w_down):
        weights = (w_qkv, w_out, w_gate, w_up, w_down)
        h1, h2, y = run_forward(x, gain_attn, gain_mlp, weights)
        kept, above = (x, h1, h2), (grad_y,)
        grads = ()
        for layer in reversed(range(LAYERS)):
            (own, chip_sum, d_mid, gains), saved = run_backward(
                layer, kept[layer], above, gain_attn, gain_mlp, weights
            )
            far = lax.ppermute(chip_sum, "tp", [(0, 2), (1, 3), (2, 0), (3, 1)])
            grads = run_wgrad(layer, saved, grads)
            far, grads = lax.optimization_barrier((far, tuple(grads)))
            above = (kept[layer], own, far, d_mid, gains)
        grad_x, *gains = run_closing(above, gain_attn)
        return (y, grad_x, *grads, *gains)

    return jax.shard_map(device_step, mesh=mesh, in_specs=in_specs, out_specs=out_specs, check_vma=False)
```

```python
import functools

import jax
import jax.numpy as jnp
from jax import lax
from jax.experimental import pallas as pl
from jax.experimental.pallas import tpu as pltpu
from jax.sharding import PartitionSpec as P

HEAD = 128
EPS = 1e-5
MESH = pl.DeviceIdType.MESH
F32 = jnp.float32
BF16 = jnp.bfloat16
VMEM_LIMIT = 67_000_000

D = 2048
S = 256
R = 64
NQ = 1536
NO = 512
NF = 2048
HEADS = 4
LAYERS = 3

HR = R // 2
HS = S // 2


def dot(a, b):
    return jnp.dot(a, b, preferred_element_type=F32)


def dot_nt(a, b):
    return lax.dot_general(a, b, (((1,), (1,)), ((), ())), preferred_element_type=F32)


def dot_tn(a, b):
    return lax.dot_general(a, b, (((0,), (0,)), ((), ())), preferred_element_type=F32)


def ds(i, n):
    return pl.ds(i * n if isinstance(i, int) else pl.multiple_of(i * n, n), n)


def loop(n, body):
    lax.fori_loop(0, n, lambda i, c: (body(i), c)[1], 0)


class Peers:
    def __init__(self):
        self.me = lax.axis_index("tp")
        core, chip = lax.rem(self.me, 2), self.me // 2
        self.sib = chip * 2 + (1 - core)
        self.cross = (1 - chip) * 2 + core
        self.diag = (1 - chip) * 2 + (1 - core)

    def here(self, *more):
        self.partners = 2 + len(more)
        for peer in (self.sib, self.cross, *more):
            pl.semaphore_signal(pltpu.get_barrier_semaphore(), inc=1, device_id={"tp": peer}, device_id_type=MESH)

    def ready(self):
        pl.semaphore_wait(pltpu.get_barrier_semaphore(), self.partners)


def remote(src, dst, send, recv, peer):
    return pltpu.make_async_remote_copy(
        src_ref=src, dst_ref=dst, send_sem=send, recv_sem=recv, device_id={"tp": peer}, device_id_type=MESH
    )


def owned(owner, half):
    return ds(half * 4 + owner, HR)


def true_position(row):
    return lax.rem(row, HS) // HR * R + row // HS * HR + lax.rem(row, HR)


class Gather:
    def __init__(self, p, buf, send, recv, which):
        self.p, self.buf, self.send, self.recv, self.which = p, buf, send, recv, which

    def _copy(self, kind, half, chunk, owner, peer):
        part = self.buf.at[owned(owner, half), ds(chunk, D // 2)]
        sems = (self.which, kind, half, chunk)
        return remote(part, part, self.send.at[sems], self.recv.at[sems], peer)

    def start(self, half):
        for chunk in range(2):
            self._copy(0, half, chunk, self.p.me, self.p.cross).start()
        for chunk in range(2):
            self._copy(1, half, chunk, self.p.me, self.p.sib).start()

    def relay(self, half, chunk):
        self._copy(0, half, chunk, self.p.cross, self.p.cross).wait_recv()
        self._copy(2, half, chunk, self.p.cross, self.p.sib).start()

    def arrived(self, half, chunk):
        self._copy(1, half, chunk, self.p.sib, self.p.sib).wait_recv()
        self._copy(2, half, chunk, self.p.diag, self.p.sib).wait_recv()

    def each(self, bodies, middle=None, after=None):
        self.relay(0, 0)

        def one(half):
            @pl.when(half == 0)
            def _():
                self.relay(0, 1)

            self.arrived(half, 0)
            bodies[0](half)

            @pl.when(half == 0)
            def _():
                self.relay(1, 0)

            if middle is not None:
                middle(half)
            self.arrived(half, 1)
            bodies[1](half)

            @pl.when(half == 0)
            def _():
                self.relay(1, 1)

            if after is not None:
                after(half)

        loop(2, one)

    def all(self):
        for half in range(2):
            for chunk in range(2):
                self.relay(half, chunk)
        for half in range(2):
            for chunk in range(2):
                self.arrived(half, chunk)

    def finish(self):
        def one(half):
            for chunk in range(2):
                self._copy(0, half, chunk, self.p.me, self.p.cross).wait_send()
                self._copy(1, half, chunk, self.p.me, self.p.sib).wait_send()
                self._copy(2, half, chunk, self.p.cross, self.p.sib).wait_send()

        loop(2, one)


class Scatter:
    def __init__(self, p, part, near, out, far, send, recv, chunks):
        self.p, self.part, self.near, self.out, self.far, self.send, self.recv = p, part, near, out, far, send, recv
        self.chunks, self.width = chunks, D // chunks

    def _near(self, kind, half, chunk):
        owner = self.p.diag if kind == 0 else self.p.sib
        cols = ds(chunk, self.width)
        return remote(
            self.part.at[owned(owner, half), cols],
            self.near.at[kind, ds(half, HR), cols],
            self.send.at[kind, half, chunk],
            self.recv.at[kind, half, chunk],
            self.p.sib,
        )

    def _far(self, half, chunk):
        cols = ds(chunk, self.width)
        return remote(
            self.out.at[ds(half, HR), cols],
            self.far.at[ds(half, HR), cols],
            self.send.at[2, half, chunk],
            self.recv.at[2, half, chunk],
            self.p.cross,
        )

    def _mid(self, half, chunk, send=True):
        self._near(0, half, chunk).wait_recv()
        cols = ds(chunk, self.width)
        total = self.part[owned(self.p.cross, half), cols] + self.near[0, ds(half, HR), cols]
        self.out[ds(half, HR), cols] = total.astype(BF16)
        if send:
            self._far(half, chunk).start()

    def mids(self, half):
        loop(self.chunks, lambda chunk: self._mid(half, chunk))

    def run(self, half, compute, unrolled=False):
        def step(chunk):
            cols = ds(chunk, self.width)
            self.part[ds(half, HS), cols] = compute(ds(half, HS), cols)
            self._near(0, half, chunk).start()
            self._near(1, half, chunk).start()

        if unrolled:
            for chunk in range(self.chunks):
                step(chunk)
        else:
            loop(self.chunks, step)

    def run_full(self, compute, send=True):
        def mids(chunk):
            self._mid(0, chunk, send)
            self._mid(1, chunk, send)

        def step(chunk):
            cols = ds(chunk, self.width)
            self.part[:, cols] = compute(cols)
            for kind in range(2):
                for half in range(2):
                    self._near(kind, half, chunk).start()

            @pl.when(chunk > 0)
            def _():
                mids(chunk - 1)

        loop(self.chunks, step)
        mids(self.chunks - 1)

    def result(self, half):
        def waits(chunk):
            self._near(1, half, chunk).wait_recv()
            self._far(half, chunk).wait_recv()

        def sent(chunk):
            self._near(0, half, chunk).wait_send()
            self._near(1, half, chunk).wait_send()
            self._far(half, chunk).wait_send()

        loop(self.chunks, waits)
        rows = ds(half, HR)
        total = self.part[owned(self.p.me, half), :] + self.near[1, rows, :] + self.far[rows, :].astype(F32)
        loop(self.chunks, sent)
        return total.astype(BF16)


    def own_sum(self, own):
        for half in range(2):
            for chunk in range(self.chunks):
                self._near(1, half, chunk).wait_recv()
            own[ds(half, HR), :] = self.part[owned(self.p.me, half), :] + self.near[1, ds(half, HR), :]
        for half in range(2):
            for chunk in range(self.chunks):
                for kind in range(2):
                    self._near(kind, half, chunk).wait_send()


def norm(h, gain):
    hf = h.astype(F32)
    inv = lax.rsqrt(jnp.mean(hf * hf, axis=-1, keepdims=True) + EPS)
    return (hf * inv * gain).astype(BF16)


def norm_back(h, gain, dy):
    hf, dyf = h.astype(F32), dy.astype(F32)
    inv = lax.rsqrt(jnp.mean(hf * hf, axis=-1, keepdims=True) + EPS)
    dgain = jnp.sum(dyf * (hf * inv), axis=0, keepdims=True)
    dn = dyf * gain
    slope = jnp.sum(dn * hf, axis=-1, keepdims=True) * (inv * inv * inv) / D
    return (dn * inv - hf * slope).astype(BF16), dgain


def softmax_scores(q, k):
    scores = dot_nt(q, k) * HEAD**-0.5
    rows = true_position(lax.broadcasted_iota(jnp.int32, (S, 1), 0))
    cols = true_position(lax.broadcasted_iota(jnp.int32, (1, S), 1))
    scores = jnp.where(rows >= cols, scores, -1e30)
    e = jnp.exp(scores - jnp.max(scores, axis=-1, keepdims=True))
    return e / jnp.sum(e, axis=-1, keepdims=True)


def head_cols(head, which):
    return ds(head * 3 + which, HEAD)


def per_head(one, together):
    def step(j):
        for i in range(together):
            one(j * together + i)

    loop(HEADS // together, step)


def attention(qkv, o, together, probs=None):
    def one(head):
        prob = softmax_scores(qkv[:, head_cols(head, 0)], qkv[:, head_cols(head, 1)])
        if probs is not None:
            probs[head] = prob
        o[:, ds(head, HEAD)] = dot(prob.astype(BF16), qkv[:, head_cols(head, 2)]).astype(BF16)

    per_head(one, together)


def half_qkv(u, wq, acc, qkv):
    def body(chunk, half):
        rows, deep = ds(half, HS), ds(chunk, D // 2)
        for j in range(NQ // 512):
            cols = ds(j, 512)
            part = dot(u[rows, deep], wq[deep, cols])
            if chunk == 0:
                acc[:, cols] = part
            else:
                qkv[rows, cols] = (acc[:, cols] + part).astype(BF16)

    return [functools.partial(body, chunk) for chunk in range(2)]


def half_mlp(n, wg, wu, acc1, acc3, last, tile):
    def body(chunk, half):
        rows, deep = ds(half, HS), ds(chunk, D // 2)

        def one(j):
            for k in range(tile // 512):
                cols = ds(j * (tile // 512) + k, 512)
                z1 = dot(n[rows, deep], wg[deep, cols])
                z3 = dot(n[rows, deep], wu[deep, cols])
                if chunk == 0:
                    acc1[:, cols] = z1
                    acc3[:, cols] = z3
                else:
                    z1 = (acc1[:, cols] + z1).astype(BF16).astype(F32)
                    z3 = (acc3[:, cols] + z3).astype(BF16).astype(F32)
                    last(rows, cols, z1, z3)

        if tile == NF:
            one(0)
        else:
            loop(NF // tile, one)

    return [functools.partial(body, chunk) for chunk in range(2)]


def forward_kernel(x, ga, gm, wq_h, wo_h, wg_h, wu_h, wd_h, h1, h2, y,
                   wq, wo, wg, wu, wd, h, u, n, acc1, acc3, qkv, o, m, part, near, out, far,
                   wsem, gsend, grecv, ssend, srecv):
    p = Peers()
    pairs = ((wq_h, wq), (wo_h, wo), (wg_h, wg), (wu_h, wu), (wd_h, wd))

    def load(i, layer):
        return pltpu.make_async_copy(pairs[i][0].at[layer], pairs[i][1], wsem.at[i])

    p.here()
    for i in range(5):
        load(i, 0).start()
    h[...] = x[...]
    gu = Gather(p, u, gsend, grecv, 0)
    gn = Gather(p, n, gsend, grecv, 1)
    scatter = Scatter(p, part, near, out, far, ssend, srecv, 2)

    def enter(half, layer):
        u[owned(p.me, half), :] = norm(h[ds(half, HR), :], ga[pl.ds(layer, 1), :])

    def add(half):
        rows = ds(half, HR)
        total = h[rows, :] + scatter.result(half)
        h[rows, :] = total
        return total

    loop(2, lambda half: enter(half, 0))
    p.ready()
    loop(2, gu.start)

    def layer_step(layer):
        more = layer < LAYERS - 1

        def refill(i):
            @pl.when(more)
            def _():
                load(i, layer + 1).start()

        load(0, layer).wait()
        gu.each(half_qkv(u, wq, acc1, qkv))
        refill(0)
        attention(qkv, o, 4)
        load(1, layer).wait()

        def project(half):
            scatter.run(half, lambda rows, cols: dot(o[rows, :], wo[:, cols]))
            scatter.mids(half)

        loop(2, project)
        refill(1)
        gu.finish()

        def between(half):
            n[owned(p.me, half), :] = norm(add(half), gm[pl.ds(layer, 1), :])
            gn.start(half)

        loop(2, between)

        def last(rows, cols, z1, z3):
            m[rows, cols] = (z1 * jax.nn.sigmoid(z1) * z3).astype(BF16)

        for i in (2, 3, 4):
            load(i, layer).wait()

        def send_first(half):
            @pl.when(half == 1)
            def _():
                scatter.mids(0)

        gn.each(
            half_mlp(n, wg, wu, acc1, acc3, last, NF),
            send_first,
            lambda half: scatter.run(half, lambda rows, cols: dot(m[rows, :], wd[:, cols]), True),
        )
        scatter.mids(1)
        refill(2)
        refill(3)
        refill(4)
        gn.finish()

        def leave(half):
            total = add(half)

            for i, kept in enumerate((h1, h2, y)):
                @pl.when(layer == i)
                def _():
                    kept[ds(half, HR), :] = total

            @pl.when(more)
            def _():
                enter(half, layer + 1)
                gu.start(half)

        loop(2, leave)

    loop(LAYERS, layer_step)


def finish_layer(h, gain, own, far, d_mid, rows):
    d_in = (own[rows, :] + far[rows, :].astype(F32)).astype(BF16)
    d_norm, dgain = norm_back(h[rows, :], gain, d_in)
    return d_mid[rows, :] + d_norm, dgain


def backward_kernel(layer, hin, *refs):
    first_call, last_call = layer == LAYERS - 1, layer == 0
    refs = list(refs)
    take = lambda k: [refs.pop(0) for _ in range(k)]
    if first_call:
        (dy,) = take(1)
    else:
        h_above, above_own, above_far, above_mid, gin = take(5)
    ga, gm, wq_h, wo_h, wg_h, wu_h, wd_h = take(7)
    own_out, far_out, mid_out, gout = take(4)
    saved_h = take(9)
    u, dqkv, o, da, n, dg, du, m, dd = saved = take(9)
    wq, wo, wg, wu, wd = take(5)
    hm, acc1, acc3, qkv, probs, dgated, dh, part, near, out, far, gbuf, gmid, gfar, dy_buf = take(15)
    wsem, osem, gsend, grecv, ssend, srecv, rsend, rrecv = take(8)

    p = Peers()
    pairs = ((wq_h, wq), (wo_h, wo), (wg_h, wg), (wu_h, wu), (wd_h, wd))
    loads = [pltpu.make_async_copy(src.at[layer], dst, wsem.at[i]) for i, (src, dst) in enumerate(pairs)]
    saves = [pltpu.make_async_copy(src, dst, osem.at[i]) for i, (src, dst) in enumerate(zip(saved, saved_h))]
    p.here()
    for i in (0, 1, 4, 2, 3):
        loads[i].start()
    h = hin
    gain_a, gain_m = ga[pl.ds(layer, 1), :], gm[pl.ds(layer, 1), :]
    gu, gd, gn, gda = (Gather(p, buf, gsend, grecv, i) for i, buf in enumerate((u, dd, n, da)))
    two = Scatter(p, part, near, out, far, ssend, srecv, 2)
    four = Scatter(p, part, near, out, far, ssend, srecv, 4)

    def enter(half):
        u[owned(p.me, half), :] = norm(h[ds(half, HR), :], gain_a)

    if first_call:
        gbuf[...] = jnp.zeros_like(gbuf)
    else:
        dy = dy_buf
        gbuf[...] = gin[...]

    def enter_d(half):
        rows = ds(half, HR)
        if not first_call:
            above = layer + 1
            total, dgain = finish_layer(h_above, ga[above : above + 1, :], above_own, above_far, above_mid, rows)
            dy[rows, :] = total
            gbuf[above : above + 1, :] = gbuf[above : above + 1, :] + dgain
        dd[owned(p.me, half), :] = dy[rows, :]
        gd.start(half)

    loop(2, enter)
    p.ready()
    loop(2, gu.start)
    loop(2, enter_d)

    loads[0].wait()
    gu.each(half_qkv(u, wq, acc1, qkv))
    saves[0].start()
    attention(qkv, o, 2, probs)
    saves[2].start()
    loads[1].wait()

    def project(half):
        two.run(half, lambda rows, cols: dot(o[rows, :], wo[:, cols]))
        two.mids(half)

    loop(2, project)

    gd.all()
    saves[8].start()
    loads[4].wait()

    def gated(j):
        dgated[:, ds(j, 512)] = dot_nt(dd[...], wd[ds(j, 512), :]).astype(BF16)

    loop(NF // 512, gated)

    def between(half):
        rows = ds(half, HR)
        h_mid = h[rows, :] + two.result(half)
        hm[rows, :] = h_mid
        n[owned(p.me, half), :] = norm(h_mid, gain_m)
        gn.start(half)

    loop(2, between)
    loads[2].wait()
    loads[3].wait()

    def last(rows, cols, z1, z3):
        sig = jax.nn.sigmoid(z1)
        silu = z1 * sig
        dm = dgated[rows, cols].astype(F32)
        m[rows, cols] = (silu * z3).astype(BF16)
        du[rows, cols] = (dm * silu).astype(BF16)
        dg[rows, cols] = (dm * z3 * (sig + silu * (1.0 - sig))).astype(BF16)

    gn.each(half_mlp(n, wg, wu, acc1, acc3, last, 1024))
    for i in (4, 5, 6, 7):
        saves[i].start()

    four.run_full(lambda cols: dot_nt(dg[...], wg[cols, :]) + dot_nt(du[...], wu[cols, :]))

    def mid_back(half):
        rows = ds(half, HR)
        d_norm, dgain = norm_back(hm[rows, :], gain_m, four.result(half))
        da[owned(p.me, half), :] = dy[rows, :] + d_norm
        gda.start(half)
        row = pl.ds(LAYERS + layer, 1)
        gbuf[row, :] = gbuf[row, :] + dgain

    loop(2, mid_back)
    if last_call:
        near_g = remote(gbuf, gmid, rsend.at[0], rrecv.at[0], p.sib)
        near_g.start()

    def heads(chunk, half):
        rows, deep = ds(half, HS), ds(chunk, D // 2)
        part_h = dot_nt(da[rows, deep], wo[:, deep])
        if chunk == 0:
            acc1[:, :NO] = part_h
        else:
            dh[rows, :] = (acc1[:, :NO] + part_h).astype(BF16)

    gda.each([functools.partial(heads, chunk) for chunk in range(2)])
    saves[3].start()

    def back(head):
        prob = probs[head]
        d_o = dh[:, ds(head, HEAD)]
        q, k, v = (qkv[:, head_cols(head, i)] for i in range(3))
        d_prob = dot_nt(d_o, v)
        d_scores = (prob * (d_prob - jnp.sum(d_prob * prob, axis=-1, keepdims=True)) * HEAD**-0.5).astype(BF16)
        dqkv[:, head_cols(head, 0)] = dot(d_scores, k).astype(BF16)
        dqkv[:, head_cols(head, 1)] = dot_tn(d_scores, q).astype(BF16)
        dqkv[:, head_cols(head, 2)] = dot_tn(prob.astype(BF16), d_o).astype(BF16)

    per_head(back, 4)
    saves[1].start()
    if last_call:
        near_g.wait()
        gbuf[...] = gbuf[...] + gmid[...]
        far_g = remote(gbuf, gfar, rsend.at[1], rrecv.at[1], p.cross)
        far_g.start()
    last_sum = Scatter(p, part, near, far_out, None, ssend, srecv, 4)
    last_sum.run_full(lambda cols: dot_nt(dqkv[...], wq[cols, :]), send=False)
    for half in range(2):
        mid_out[ds(half, HR), :] = da[owned(p.me, half), :]
    last_sum.own_sum(own_out)
    if last_call:
        far_g.wait()
        gout[...] = gbuf[...] + gfar[...]
    else:
        gout[...] = gbuf[...]
    for g in (gu, gd, gn, gda):
        g.finish()
    for save in saves:
        save.wait()


def closing_kernel(x, own, far, d_mid, gin, ga, dx, ga_out, gm_out, mine, others, send, recv):
    p = Peers()
    p.here(p.diag)
    mine[...] = jnp.zeros_like(mine)

    def finish(half):
        rows = ds(half, HR)
        total, dgain = finish_layer(x, ga[0:1, :], own, far, d_mid, rows)
        dx[rows, :] = total
        mine[0:1, :] = mine[0:1, :] + dgain

    loop(2, finish)
    p.ready()
    copies = [
        remote(mine, others.at[i], send.at[i], recv.at[i], peer) for i, peer in enumerate((p.cross, p.diag, p.sib))
    ]
    for copy in copies:
        copy.start()
    ga_out[1:LAYERS, :] = gin[1:LAYERS, :]
    gm_out[...] = gin[LAYERS : 2 * LAYERS, :]
    for copy in copies:
        copy.wait()
    ga_out[0:1, :] = ((mine[...] + others[2]) + (others[0] + others[1]))[0:1, :]


def wgrad_kernel(layer, n_alias, u_h, dqkv_h, o_h, da_h, n_h, dg_h, du_h, m_h, dd_h, *refs):
    refs = list(refs)
    take = lambda k: [refs.pop(0) for _ in range(k)]
    take(n_alias)
    passed = n_alias == 0
    y_in = take(1) if passed else ()
    gqkv_h, gout_h, ggate_h, gup_h, gdown_h = take(5)
    y_out = take(1) if passed else ()
    u, dqkv, lhs, rhs, gqkv, gwide, y_buf = take(7)
    isem, osem, ysem = take(3)
    y_load = [pltpu.make_async_copy(y, y_buf, ysem.at[0]) for y in y_in]
    y_save = [pltpu.make_async_copy(y_buf, y, ysem.at[1]) for y in y_out]
    sources = (n_h, dg_h, du_h, m_h, dd_h, o_h, da_h, u_h, dqkv_h)
    targets = (lhs.at[0], rhs.at[0], rhs.at[1], lhs.at[1], rhs.at[2], lhs.at[2, :, :NO], rhs.at[3], u, dqkv)
    loads = [pltpu.make_async_copy(src, dst, isem.at[i]) for i, (src, dst) in enumerate(zip(sources, targets))]
    for load in loads + y_load:
        load.start()

    def tiles(a, b, stage, first, count):
        for i in [first + k for k in range(count)]:
            left = a[:, ds(i, S)].T
            for c in range(b.shape[1] // 512):
                stage[ds(i, S), ds(c, 512)] = dot(left, b[:, ds(c, 512)]).astype(BF16)

    def copy(stage, out, i, sem):
        return pltpu.make_async_copy(stage.at[ds(i, 2 * S), :], out.at[layer, ds(i, 2 * S), :], sem)

    wide_outs = (ggate_h, gup_h, gdown_h, gout_h)
    loads[0].wait()
    loads[1].wait()

    def wide(step):
        which, i = step // 4, lax.rem(step, 4)
        for at, needed in ((4, loads[2:3]), (8, loads[3:5]), (12, loads[5:7])):
            @pl.when(step == at)
            def _():
                for load in needed:
                    load.wait()

        stage = gwide.at[which]
        tiles(lhs.at[jnp.maximum(which - 1, 0)], rhs.at[which], stage, i * 2, 2)
        for k, out in enumerate(wide_outs):
            @pl.when(which == k)
            def _():
                copy(stage, out, i if k < 3 else 0, osem.at[k, i]).start()

    loop(13, wide)
    for load in loads[7:] + y_load:
        load.wait()
    for save in y_save:
        save.start()

    def qkv(i):
        tiles(u, dqkv, gqkv, i * 2, 2)
        copy(gqkv, gqkv_h, i, osem.at[4, i]).start()

    loop(4, qkv)
    for i in range(4):
        for k, out in enumerate(wide_outs[:3]):
            copy(gwide.at[k], out, i, osem.at[k, i]).wait()
        copy(gqkv, gqkv_h, i, osem.at[4, i]).wait()
    copy(gwide.at[3], gout_h, 0, osem.at[3, 0]).wait()
    for save in y_save:
        save.wait()


def vmem():
    return pl.BlockSpec(memory_space=pltpu.VMEM)


def hbm():
    return pl.BlockSpec(memory_space=pltpu.HBM)


WEIGHT_SCRATCH = [
    pltpu.VMEM((D, NQ), BF16),
    pltpu.VMEM((NO, D), BF16),
    pltpu.VMEM((D, NF), BF16),
    pltpu.VMEM((D, NF), BF16),
    pltpu.VMEM((NF, D), BF16),
]
SCATTER_SCRATCH = [
    pltpu.VMEM((S, D), F32),
    pltpu.VMEM((2, R, D), F32),
    pltpu.VMEM((R, D), BF16),
    pltpu.VMEM((R, D), BF16),
]
SAVED = [(S, D), (S, NQ), (S, NO), (S, D), (S, D), (S, NF), (S, NF), (S, NF), (S, D)]
GRADS = [(D, NQ), (NO, D), (D, NF), (D, NF), (NF, D)]


def run_forward(x, ga, gm, weights):
    dma = pltpu.SemaphoreType.DMA
    return pl.pallas_call(
        forward_kernel,
        name="forward",
        out_shape=[jax.ShapeDtypeStruct((R, D), BF16)] * 3,
        in_specs=[vmem()] * 3 + [hbm()] * 5,
        out_specs=[vmem()] * 3,
        scratch_shapes=WEIGHT_SCRATCH
        + [
            pltpu.VMEM((R, D), BF16),
            pltpu.VMEM((S, D), BF16),
            pltpu.VMEM((S, D), BF16),
            pltpu.VMEM((HS, NF), F32),
            pltpu.VMEM((HS, NF), F32),
            pltpu.VMEM((S, NQ), BF16),
            pltpu.VMEM((S, NO), BF16),
            pltpu.VMEM((S, NF), BF16),
        ]
        + SCATTER_SCRATCH
        + [dma((5,)), dma((2, 3, 2, 2)), dma((2, 3, 2, 2)), dma((3, 2, 2)), dma((3, 2, 2))],
        compiler_params=pltpu.CompilerParams(collective_id=0, has_side_effects=True, vmem_limit_bytes=VMEM_LIMIT),
    )(x, ga, gm, *weights)


def run_backward(layer, hin, above, ga, gm, weights):
    dma = pltpu.SemaphoreType.DMA
    results = [((R, D), F32), ((R, D), BF16), ((R, D), BF16), ((8, D), F32)] + [(shape, BF16) for shape in SAVED]
    outs = pl.pallas_call(
        functools.partial(backward_kernel, layer),
        name=f"backward{layer}",
        out_shape=[jax.ShapeDtypeStruct(*result) for result in results],
        in_specs=[vmem()] * (3 + len(above)) + [hbm()] * 5,
        out_specs=[vmem()] * 4 + [hbm()] * 9,
        scratch_shapes=[pltpu.VMEM(shape, BF16) for shape in SAVED]
        + WEIGHT_SCRATCH
        + [
            pltpu.VMEM((R, D), BF16),
            pltpu.VMEM((HS, NF), F32),
            pltpu.VMEM((HS, NF), F32),
            pltpu.VMEM((S, NQ), BF16),
            pltpu.VMEM((HEADS, S, S), F32),
            pltpu.VMEM((S, NF), BF16),
            pltpu.VMEM((S, NO), BF16),
        ]
        + SCATTER_SCRATCH
        + [pltpu.VMEM((8, D), F32)] * 3
        + [pltpu.VMEM((R, D), BF16)]
        + [dma((5,)), dma((9,)), dma((4, 3, 2, 2)), dma((4, 3, 2, 2)), dma((3, 2, 4)), dma((3, 2, 4)), dma((2,)), dma((2,))],
        compiler_params=pltpu.CompilerParams(
            collective_id=1 + layer, has_side_effects=True, vmem_limit_bytes=VMEM_LIMIT
        ),
    )(hin, *above, ga, gm, *weights)
    return outs[:4], outs[4:]


def run_closing(above, ga):
    dma = pltpu.SemaphoreType.DMA
    return pl.pallas_call(
        closing_kernel,
        name="closing",
        out_shape=[jax.ShapeDtypeStruct((R, D), BF16)] + [jax.ShapeDtypeStruct((LAYERS, D), F32)] * 2,
        in_specs=[vmem()] * 6,
        out_specs=[vmem()] * 3,
        scratch_shapes=[pltpu.VMEM((8, D), F32), pltpu.VMEM((3, 8, D), F32), dma((3,)), dma((3,))],
        compiler_params=pltpu.CompilerParams(
            collective_id=1 + LAYERS, has_side_effects=True, vmem_limit_bytes=8_000_000
        ),
    )(*above, ga)


def run_wgrad(layer, saved, grads, y):
    dma = pltpu.SemaphoreType.DMA
    n_alias = len(grads)
    return pl.pallas_call(
        functools.partial(wgrad_kernel, layer, n_alias),
        name=f"wgrad{layer}",
        out_shape=[jax.ShapeDtypeStruct((LAYERS, *shape), BF16) for shape in GRADS]
        + [jax.ShapeDtypeStruct((R, D), BF16)] * len(y),
        in_specs=[hbm()] * (9 + n_alias + len(y)),
        out_specs=[hbm()] * (5 + len(y)),
        input_output_aliases={9 + i: i for i in range(n_alias)},
        scratch_shapes=[pltpu.VMEM(shape, BF16) for shape in SAVED[:2]]
        + [pltpu.VMEM(shape, BF16) for shape in ((3, S, D), (4, S, D), GRADS[0], (4, D, D), (R, D))]
        + [dma((9,)), dma((5, 4)), dma((2,))],
        compiler_params=pltpu.CompilerParams(vmem_limit_bytes=VMEM_LIMIT if layer > 0 else 66_200_000),
        cost_estimate=pl.CostEstimate(flops=8_600_000_000, bytes_accessed=42_000_000, transcendentals=0),
    )(*saved, *grads, *y)


def solution(mesh):
    row_spec = P(("dp", "tp"), None)
    col_spec = P(None, None, "tp")
    mid_spec = P(None, "tp", None)
    in_specs = (row_spec, row_spec, P(None, None), P(None, None), col_spec, mid_spec, col_spec, col_spec, mid_spec)
    out_specs = (
        row_spec, row_spec, P("dp", None, "tp"), P("dp", "tp", None), P("dp", None, "tp"), P("dp", None, "tp"),
        P("dp", "tp", None), P("dp", None), P("dp", None),
    )

    def device_step(x, grad_y, gain_attn, gain_mlp, w_qkv, w_out, w_gate, w_up, w_down):
        weights = (w_qkv, w_out, w_gate, w_up, w_down)
        h1, h2, y = run_forward(x, gain_attn, gain_mlp, weights)
        kept, above = (x, h1, h2), (grad_y,)
        grads = ()
        for layer in reversed(range(LAYERS)):
            (own, chip_sum, d_mid, gains), saved = run_backward(
                layer, kept[layer], above, gain_attn, gain_mlp, weights
            )
            far = lax.ppermute(chip_sum, "tp", [(0, 2), (1, 3), (2, 0), (3, 1)])
            grads = run_wgrad(layer, saved, grads, () if grads else (y,))
            if len(grads) > len(GRADS):
                *grads, y = grads
            far, grads = lax.optimization_barrier((far, tuple(grads)))
            above = (kept[layer], own, far, d_mid, gains)
        grad_x, *gains = run_closing(above, gain_attn)
        return (y, grad_x, *grads, *gains)

    return jax.shard_map(device_step, mesh=mesh, in_specs=in_specs, out_specs=out_specs, check_vma=False)
```

```python
import functools

import jax
import jax.numpy as jnp
from jax import lax
from jax.experimental import pallas as pl
from jax.experimental.pallas import tpu as pltpu
from jax.sharding import PartitionSpec as P

HEAD = 128
EPS = 1e-5
MESH = pl.DeviceIdType.MESH
F32 = jnp.float32
BF16 = jnp.bfloat16
VMEM_LIMIT = 67_000_000

D = 2048
S = 256
R = 64
NQ = 1536
NO = 512
NF = 2048
HEADS = 4
LAYERS = 3

HR = R // 2
HS = S // 2


def dot(a, b):
    return jnp.dot(a, b, preferred_element_type=F32)


def dot_nt(a, b):
    return lax.dot_general(a, b, (((1,), (1,)), ((), ())), preferred_element_type=F32)


def dot_tn(a, b):
    return lax.dot_general(a, b, (((0,), (0,)), ((), ())), preferred_element_type=F32)


def ds(i, n):
    return pl.ds(i * n if isinstance(i, int) else pl.multiple_of(i * n, n), n)


def loop(n, body):
    lax.fori_loop(0, n, lambda i, c: (body(i), c)[1], 0)


class Peers:
    def __init__(self):
        self.me = lax.axis_index("tp")
        core, chip = lax.rem(self.me, 2), self.me // 2
        self.sib = chip * 2 + (1 - core)
        self.cross = (1 - chip) * 2 + core
        self.diag = (1 - chip) * 2 + (1 - core)

    def here(self, *more):
        self.partners = 2 + len(more)
        for peer in (self.sib, self.cross, *more):
            pl.semaphore_signal(pltpu.get_barrier_semaphore(), inc=1, device_id={"tp": peer}, device_id_type=MESH)

    def ready(self):
        pl.semaphore_wait(pltpu.get_barrier_semaphore(), self.partners)


def remote(src, dst, send, recv, peer):
    return pltpu.make_async_remote_copy(
        src_ref=src, dst_ref=dst, send_sem=send, recv_sem=recv, device_id={"tp": peer}, device_id_type=MESH
    )


def owned(owner, half):
    return ds(half * 4 + owner, HR)


def true_position(row):
    return lax.rem(row, HS) // HR * R + row // HS * HR + lax.rem(row, HR)


class Gather:
    def __init__(self, p, buf, send, recv, which):
        self.p, self.buf, self.send, self.recv, self.which = p, buf, send, recv, which

    def _copy(self, kind, half, chunk, owner, peer):
        part = self.buf.at[owned(owner, half), ds(chunk, D // 2)]
        sems = (self.which, kind, half, chunk)
        return remote(part, part, self.send.at[sems], self.recv.at[sems], peer)

    def start(self, half):
        for chunk in range(2):
            self._copy(0, half, chunk, self.p.me, self.p.cross).start()
        for chunk in range(2):
            self._copy(1, half, chunk, self.p.me, self.p.sib).start()

    def relay(self, half, chunk):
        self._copy(0, half, chunk, self.p.cross, self.p.cross).wait_recv()
        self._copy(2, half, chunk, self.p.cross, self.p.sib).start()

    def arrived(self, half, chunk):
        self._copy(1, half, chunk, self.p.sib, self.p.sib).wait_recv()
        self._copy(2, half, chunk, self.p.diag, self.p.sib).wait_recv()

    def each(self, bodies, middle=None, after=None):
        self.relay(0, 0)

        def one(half):
            @pl.when(half == 0)
            def _():
                self.relay(0, 1)

            self.arrived(half, 0)
            bodies[0](half)

            @pl.when(half == 0)
            def _():
                self.relay(1, 0)

            if middle is not None:
                middle(half)
            self.arrived(half, 1)
            bodies[1](half)

            @pl.when(half == 0)
            def _():
                self.relay(1, 1)

            if after is not None:
                after(half)

        loop(2, one)

    def all(self):
        for half in range(2):
            for chunk in range(2):
                self.relay(half, chunk)
        for half in range(2):
            for chunk in range(2):
                self.arrived(half, chunk)

    def finish(self):
        def one(half):
            for chunk in range(2):
                self._copy(0, half, chunk, self.p.me, self.p.cross).wait_send()
                self._copy(1, half, chunk, self.p.me, self.p.sib).wait_send()
                self._copy(2, half, chunk, self.p.cross, self.p.sib).wait_send()

        loop(2, one)


class Scatter:
    def __init__(self, p, part, near, out, far, send, recv, chunks):
        self.p, self.part, self.near, self.out, self.far, self.send, self.recv = p, part, near, out, far, send, recv
        self.chunks, self.width = chunks, D // chunks

    def _near(self, kind, half, chunk):
        owner = self.p.diag if kind == 0 else self.p.sib
        cols = ds(chunk, self.width)
        return remote(
            self.part.at[owned(owner, half), cols],
            self.near.at[kind, ds(half, HR), cols],
            self.send.at[kind, half, chunk],
            self.recv.at[kind, half, chunk],
            self.p.sib,
        )

    def _far(self, half, chunk):
        cols = ds(chunk, self.width)
        return remote(
            self.out.at[ds(half, HR), cols],
            self.far.at[ds(half, HR), cols],
            self.send.at[2, half, chunk],
            self.recv.at[2, half, chunk],
            self.p.cross,
        )

    def _mid(self, half, chunk, send=True):
        self._near(0, half, chunk).wait_recv()
        cols = ds(chunk, self.width)
        total = self.part[owned(self.p.cross, half), cols] + self.near[0, ds(half, HR), cols]
        self.out[ds(half, HR), cols] = total.astype(BF16)
        if send:
            self._far(half, chunk).start()

    def mids(self, half):
        loop(self.chunks, lambda chunk: self._mid(half, chunk))

    def run(self, half, compute, unrolled=False):
        def step(chunk):
            cols = ds(chunk, self.width)
            self.part[ds(half, HS), cols] = compute(ds(half, HS), cols)
            self._near(0, half, chunk).start()
            self._near(1, half, chunk).start()

        if unrolled:
            for chunk in range(self.chunks):
                step(chunk)
        else:
            loop(self.chunks, step)

    def run_full(self, compute, send=True):
        def mids(chunk):
            self._mid(0, chunk, send)
            self._mid(1, chunk, send)

        def step(chunk):
            cols = ds(chunk, self.width)
            self.part[:, cols] = compute(cols)
            for kind in range(2):
                for half in range(2):
                    self._near(kind, half, chunk).start()

            @pl.when(chunk > 0)
            def _():
                mids(chunk - 1)

        loop(self.chunks, step)
        mids(self.chunks - 1)

    def result(self, half):
        def waits(chunk):
            self._near(1, half, chunk).wait_recv()
            self._far(half, chunk).wait_recv()

        def sent(chunk):
            self._near(0, half, chunk).wait_send()
            self._near(1, half, chunk).wait_send()
            self._far(half, chunk).wait_send()

        loop(self.chunks, waits)
        rows = ds(half, HR)
        total = self.part[owned(self.p.me, half), :] + self.near[1, rows, :] + self.far[rows, :].astype(F32)
        loop(self.chunks, sent)
        return total.astype(BF16)


    def own_sum(self, own):
        for half in range(2):
            for chunk in range(self.chunks):
                self._near(1, half, chunk).wait_recv()
            own[ds(half, HR), :] = self.part[owned(self.p.me, half), :] + self.near[1, ds(half, HR), :]
        for half in range(2):
            for chunk in range(self.chunks):
                for kind in range(2):
                    self._near(kind, half, chunk).wait_send()


def norm(h, gain):
    hf = h.astype(F32)
    inv = lax.rsqrt(jnp.mean(hf * hf, axis=-1, keepdims=True) + EPS)
    return (hf * inv * gain).astype(BF16)


def norm_back(h, gain, dy):
    hf, dyf = h.astype(F32), dy.astype(F32)
    inv = lax.rsqrt(jnp.mean(hf * hf, axis=-1, keepdims=True) + EPS)
    dgain = jnp.sum(dyf * (hf * inv), axis=0, keepdims=True)
    dn = dyf * gain
    slope = jnp.sum(dn * hf, axis=-1, keepdims=True) * (inv * inv * inv) / D
    return (dn * inv - hf * slope).astype(BF16), dgain


def softmax_scores(q, k):
    scores = dot_nt(q, k) * HEAD**-0.5
    rows = true_position(lax.broadcasted_iota(jnp.int32, (S, 1), 0))
    cols = true_position(lax.broadcasted_iota(jnp.int32, (1, S), 1))
    scores = jnp.where(rows >= cols, scores, -1e30)
    e = jnp.exp(scores - jnp.max(scores, axis=-1, keepdims=True))
    return e / jnp.sum(e, axis=-1, keepdims=True)


def head_cols(head, which):
    return ds(head * 3 + which, HEAD)


def per_head(one, together):
    def step(j):
        for i in range(together):
            one(j * together + i)

    loop(HEADS // together, step)


def attention(qkv, o, together, probs=None):
    def one(head):
        prob = softmax_scores(qkv[:, head_cols(head, 0)], qkv[:, head_cols(head, 1)])
        if probs is not None:
            probs[head] = prob
        o[:, ds(head, HEAD)] = dot(prob.astype(BF16), qkv[:, head_cols(head, 2)]).astype(BF16)

    per_head(one, together)


def half_qkv(u, wq, acc, qkv):
    def body(chunk, half):
        rows, deep = ds(half, HS), ds(chunk, D // 2)
        for j in range(NQ // 512):
            cols = ds(j, 512)
            part = dot(u[rows, deep], wq[deep, cols])
            if chunk == 0:
                acc[:, cols] = part
            else:
                qkv[rows, cols] = (acc[:, cols] + part).astype(BF16)

    return [functools.partial(body, chunk) for chunk in range(2)]


def half_mlp(n, wg, wu, acc1, acc3, last, tile):
    def body(chunk, half):
        rows, deep = ds(half, HS), ds(chunk, D // 2)

        def one(j):
            for k in range(tile // 512):
                cols = ds(j * (tile // 512) + k, 512)
                z1 = dot(n[rows, deep], wg[deep, cols])
                z3 = dot(n[rows, deep], wu[deep, cols])
                if chunk == 0:
                    acc1[:, cols] = z1
                    acc3[:, cols] = z3
                else:
                    z1 = (acc1[:, cols] + z1).astype(BF16).astype(F32)
                    z3 = (acc3[:, cols] + z3).astype(BF16).astype(F32)
                    last(rows, cols, z1, z3)

        if tile == NF:
            one(0)
        else:
            loop(NF // tile, one)

    return [functools.partial(body, chunk) for chunk in range(2)]


def forward_kernel(x, ga, gm, wq_h, wo_h, wg_h, wu_h, wd_h, h1, h2, y,
                   wq, wo, wg, wu, wd, h, u, n, acc1, acc3, qkv, o, m, part, near, out, far,
                   wsem, gsend, grecv, ssend, srecv):
    p = Peers()
    pairs = ((wq_h, wq), (wo_h, wo), (wg_h, wg), (wu_h, wu), (wd_h, wd))

    def load(i, layer):
        return pltpu.make_async_copy(pairs[i][0].at[layer], pairs[i][1], wsem.at[i])

    p.here()
    for i in range(5):
        load(i, 0).start()
    h[...] = x[...]
    gu = Gather(p, u, gsend, grecv, 0)
    gn = Gather(p, n, gsend, grecv, 1)
    scatter = Scatter(p, part, near, out, far, ssend, srecv, 2)

    def enter(half, layer):
        u[owned(p.me, half), :] = norm(h[ds(half, HR), :], ga[pl.ds(layer, 1), :])

    def add(half):
        rows = ds(half, HR)
        total = h[rows, :] + scatter.result(half)
        h[rows, :] = total
        return total

    loop(2, lambda half: enter(half, 0))
    p.ready()
    loop(2, gu.start)

    def layer_step(layer):
        more = layer < LAYERS - 1

        def refill(i):
            @pl.when(more)
            def _():
                load(i, layer + 1).start()

        load(0, layer).wait()
        gu.each(half_qkv(u, wq, acc1, qkv))
        refill(0)
        attention(qkv, o, 4)
        load(1, layer).wait()

        def project(half):
            scatter.run(half, lambda rows, cols: dot(o[rows, :], wo[:, cols]), True)
            scatter.mids(half)

        loop(2, project)
        refill(1)
        gu.finish()

        def between(half):
            n[owned(p.me, half), :] = norm(add(half), gm[pl.ds(layer, 1), :])
            gn.start(half)

        loop(2, between)

        def last(rows, cols, z1, z3):
            m[rows, cols] = (z1 * jax.nn.sigmoid(z1) * z3).astype(BF16)

        for i in (2, 3, 4):
            load(i, layer).wait()

        def send_first(half):
            @pl.when(half == 1)
            def _():
                scatter.mids(0)

        gn.each(
            half_mlp(n, wg, wu, acc1, acc3, last, NF),
            send_first,
            lambda half: scatter.run(half, lambda rows, cols: dot(m[rows, :], wd[:, cols]), True),
        )
        scatter.mids(1)
        refill(2)
        refill(3)
        refill(4)
        gn.finish()

        def leave(half):
            total = add(half)

            for i, kept in enumerate((h1, h2, y)):
                @pl.when(layer == i)
                def _():
                    kept[ds(half, HR), :] = total

            @pl.when(more)
            def _():
                enter(half, layer + 1)
                gu.start(half)

        loop(2, leave)

    loop(LAYERS, layer_step)


def finish_layer(h, gain, own, far, d_mid, rows):
    d_in = (own[rows, :] + far[rows, :].astype(F32)).astype(BF16)
    d_norm, dgain = norm_back(h[rows, :], gain, d_in)
    return d_mid[rows, :] + d_norm, dgain


def backward_kernel(layer, hin, *refs):
    first_call, last_call = layer == LAYERS - 1, layer == 0
    refs = list(refs)
    take = lambda k: [refs.pop(0) for _ in range(k)]
    if first_call:
        (dy,) = take(1)
    else:
        h_above, above_own, above_far, above_mid, gin = take(5)
    ga, gm, wq_h, wo_h, wg_h, wu_h, wd_h = take(7)
    own_out, far_out, mid_out, gout = take(4)
    saved_h = take(9)
    u, dqkv, o, da, n, dg, du, m, dd = saved = take(9)
    wq, wo, wg, wu, wd = take(5)
    hm, acc1, acc3, qkv, probs, dgated, dh, part, near, out, far, gbuf, gmid, gfar, dy_buf = take(15)
    wsem, osem, gsend, grecv, ssend, srecv, rsend, rrecv = take(8)

    p = Peers()
    pairs = ((wq_h, wq), (wo_h, wo), (wg_h, wg), (wu_h, wu), (wd_h, wd))
    loads = [pltpu.make_async_copy(src.at[layer], dst, wsem.at[i]) for i, (src, dst) in enumerate(pairs)]
    saves = [pltpu.make_async_copy(src, dst, osem.at[i]) for i, (src, dst) in enumerate(zip(saved, saved_h))]
    p.here()
    for i in (0, 1, 4, 2, 3):
        loads[i].start()
    h = hin
    gain_a, gain_m = ga[pl.ds(layer, 1), :], gm[pl.ds(layer, 1), :]
    gu, gd, gn, gda = (Gather(p, buf, gsend, grecv, i) for i, buf in enumerate((u, dd, n, da)))
    two = Scatter(p, part, near, out, far, ssend, srecv, 2)
    four = Scatter(p, part, near, out, far, ssend, srecv, 4)

    def enter(half):
        u[owned(p.me, half), :] = norm(h[ds(half, HR), :], gain_a)

    if first_call:
        gbuf[...] = jnp.zeros_like(gbuf)
    else:
        dy = dy_buf
        gbuf[...] = gin[...]

    def enter_d(half):
        rows = ds(half, HR)
        if not first_call:
            above = layer + 1
            total, dgain = finish_layer(h_above, ga[above : above + 1, :], above_own, above_far, above_mid, rows)
            dy[rows, :] = total
            gbuf[above : above + 1, :] = gbuf[above : above + 1, :] + dgain
        dd[owned(p.me, half), :] = dy[rows, :]
        gd.start(half)

    loop(2, enter)
    p.ready()
    loop(2, gu.start)
    loop(2, enter_d)

    loads[0].wait()
    gu.each(half_qkv(u, wq, acc1, qkv))
    saves[0].start()
    attention(qkv, o, 2, probs)
    saves[2].start()
    loads[1].wait()

    def project(half):
        two.run(half, lambda rows, cols: dot(o[rows, :], wo[:, cols]))
        two.mids(half)

    loop(2, project)

    gd.all()
    saves[8].start()
    loads[4].wait()

    def gated(j):
        dgated[:, ds(j, 512)] = dot_nt(dd[...], wd[ds(j, 512), :]).astype(BF16)

    loop(NF // 512, gated)

    def between(half):
        rows = ds(half, HR)
        h_mid = h[rows, :] + two.result(half)
        hm[rows, :] = h_mid
        n[owned(p.me, half), :] = norm(h_mid, gain_m)
        gn.start(half)

    loop(2, between)
    loads[2].wait()
    loads[3].wait()

    def last(rows, cols, z1, z3):
        sig = jax.nn.sigmoid(z1)
        silu = z1 * sig
        dm = dgated[rows, cols].astype(F32)
        m[rows, cols] = (silu * z3).astype(BF16)
        du[rows, cols] = (dm * silu).astype(BF16)
        dg[rows, cols] = (dm * z3 * (sig + silu * (1.0 - sig))).astype(BF16)

    gn.each(half_mlp(n, wg, wu, acc1, acc3, last, 1024))
    for i in (4, 5, 6, 7):
        saves[i].start()

    four.run_full(lambda cols: dot_nt(dg[...], wg[cols, :]) + dot_nt(du[...], wu[cols, :]))

    def mid_back(half):
        rows = ds(half, HR)
        d_norm, dgain = norm_back(hm[rows, :], gain_m, four.result(half))
        da[owned(p.me, half), :] = dy[rows, :] + d_norm
        gda.start(half)
        row = pl.ds(LAYERS + layer, 1)
        gbuf[row, :] = gbuf[row, :] + dgain

    loop(2, mid_back)
    if last_call:
        near_g = remote(gbuf, gmid, rsend.at[0], rrecv.at[0], p.sib)
        near_g.start()

    def heads(chunk, half):
        rows, deep = ds(half, HS), ds(chunk, D // 2)
        part_h = dot_nt(da[rows, deep], wo[:, deep])
        if chunk == 0:
            acc1[:, :NO] = part_h
        else:
            dh[rows, :] = (acc1[:, :NO] + part_h).astype(BF16)

    gda.each([functools.partial(heads, chunk) for chunk in range(2)])
    saves[3].start()

    def back(head):
        prob = probs[head]
        d_o = dh[:, ds(head, HEAD)]
        q, k, v = (qkv[:, head_cols(head, i)] for i in range(3))
        d_prob = dot_nt(d_o, v)
        d_scores = (prob * (d_prob - jnp.sum(d_prob * prob, axis=-1, keepdims=True)) * HEAD**-0.5).astype(BF16)
        dqkv[:, head_cols(head, 0)] = dot(d_scores, k).astype(BF16)
        dqkv[:, head_cols(head, 1)] = dot_tn(d_scores, q).astype(BF16)
        dqkv[:, head_cols(head, 2)] = dot_tn(prob.astype(BF16), d_o).astype(BF16)

    per_head(back, 4)
    saves[1].start()
    if last_call:
        near_g.wait()
        gbuf[...] = gbuf[...] + gmid[...]
        far_g = remote(gbuf, gfar, rsend.at[1], rrecv.at[1], p.cross)
        far_g.start()
    last_sum = Scatter(p, part, near, far_out, None, ssend, srecv, 4)
    last_sum.run_full(lambda cols: dot_nt(dqkv[...], wq[cols, :]), send=False)
    for half in range(2):
        mid_out[ds(half, HR), :] = da[owned(p.me, half), :]
    last_sum.own_sum(own_out)
    if last_call:
        far_g.wait()
        gout[...] = gbuf[...] + gfar[...]
    else:
        gout[...] = gbuf[...]
    for g in (gu, gd, gn, gda):
        g.finish()
    for save in saves:
        save.wait()


def closing_kernel(x, own, far, d_mid, gin, ga, dx, ga_out, gm_out, mine, others, send, recv):
    p = Peers()
    p.here(p.diag)
    mine[...] = jnp.zeros_like(mine)

    def finish(half):
        rows = ds(half, HR)
        total, dgain = finish_layer(x, ga[0:1, :], own, far, d_mid, rows)
        dx[rows, :] = total
        mine[0:1, :] = mine[0:1, :] + dgain

    loop(2, finish)
    p.ready()
    copies = [
        remote(mine, others.at[i], send.at[i], recv.at[i], peer) for i, peer in enumerate((p.cross, p.diag, p.sib))
    ]
    for copy in copies:
        copy.start()
    ga_out[1:LAYERS, :] = gin[1:LAYERS, :]
    gm_out[...] = gin[LAYERS : 2 * LAYERS, :]
    for copy in copies:
        copy.wait()
    ga_out[0:1, :] = ((mine[...] + others[2]) + (others[0] + others[1]))[0:1, :]


def wgrad_kernel(layer, n_alias, u_h, dqkv_h, o_h, da_h, n_h, dg_h, du_h, m_h, dd_h, *refs):
    refs = list(refs)
    take = lambda k: [refs.pop(0) for _ in range(k)]
    take(n_alias)
    passed = n_alias == 0
    y_in = take(1) if passed else ()
    gqkv_h, gout_h, ggate_h, gup_h, gdown_h = take(5)
    y_out = take(1) if passed else ()
    u, dqkv, lhs, rhs, gqkv, gwide, y_buf, turned = take(8)
    isem, osem, ysem = take(3)
    y_load = [pltpu.make_async_copy(y, y_buf, ysem.at[0]) for y in y_in]
    y_save = [pltpu.make_async_copy(y_buf, y, ysem.at[1]) for y in y_out]
    sources = (n_h, dg_h, du_h, m_h, dd_h, o_h, da_h, u_h, dqkv_h)
    targets = (lhs.at[0], rhs.at[0], rhs.at[1], lhs.at[1], rhs.at[2], lhs.at[2, :, :NO], rhs.at[3], u, dqkv)
    loads = [pltpu.make_async_copy(src, dst, isem.at[i]) for i, (src, dst) in enumerate(zip(sources, targets))]
    for load in loads + y_load:
        load.start()

    def pair(a, b, stage, i, following, j):
        for k in range(2):
            for c in range(b.shape[1] // 512):
                stage[ds(2 * i + k, S), ds(c, 512)] = dot(turned[k], b[:, ds(c, 512)]).astype(BF16)
            if k == 0:
                turned[1] = a[:, ds(2 * i + 1, S)].T
            else:
                turned[0] = following[:, ds(2 * j, S)].T

    def copy(stage, out, i, sem):
        return pltpu.make_async_copy(stage.at[ds(i, 2 * S), :], out.at[layer, ds(i, 2 * S), :], sem)

    wide_outs = (ggate_h, gup_h, gdown_h, gout_h)
    loads[0].wait()
    loads[1].wait()

    turned[0] = lhs[0, :, :S].T

    def wide(step):
        which, i = step // 4, lax.rem(step, 4)
        after = jnp.minimum(step + 1, 12)
        for at, needed in ((3, loads[2:3]), (7, loads[3:5]), (11, loads[5:7])):
            @pl.when(step == at)
            def _():
                for load in needed:
                    load.wait()

        stage = gwide.at[which]
        left = lhs.at[jnp.maximum(which - 1, 0)]
        pair(left, rhs.at[which], stage, i, lhs.at[jnp.maximum(after // 4 - 1, 0)], lax.rem(after, 4))
        for k, out in enumerate(wide_outs):
            @pl.when(which == k)
            def _():
                copy(stage, out, i if k < 3 else 0, osem.at[k, i]).start()

    loop(13, wide)
    for load in loads[7:] + y_load:
        load.wait()
    for save in y_save:
        save.start()

    turned[0] = u[:, :S].T

    def qkv(i):
        pair(u, dqkv, gqkv, i, u, jnp.minimum(i + 1, 3))
        copy(gqkv, gqkv_h, i, osem.at[4, i]).start()

    loop(4, qkv)
    for i in range(4):
        for k, out in enumerate(wide_outs[:3]):
            copy(gwide.at[k], out, i, osem.at[k, i]).wait()
        copy(gqkv, gqkv_h, i, osem.at[4, i]).wait()
    copy(gwide.at[3], gout_h, 0, osem.at[3, 0]).wait()
    for save in y_save:
        save.wait()


def vmem():
    return pl.BlockSpec(memory_space=pltpu.VMEM)


def hbm():
    return pl.BlockSpec(memory_space=pltpu.HBM)


WEIGHT_SCRATCH = [
    pltpu.VMEM((D, NQ), BF16),
    pltpu.VMEM((NO, D), BF16),
    pltpu.VMEM((D, NF), BF16),
    pltpu.VMEM((D, NF), BF16),
    pltpu.VMEM((NF, D), BF16),
]
SCATTER_SCRATCH = [
    pltpu.VMEM((S, D), F32),
    pltpu.VMEM((2, R, D), F32),
    pltpu.VMEM((R, D), BF16),
    pltpu.VMEM((R, D), BF16),
]
SAVED = [(S, D), (S, NQ), (S, NO), (S, D), (S, D), (S, NF), (S, NF), (S, NF), (S, D)]
GRADS = [(D, NQ), (NO, D), (D, NF), (D, NF), (NF, D)]


def run_forward(x, ga, gm, weights):
    dma = pltpu.SemaphoreType.DMA
    return pl.pallas_call(
        forward_kernel,
        name="forward",
        out_shape=[jax.ShapeDtypeStruct((R, D), BF16)] * 3,
        in_specs=[vmem()] * 3 + [hbm()] * 5,
        out_specs=[vmem()] * 3,
        scratch_shapes=WEIGHT_SCRATCH
        + [
            pltpu.VMEM((R, D), BF16),
            pltpu.VMEM((S, D), BF16),
            pltpu.VMEM((S, D), BF16),
            pltpu.VMEM((HS, NF), F32),
            pltpu.VMEM((HS, NF), F32),
            pltpu.VMEM((S, NQ), BF16),
            pltpu.VMEM((S, NO), BF16),
            pltpu.VMEM((S, NF), BF16),
        ]
        + SCATTER_SCRATCH
        + [dma((5,)), dma((2, 3, 2, 2)), dma((2, 3, 2, 2)), dma((3, 2, 2)), dma((3, 2, 2))],
        compiler_params=pltpu.CompilerParams(collective_id=0, has_side_effects=True, vmem_limit_bytes=VMEM_LIMIT),
    )(x, ga, gm, *weights)


def run_backward(layer, hin, above, ga, gm, weights):
    dma = pltpu.SemaphoreType.DMA
    results = [((R, D), F32), ((R, D), BF16), ((R, D), BF16), ((8, D), F32)] + [(shape, BF16) for shape in SAVED]
    outs = pl.pallas_call(
        functools.partial(backward_kernel, layer),
        name=f"backward{layer}",
        out_shape=[jax.ShapeDtypeStruct(*result) for result in results],
        in_specs=[vmem()] * (3 + len(above)) + [hbm()] * 5,
        out_specs=[vmem()] * 4 + [hbm()] * 9,
        scratch_shapes=[pltpu.VMEM(shape, BF16) for shape in SAVED]
        + WEIGHT_SCRATCH
        + [
            pltpu.VMEM((R, D), BF16),
            pltpu.VMEM((HS, NF), F32),
            pltpu.VMEM((HS, NF), F32),
            pltpu.VMEM((S, NQ), BF16),
            pltpu.VMEM((HEADS, S, S), F32),
            pltpu.VMEM((S, NF), BF16),
            pltpu.VMEM((S, NO), BF16),
        ]
        + SCATTER_SCRATCH
        + [pltpu.VMEM((8, D), F32)] * 3
        + [pltpu.VMEM((R, D), BF16)]
        + [dma((5,)), dma((9,)), dma((4, 3, 2, 2)), dma((4, 3, 2, 2)), dma((3, 2, 4)), dma((3, 2, 4)), dma((2,)), dma((2,))],
        compiler_params=pltpu.CompilerParams(
            collective_id=1 + layer, has_side_effects=True, vmem_limit_bytes=VMEM_LIMIT
        ),
    )(hin, *above, ga, gm, *weights)
    return outs[:4], outs[4:]


def run_closing(above, ga):
    dma = pltpu.SemaphoreType.DMA
    return pl.pallas_call(
        closing_kernel,
        name="closing",
        out_shape=[jax.ShapeDtypeStruct((R, D), BF16)] + [jax.ShapeDtypeStruct((LAYERS, D), F32)] * 2,
        in_specs=[vmem()] * 6,
        out_specs=[vmem()] * 3,
        scratch_shapes=[pltpu.VMEM((8, D), F32), pltpu.VMEM((3, 8, D), F32), dma((3,)), dma((3,))],
        compiler_params=pltpu.CompilerParams(
            collective_id=1 + LAYERS, has_side_effects=True, vmem_limit_bytes=8_000_000
        ),
    )(*above, ga)


def run_wgrad(layer, saved, grads, y):
    dma = pltpu.SemaphoreType.DMA
    n_alias = len(grads)
    return pl.pallas_call(
        functools.partial(wgrad_kernel, layer, n_alias),
        name=f"wgrad{layer}",
        out_shape=[jax.ShapeDtypeStruct((LAYERS, *shape), BF16) for shape in GRADS]
        + [jax.ShapeDtypeStruct((R, D), BF16)] * len(y),
        in_specs=[hbm()] * (9 + n_alias + len(y)),
        out_specs=[hbm()] * (5 + len(y)),
        input_output_aliases={9 + i: i for i in range(n_alias)},
        scratch_shapes=[pltpu.VMEM(shape, BF16) for shape in SAVED[:2]]
        + [pltpu.VMEM(shape, BF16) for shape in ((3, S, D), (4, S, D), GRADS[0], (4, D, D), (R, D), (2, S, S))]
        + [dma((9,)), dma((5, 4)), dma((2,))],
        compiler_params=pltpu.CompilerParams(vmem_limit_bytes=VMEM_LIMIT if layer > 0 else 65_600_000),
        cost_estimate=pl.CostEstimate(flops=8_600_000_000, bytes_accessed=42_000_000, transcendentals=0),
    )(*saved, *grads, *y)


def solution(mesh):
    row_spec = P(("dp", "tp"), None)
    col_spec = P(None, None, "tp")
    mid_spec = P(None, "tp", None)
    in_specs = (row_spec, row_spec, P(None, None), P(None, None), col_spec, mid_spec, col_spec, col_spec, mid_spec)
    out_specs = (
        row_spec, row_spec, P("dp", None, "tp"), P("dp", "tp", None), P("dp", None, "tp"), P("dp", None, "tp"),
        P("dp", "tp", None), P("dp", None), P("dp", None),
    )

    def device_step(x, grad_y, gain_attn, gain_mlp, w_qkv, w_out, w_gate, w_up, w_down):
        weights = (w_qkv, w_out, w_gate, w_up, w_down)
        h1, h2, y = run_forward(x, gain_attn, gain_mlp, weights)
        kept, above = (x, h1, h2), (grad_y,)
        grads = ()
        for layer in reversed(range(LAYERS)):
            (own, chip_sum, d_mid, gains), saved = run_backward(
                layer, kept[layer], above, gain_attn, gain_mlp, weights
            )
            far = lax.ppermute(chip_sum, "tp", [(0, 2), (1, 3), (2, 0), (3, 1)])
            grads = run_wgrad(layer, saved, grads, () if grads else (y,))
            if len(grads) > len(GRADS):
                *grads, y = grads
            far, grads = lax.optimization_barrier((far, tuple(grads)))
            above = (kept[layer], own, far, d_mid, gains)
        grad_x, *gains = run_closing(above, gain_attn)
        return (y, grad_x, *grads, *gains)

    return jax.shard_map(device_step, mesh=mesh, in_specs=in_specs, out_specs=out_specs, check_vma=False)
```

```python
import functools

import jax
import jax.numpy as jnp
from jax import lax
from jax.experimental import pallas as pl
from jax.experimental.pallas import tpu as pltpu
from jax.sharding import PartitionSpec as P

HEAD = 128
EPS = 1e-5
MESH = pl.DeviceIdType.MESH
F32 = jnp.float32
BF16 = jnp.bfloat16
VMEM_LIMIT = 67_000_000

D = 2048
S = 256
R = 64
NQ = 1536
NO = 512
NF = 2048
HEADS = 4
LAYERS = 3

HR = R // 2
HS = S // 2


def dot(a, b):
    return jnp.dot(a, b, preferred_element_type=F32)


def dot_nt(a, b):
    return lax.dot_general(a, b, (((1,), (1,)), ((), ())), preferred_element_type=F32)


def dot_tn(a, b):
    return lax.dot_general(a, b, (((0,), (0,)), ((), ())), preferred_element_type=F32)


def ds(i, n):
    return pl.ds(i * n if isinstance(i, int) else pl.multiple_of(i * n, n), n)


def loop(n, body):
    lax.fori_loop(0, n, lambda i, c: (body(i), c)[1], 0)


class Peers:
    def __init__(self):
        self.me = lax.axis_index("tp")
        core, chip = lax.rem(self.me, 2), self.me // 2
        self.sib = chip * 2 + (1 - core)
        self.cross = (1 - chip) * 2 + core
        self.diag = (1 - chip) * 2 + (1 - core)

    def here(self, *more):
        self.partners = 2 + len(more)
        for peer in (self.sib, self.cross, *more):
            pl.semaphore_signal(pltpu.get_barrier_semaphore(), inc=1, device_id={"tp": peer}, device_id_type=MESH)

    def ready(self):
        pl.semaphore_wait(pltpu.get_barrier_semaphore(), self.partners)


def remote(src, dst, send, recv, peer):
    return pltpu.make_async_remote_copy(
        src_ref=src, dst_ref=dst, send_sem=send, recv_sem=recv, device_id={"tp": peer}, device_id_type=MESH
    )


def owned(owner, half):
    return ds(half * 4 + owner, HR)


def true_position(row):
    return lax.rem(row, HS) // HR * R + row // HS * HR + lax.rem(row, HR)


class Gather:
    def __init__(self, p, buf, send, recv, which):
        self.p, self.buf, self.send, self.recv, self.which = p, buf, send, recv, which

    def _copy(self, kind, half, chunk, owner, peer):
        part = self.buf.at[owned(owner, half), ds(chunk, D // 2)]
        sems = (self.which, kind, half, chunk)
        return remote(part, part, self.send.at[sems], self.recv.at[sems], peer)

    def start(self, half):
        for chunk in range(2):
            self._copy(0, half, chunk, self.p.me, self.p.cross).start()
        for chunk in range(2):
            self._copy(1, half, chunk, self.p.me, self.p.sib).start()

    def relay(self, half, chunk):
        self._copy(0, half, chunk, self.p.cross, self.p.cross).wait_recv()
        self._copy(2, half, chunk, self.p.cross, self.p.sib).start()

    def arrived(self, half, chunk):
        self._copy(1, half, chunk, self.p.sib, self.p.sib).wait_recv()
        self._copy(2, half, chunk, self.p.diag, self.p.sib).wait_recv()

    def each(self, bodies, middle=None, after=None):
        self.relay(0, 0)

        def one(half):
            @pl.when(half == 0)
            def _():
                self.relay(0, 1)

            self.arrived(half, 0)
            bodies[0](half)

            @pl.when(half == 0)
            def _():
                self.relay(1, 0)

            if middle is not None:
                middle(half)
            self.arrived(half, 1)
            bodies[1](half)

            @pl.when(half == 0)
            def _():
                self.relay(1, 1)

            if after is not None:
                after(half)

        loop(2, one)

    def all(self):
        for half in range(2):
            for chunk in range(2):
                self.relay(half, chunk)
        for half in range(2):
            for chunk in range(2):
                self.arrived(half, chunk)

    def finish(self):
        def one(half):
            for chunk in range(2):
                self._copy(0, half, chunk, self.p.me, self.p.cross).wait_send()
                self._copy(1, half, chunk, self.p.me, self.p.sib).wait_send()
                self._copy(2, half, chunk, self.p.cross, self.p.sib).wait_send()

        loop(2, one)


class Scatter:
    def __init__(self, p, part, near, out, far, send, recv, chunks):
        self.p, self.part, self.near, self.out, self.far, self.send, self.recv = p, part, near, out, far, send, recv
        self.chunks, self.width = chunks, D // chunks

    def _near(self, kind, half, chunk):
        owner = self.p.diag if kind == 0 else self.p.sib
        cols = ds(chunk, self.width)
        return remote(
            self.part.at[owned(owner, half), cols],
            self.near.at[kind, ds(half, HR), cols],
            self.send.at[kind, half, chunk],
            self.recv.at[kind, half, chunk],
            self.p.sib,
        )

    def _far(self, half, chunk):
        cols = ds(chunk, self.width)
        return remote(
            self.out.at[ds(half, HR), cols],
            self.far.at[ds(half, HR), cols],
            self.send.at[2, half, chunk],
            self.recv.at[2, half, chunk],
            self.p.cross,
        )

    def _mid(self, half, chunk, send=True):
        self._near(0, half, chunk).wait_recv()
        cols = ds(chunk, self.width)
        total = self.part[owned(self.p.cross, half), cols] + self.near[0, ds(half, HR), cols]
        self.out[ds(half, HR), cols] = total.astype(BF16)
        if send:
            self._far(half, chunk).start()

    def mids(self, half):
        loop(self.chunks, lambda chunk: self._mid(half, chunk))

    def run(self, half, compute, unrolled=False):
        def step(chunk):
            cols = ds(chunk, self.width)
            self.part[ds(half, HS), cols] = compute(ds(half, HS), cols)
            self._near(0, half, chunk).start()
            self._near(1, half, chunk).start()

        if unrolled:
            for chunk in range(self.chunks):
                step(chunk)
        else:
            loop(self.chunks, step)

    def run_full(self, compute, send=True):
        def mids(chunk):
            self._mid(0, chunk, send)
            self._mid(1, chunk, send)

        def step(chunk):
            cols = ds(chunk, self.width)
            self.part[:, cols] = compute(cols)
            for kind in range(2):
                for half in range(2):
                    self._near(kind, half, chunk).start()

            @pl.when(chunk > 0)
            def _():
                mids(chunk - 1)

        loop(self.chunks, step)
        mids(self.chunks - 1)

    def result(self, half):
        def waits(chunk):
            self._near(1, half, chunk).wait_recv()
            self._far(half, chunk).wait_recv()

        def sent(chunk):
            self._near(0, half, chunk).wait_send()
            self._near(1, half, chunk).wait_send()
            self._far(half, chunk).wait_send()

        loop(self.chunks, waits)
        rows = ds(half, HR)
        total = self.part[owned(self.p.me, half), :] + self.near[1, rows, :] + self.far[rows, :].astype(F32)
        loop(self.chunks, sent)
        return total.astype(BF16)


    def own_sum(self, own):
        for half in range(2):
            for chunk in range(self.chunks):
                self._near(1, half, chunk).wait_recv()
            own[ds(half, HR), :] = self.part[owned(self.p.me, half), :] + self.near[1, ds(half, HR), :]
        for half in range(2):
            for chunk in range(self.chunks):
                for kind in range(2):
                    self._near(kind, half, chunk).wait_send()


def norm(h, gain):
    hf = h.astype(F32)
    inv = lax.rsqrt(jnp.mean(hf * hf, axis=-1, keepdims=True) + EPS)
    return (hf * inv * gain).astype(BF16)


def norm_back(h, gain, dy):
    hf, dyf = h.astype(F32), dy.astype(F32)
    inv = lax.rsqrt(jnp.mean(hf * hf, axis=-1, keepdims=True) + EPS)
    dgain = jnp.sum(dyf * (hf * inv), axis=0, keepdims=True)
    dn = dyf * gain
    slope = jnp.sum(dn * hf, axis=-1, keepdims=True) * (inv * inv * inv) / D
    return (dn * inv - hf * slope).astype(BF16), dgain


def softmax_scores(q, k):
    scores = dot_nt(q, k) * HEAD**-0.5
    rows = true_position(lax.broadcasted_iota(jnp.int32, (S, 1), 0))
    cols = true_position(lax.broadcasted_iota(jnp.int32, (1, S), 1))
    scores = jnp.where(rows >= cols, scores, -1e30)
    e = jnp.exp(scores - jnp.max(scores, axis=-1, keepdims=True))
    return e / jnp.sum(e, axis=-1, keepdims=True)


def head_cols(head, which):
    return ds(head * 3 + which, HEAD)


def per_head(one, together):
    def step(j):
        for i in range(together):
            one(j * together + i)

    loop(HEADS // together, step)


def attention(qkv, o, together, probs=None):
    def one(head):
        prob = softmax_scores(qkv[:, head_cols(head, 0)], qkv[:, head_cols(head, 1)])
        if probs is not None:
            probs[head] = prob
        o[:, ds(head, HEAD)] = dot(prob.astype(BF16), qkv[:, head_cols(head, 2)]).astype(BF16)

    per_head(one, together)


def half_qkv(u, wq, acc, qkv):
    def body(chunk, half):
        rows, deep = ds(half, HS), ds(chunk, D // 2)
        for j in range(NQ // 512):
            cols = ds(j, 512)
            part = dot(u[rows, deep], wq[deep, cols])
            if chunk == 0:
                acc[:, cols] = part
            else:
                qkv[rows, cols] = (acc[:, cols] + part).astype(BF16)

    return [functools.partial(body, chunk) for chunk in range(2)]


def half_mlp(n, wg, wu, acc1, acc3, last, tile):
    def body(chunk, half):
        rows, deep = ds(half, HS), ds(chunk, D // 2)

        def one(j):
            for k in range(tile // 512):
                cols = ds(j * (tile // 512) + k, 512)
                z1 = dot(n[rows, deep], wg[deep, cols])
                z3 = dot(n[rows, deep], wu[deep, cols])
                if chunk == 0:
                    acc1[:, cols] = z1
                    acc3[:, cols] = z3
                else:
                    z1 = (acc1[:, cols] + z1).astype(BF16).astype(F32)
                    z3 = (acc3[:, cols] + z3).astype(BF16).astype(F32)
                    last(rows, cols, z1, z3)

        if tile == NF:
            one(0)
        else:
            loop(NF // tile, one)

    return [functools.partial(body, chunk) for chunk in range(2)]


def forward_kernel(x, ga, gm, wq_h, wo_h, wg_h, wu_h, wd_h, h1, h2, y,
                   wq, wo, wg, wu, wd, h, u, n, acc1, acc3, qkv, o, m, part, near, out, far,
                   wsem, gsend, grecv, ssend, srecv):
    p = Peers()
    pairs = ((wq_h, wq), (wo_h, wo), (wg_h, wg), (wu_h, wu), (wd_h, wd))

    def load(i, layer):
        return pltpu.make_async_copy(pairs[i][0].at[layer], pairs[i][1], wsem.at[i])

    p.here()
    for i in range(5):
        load(i, 0).start()
    h[...] = x[...]
    gu = Gather(p, u, gsend, grecv, 0)
    gn = Gather(p, n, gsend, grecv, 1)
    scatter = Scatter(p, part, near, out, far, ssend, srecv, 2)

    def enter(half, layer):
        u[owned(p.me, half), :] = norm(h[ds(half, HR), :], ga[pl.ds(layer, 1), :])

    def add(half):
        rows = ds(half, HR)
        total = h[rows, :] + scatter.result(half)
        h[rows, :] = total
        return total

    loop(2, lambda half: enter(half, 0))
    p.ready()
    loop(2, gu.start)

    def layer_step(layer):
        more = layer < LAYERS - 1

        def refill(i):
            @pl.when(more)
            def _():
                load(i, layer + 1).start()

        load(0, layer).wait()
        gu.each(half_qkv(u, wq, acc1, qkv))
        refill(0)
        attention(qkv, o, 4)
        load(1, layer).wait()

        def project(half):
            scatter.run(half, lambda rows, cols: dot(o[rows, :], wo[:, cols]), True)
            scatter.mids(half)

        loop(2, project)
        refill(1)
        gu.finish()

        def between(half):
            n[owned(p.me, half), :] = norm(add(half), gm[pl.ds(layer, 1), :])
            gn.start(half)

        loop(2, between)

        def last(rows, cols, z1, z3):
            m[rows, cols] = (z1 * jax.nn.sigmoid(z1) * z3).astype(BF16)

        for i in (2, 3, 4):
            load(i, layer).wait()

        def send_first(half):
            @pl.when(half == 1)
            def _():
                scatter.mids(0)

        gn.each(
            half_mlp(n, wg, wu, acc1, acc3, last, NF),
            send_first,
            lambda half: scatter.run(half, lambda rows, cols: dot(m[rows, :], wd[:, cols]), True),
        )
        scatter.mids(1)
        refill(2)
        refill(3)
        refill(4)
        gn.finish()

        def leave(half):
            total = add(half)

            for i, kept in enumerate((h1, h2, y)):
                @pl.when(layer == i)
                def _():
                    kept[ds(half, HR), :] = total

            @pl.when(more)
            def _():
                enter(half, layer + 1)
                gu.start(half)

        loop(2, leave)

    loop(LAYERS, layer_step)


def finish_layer(h, gain, own, far, d_mid, rows):
    d_in = (own[rows, :] + far[rows, :].astype(F32)).astype(BF16)
    d_norm, dgain = norm_back(h[rows, :], gain, d_in)
    return d_mid[rows, :] + d_norm, dgain


def backward_kernel(layer, hin, *refs):
    first_call, last_call = layer == LAYERS - 1, layer == 0
    refs = list(refs)
    take = lambda k: [refs.pop(0) for _ in range(k)]
    above_h = take(1 if first_call else 5)
    ga_h, gm_h, wq_h, wo_h, wg_h, wu_h, wd_h = take(7)
    own_out, far_out, mid_out, gout = take(4)
    saved_h = take(9)
    u, dqkv, o, da, n, dg, du, m, dd = saved = take(9)
    wq, wo, wg, wu, wd = take(5)
    hm, acc1, acc3, qkv, probs, dgated, dh, part, near, out, far, gbuf, gmid, gfar, dy = take(15)
    h, ga, gm, h_above, above_own, above_far, above_mid, isem = take(8)
    wsem, osem, gsend, grecv, ssend, srecv, rsend, rrecv = take(8)

    p = Peers()
    pairs = ((wq_h, wq), (wo_h, wo), (wg_h, wg), (wu_h, wu), (wd_h, wd))
    loads = [pltpu.make_async_copy(src.at[layer], dst, wsem.at[i]) for i, (src, dst) in enumerate(pairs)]
    saves = [pltpu.make_async_copy(src, dst, osem.at[i]) for i, (src, dst) in enumerate(zip(saved, saved_h))]
    p.here()
    held = (dy,) if first_call else (h_above, above_own, above_far, above_mid, gbuf)
    inputs = [
        pltpu.make_async_copy(src, dst, isem.at[i])
        for i, (src, dst) in enumerate(zip((hin, ga_h, gm_h, *above_h), (h, ga, gm, *held)))
    ]
    for copy in inputs:
        copy.start()
    for i in (0, 1, 4, 2, 3):
        loads[i].start()
    if first_call:
        gbuf[...] = jnp.zeros_like(gbuf)
    for copy in inputs[:3]:
        copy.wait()
    gain_a, gain_m = ga[pl.ds(layer, 1), :], gm[pl.ds(layer, 1), :]
    gu, gd, gn, gda = (Gather(p, buf, gsend, grecv, i) for i, buf in enumerate((u, dd, n, da)))
    two = Scatter(p, part, near, out, far, ssend, srecv, 2)
    four = Scatter(p, part, near, out, far, ssend, srecv, 4)

    def enter(half):
        u[owned(p.me, half), :] = norm(h[ds(half, HR), :], gain_a)

    def enter_d(half):
        rows = ds(half, HR)
        if not first_call:
            above = layer + 1
            total, dgain = finish_layer(h_above, ga[above : above + 1, :], above_own, above_far, above_mid, rows)
            dy[rows, :] = total
            gbuf[above : above + 1, :] = gbuf[above : above + 1, :] + dgain
        dd[owned(p.me, half), :] = dy[rows, :]
        gd.start(half)

    loop(2, enter)
    p.ready()
    loop(2, gu.start)
    for copy in inputs[3:]:
        copy.wait()
    loop(2, enter_d)

    loads[0].wait()
    gu.each(half_qkv(u, wq, acc1, qkv))
    saves[0].start()
    attention(qkv, o, 2, probs)
    saves[2].start()
    loads[1].wait()

    def project(half):
        two.run(half, lambda rows, cols: dot(o[rows, :], wo[:, cols]))
        two.mids(half)

    loop(2, project)

    gd.all()
    saves[8].start()
    loads[4].wait()

    def gated(j):
        dgated[:, ds(j, 512)] = dot_nt(dd[...], wd[ds(j, 512), :]).astype(BF16)

    loop(NF // 512, gated)

    def between(half):
        rows = ds(half, HR)
        h_mid = h[rows, :] + two.result(half)
        hm[rows, :] = h_mid
        n[owned(p.me, half), :] = norm(h_mid, gain_m)
        gn.start(half)

    loop(2, between)
    loads[2].wait()
    loads[3].wait()

    def last(rows, cols, z1, z3):
        sig = jax.nn.sigmoid(z1)
        silu = z1 * sig
        dm = dgated[rows, cols].astype(F32)
        m[rows, cols] = (silu * z3).astype(BF16)
        du[rows, cols] = (dm * silu).astype(BF16)
        dg[rows, cols] = (dm * z3 * (sig + silu * (1.0 - sig))).astype(BF16)

    gn.each(half_mlp(n, wg, wu, acc1, acc3, last, 1024))
    for i in (4, 5, 6, 7):
        saves[i].start()

    four.run_full(lambda cols: dot_nt(dg[...], wg[cols, :]) + dot_nt(du[...], wu[cols, :]))

    def mid_back(half):
        rows = ds(half, HR)
        d_norm, dgain = norm_back(hm[rows, :], gain_m, four.result(half))
        da[owned(p.me, half), :] = dy[rows, :] + d_norm
        gda.start(half)
        row = pl.ds(LAYERS + layer, 1)
        gbuf[row, :] = gbuf[row, :] + dgain

    loop(2, mid_back)
    if last_call:
        near_g = remote(gbuf, gmid, rsend.at[0], rrecv.at[0], p.sib)
        near_g.start()

    def heads(chunk, half):
        rows, deep = ds(half, HS), ds(chunk, D // 2)
        part_h = dot_nt(da[rows, deep], wo[:, deep])
        if chunk == 0:
            acc1[:, :NO] = part_h
        else:
            dh[rows, :] = (acc1[:, :NO] + part_h).astype(BF16)

    gda.each([functools.partial(heads, chunk) for chunk in range(2)])
    saves[3].start()

    def back(head):
        prob = probs[head]
        d_o = dh[:, ds(head, HEAD)]
        q, k, v = (qkv[:, head_cols(head, i)] for i in range(3))
        d_prob = dot_nt(d_o, v)
        d_scores = (prob * (d_prob - jnp.sum(d_prob * prob, axis=-1, keepdims=True)) * HEAD**-0.5).astype(BF16)
        dqkv[:, head_cols(head, 0)] = dot(d_scores, k).astype(BF16)
        dqkv[:, head_cols(head, 1)] = dot_tn(d_scores, q).astype(BF16)
        dqkv[:, head_cols(head, 2)] = dot_tn(prob.astype(BF16), d_o).astype(BF16)

    per_head(back, 4)
    saves[1].start()
    if last_call:
        near_g.wait()
        gbuf[...] = gbuf[...] + gmid[...]
        far_g = remote(gbuf, gfar, rsend.at[1], rrecv.at[1], p.cross)
        far_g.start()
    last_sum = Scatter(p, part, near, far_out, None, ssend, srecv, 4)
    last_sum.run_full(lambda cols: dot_nt(dqkv[...], wq[cols, :]), send=False)
    for half in range(2):
        mid_out[ds(half, HR), :] = da[owned(p.me, half), :]
    last_sum.own_sum(own_out)
    if last_call:
        far_g.wait()
        gout[...] = gbuf[...] + gfar[...]
    else:
        gout[...] = gbuf[...]
    for g in (gu, gd, gn, gda):
        g.finish()
    for save in saves:
        save.wait()


def closing_kernel(x, own, far, d_mid, gin, ga, dx, ga_out, gm_out, mine, others, send, recv):
    p = Peers()
    p.here(p.diag)
    mine[...] = jnp.zeros_like(mine)

    def finish(half):
        rows = ds(half, HR)
        total, dgain = finish_layer(x, ga[0:1, :], own, far, d_mid, rows)
        dx[rows, :] = total
        mine[0:1, :] = mine[0:1, :] + dgain

    loop(2, finish)
    p.ready()
    copies = [
        remote(mine, others.at[i], send.at[i], recv.at[i], peer) for i, peer in enumerate((p.cross, p.diag, p.sib))
    ]
    for copy in copies:
        copy.start()
    ga_out[1:LAYERS, :] = gin[1:LAYERS, :]
    gm_out[...] = gin[LAYERS : 2 * LAYERS, :]
    for copy in copies:
        copy.wait()
    ga_out[0:1, :] = ((mine[...] + others[2]) + (others[0] + others[1]))[0:1, :]


def wgrad_kernel(layer, n_alias, u_h, dqkv_h, o_h, da_h, n_h, dg_h, du_h, m_h, dd_h, *refs):
    refs = list(refs)
    take = lambda k: [refs.pop(0) for _ in range(k)]
    take(n_alias)
    passed = n_alias == 0
    y_in = take(1) if passed else ()
    gqkv_h, gout_h, ggate_h, gup_h, gdown_h = take(5)
    y_out = take(1) if passed else ()
    u, dqkv, lhs, rhs, gqkv, gwide, y_buf, turned = take(8)
    isem, osem, ysem = take(3)
    y_load = [pltpu.make_async_copy(y, y_buf, ysem.at[0]) for y in y_in]
    y_save = [pltpu.make_async_copy(y_buf, y, ysem.at[1]) for y in y_out]
    sources = (n_h, dg_h, du_h, m_h, dd_h, o_h, da_h, u_h, dqkv_h)
    targets = (lhs.at[0], rhs.at[0], rhs.at[1], lhs.at[1], rhs.at[2], lhs.at[2, :, :NO], rhs.at[3], u, dqkv)
    loads = [pltpu.make_async_copy(src, dst, isem.at[i]) for i, (src, dst) in enumerate(zip(sources, targets))]
    for load in loads + y_load:
        load.start()

    def pair(a, b, stage, i, following, j):
        for k in range(2):
            for c in range(b.shape[1] // 512):
                stage[ds(2 * i + k, S), ds(c, 512)] = dot(turned[k], b[:, ds(c, 512)]).astype(BF16)
            if k == 0:
                turned[1] = a[:, ds(2 * i + 1, S)].T
            else:
                turned[0] = following[:, ds(2 * j, S)].T

    def copy(stage, out, i, sem):
        return pltpu.make_async_copy(stage.at[ds(i, 2 * S), :], out.at[layer, ds(i, 2 * S), :], sem)

    wide_outs = (ggate_h, gup_h, gdown_h, gout_h)
    loads[0].wait()
    loads[1].wait()

    turned[0] = lhs[0, :, :S].T

    def wide(step):
        which, i = step // 4, lax.rem(step, 4)
        after = jnp.minimum(step + 1, 12)
        for at, needed in ((3, loads[2:3]), (7, loads[3:5]), (11, loads[5:7])):
            @pl.when(step == at)
            def _():
                for load in needed:
                    load.wait()

        stage = gwide.at[which]
        left = lhs.at[jnp.maximum(which - 1, 0)]
        pair(left, rhs.at[which], stage, i, lhs.at[jnp.maximum(after // 4 - 1, 0)], lax.rem(after, 4))
        for k, out in enumerate(wide_outs):
            @pl.when(which == k)
            def _():
                copy(stage, out, i if k < 3 else 0, osem.at[k, i]).start()

    loop(13, wide)
    for load in loads[7:] + y_load:
        load.wait()
    for save in y_save:
        save.start()

    turned[0] = u[:, :S].T

    def qkv(i):
        pair(u, dqkv, gqkv, i, u, jnp.minimum(i + 1, 3))
        copy(gqkv, gqkv_h, i, osem.at[4, i]).start()

    loop(4, qkv)
    for i in range(4):
        for k, out in enumerate(wide_outs[:3]):
            copy(gwide.at[k], out, i, osem.at[k, i]).wait()
        copy(gqkv, gqkv_h, i, osem.at[4, i]).wait()
    copy(gwide.at[3], gout_h, 0, osem.at[3, 0]).wait()
    for save in y_save:
        save.wait()


def vmem():
    return pl.BlockSpec(memory_space=pltpu.VMEM)


def hbm():
    return pl.BlockSpec(memory_space=pltpu.HBM)


WEIGHT_SCRATCH = [
    pltpu.VMEM((D, NQ), BF16),
    pltpu.VMEM((NO, D), BF16),
    pltpu.VMEM((D, NF), BF16),
    pltpu.VMEM((D, NF), BF16),
    pltpu.VMEM((NF, D), BF16),
]
SCATTER_SCRATCH = [
    pltpu.VMEM((S, D), F32),
    pltpu.VMEM((2, R, D), F32),
    pltpu.VMEM((R, D), BF16),
    pltpu.VMEM((R, D), BF16),
]
SAVED = [(S, D), (S, NQ), (S, NO), (S, D), (S, D), (S, NF), (S, NF), (S, NF), (S, D)]
GRADS = [(D, NQ), (NO, D), (D, NF), (D, NF), (NF, D)]


def run_forward(x, ga, gm, weights):
    dma = pltpu.SemaphoreType.DMA
    return pl.pallas_call(
        forward_kernel,
        name="forward",
        out_shape=[jax.ShapeDtypeStruct((R, D), BF16)] * 3,
        in_specs=[vmem()] * 3 + [hbm()] * 5,
        out_specs=[vmem()] * 3,
        scratch_shapes=WEIGHT_SCRATCH
        + [
            pltpu.VMEM((R, D), BF16),
            pltpu.VMEM((S, D), BF16),
            pltpu.VMEM((S, D), BF16),
            pltpu.VMEM((HS, NF), F32),
            pltpu.VMEM((HS, NF), F32),
            pltpu.VMEM((S, NQ), BF16),
            pltpu.VMEM((S, NO), BF16),
            pltpu.VMEM((S, NF), BF16),
        ]
        + SCATTER_SCRATCH
        + [dma((5,)), dma((2, 3, 2, 2)), dma((2, 3, 2, 2)), dma((3, 2, 2)), dma((3, 2, 2))],
        compiler_params=pltpu.CompilerParams(collective_id=0, has_side_effects=True, vmem_limit_bytes=VMEM_LIMIT),
    )(x, ga, gm, *weights)


def run_backward(layer, hin, above, ga, gm, weights):
    dma = pltpu.SemaphoreType.DMA
    results = [((R, D), F32), ((R, D), BF16), ((R, D), BF16), ((8, D), F32)] + [(shape, BF16) for shape in SAVED]
    outs = pl.pallas_call(
        functools.partial(backward_kernel, layer),
        name=f"backward{layer}",
        out_shape=[jax.ShapeDtypeStruct(*result) for result in results],
        in_specs=[hbm()] * (8 + len(above)),
        out_specs=[vmem()] * 4 + [hbm()] * 9,
        scratch_shapes=[pltpu.VMEM(shape, BF16) for shape in SAVED]
        + WEIGHT_SCRATCH
        + [
            pltpu.VMEM((R, D), BF16),
            pltpu.VMEM((HS, NF), F32),
            pltpu.VMEM((HS, NF), F32),
            pltpu.VMEM((S, NQ), BF16),
            pltpu.VMEM((HEADS, S, S), F32),
            pltpu.VMEM((S, NF), BF16),
            pltpu.VMEM((S, NO), BF16),
        ]
        + SCATTER_SCRATCH
        + [pltpu.VMEM((8, D), F32)] * 3
        + [pltpu.VMEM((R, D), BF16)] * 2
        + [pltpu.VMEM((LAYERS, D), F32)] * 2
        + [pltpu.VMEM((R, D), dtype) for dtype in (BF16, F32, BF16, BF16)]
        + [dma((8,)), dma((5,)), dma((9,)), dma((4, 3, 2, 2)), dma((4, 3, 2, 2)), dma((3, 2, 4)), dma((3, 2, 4)), dma((2,)), dma((2,))],
        compiler_params=pltpu.CompilerParams(
            collective_id=1 + layer, has_side_effects=True, vmem_limit_bytes=VMEM_LIMIT
        ),
    )(hin, *above, ga, gm, *weights)
    return outs[:4], outs[4:]


def run_closing(above, ga):
    dma = pltpu.SemaphoreType.DMA
    return pl.pallas_call(
        closing_kernel,
        name="closing",
        out_shape=[jax.ShapeDtypeStruct((R, D), BF16)] + [jax.ShapeDtypeStruct((LAYERS, D), F32)] * 2,
        in_specs=[vmem()] * 6,
        out_specs=[vmem()] * 3,
        scratch_shapes=[pltpu.VMEM((8, D), F32), pltpu.VMEM((3, 8, D), F32), dma((3,)), dma((3,))],
        compiler_params=pltpu.CompilerParams(
            collective_id=1 + LAYERS, has_side_effects=True, vmem_limit_bytes=8_000_000
        ),
    )(*above, ga)


def run_wgrad(layer, saved, grads, y):
    dma = pltpu.SemaphoreType.DMA
    n_alias = len(grads)
    return pl.pallas_call(
        functools.partial(wgrad_kernel, layer, n_alias),
        name=f"wgrad{layer}",
        out_shape=[jax.ShapeDtypeStruct((LAYERS, *shape), BF16) for shape in GRADS]
        + [jax.ShapeDtypeStruct((R, D), BF16)] * len(y),
        in_specs=[hbm()] * (9 + n_alias + len(y)),
        out_specs=[hbm()] * (5 + len(y)),
        input_output_aliases={9 + i: i for i in range(n_alias)},
        scratch_shapes=[pltpu.VMEM(shape, BF16) for shape in SAVED[:2]]
        + [pltpu.VMEM(shape, BF16) for shape in ((3, S, D), (4, S, D), GRADS[0], (4, D, D), (R, D), (2, S, S))]
        + [dma((9,)), dma((5, 4)), dma((2,))],
        compiler_params=pltpu.CompilerParams(vmem_limit_bytes=VMEM_LIMIT if layer > 0 else 65_600_000),
        cost_estimate=pl.CostEstimate(flops=8_600_000_000, bytes_accessed=42_000_000, transcendentals=0),
    )(*saved, *grads, *y)


def solution(mesh):
    row_spec = P(("dp", "tp"), None)
    col_spec = P(None, None, "tp")
    mid_spec = P(None, "tp", None)
    in_specs = (row_spec, row_spec, P(None, None), P(None, None), col_spec, mid_spec, col_spec, col_spec, mid_spec)
    out_specs = (
        row_spec, row_spec, P("dp", None, "tp"), P("dp", "tp", None), P("dp", None, "tp"), P("dp", None, "tp"),
        P("dp", "tp", None), P("dp", None), P("dp", None),
    )

    def device_step(x, grad_y, gain_attn, gain_mlp, w_qkv, w_out, w_gate, w_up, w_down):
        weights = (w_qkv, w_out, w_gate, w_up, w_down)
        h1, h2, y = run_forward(x, gain_attn, gain_mlp, weights)
        kept, above = (x, h1, h2), (grad_y,)
        grads = ()
        for layer in reversed(range(LAYERS)):
            (own, chip_sum, d_mid, gains), saved = run_backward(
                layer, kept[layer], above, gain_attn, gain_mlp, weights
            )
            far = lax.ppermute(chip_sum, "tp", [(0, 2), (1, 3), (2, 0), (3, 1)])
            grads = run_wgrad(layer, saved, grads, () if grads else (y,))
            if len(grads) > len(GRADS):
                *grads, y = grads
            far, grads = lax.optimization_barrier((far, tuple(grads)))
            above = (kept[layer], own, far, d_mid, gains)
        grad_x, *gains = run_closing(above, gain_attn)
        return (y, grad_x, *grads, *gains)

    return jax.shard_map(device_step, mesh=mesh, in_specs=in_specs, out_specs=out_specs, check_vma=False)
```

```python
import functools

import jax
import jax.numpy as jnp
from jax import lax
from jax.experimental import pallas as pl
from jax.experimental.pallas import tpu as pltpu
from jax.sharding import PartitionSpec as P

HEAD = 128
EPS = 1e-5
MESH = pl.DeviceIdType.MESH
F32 = jnp.float32
BF16 = jnp.bfloat16
VMEM_LIMIT = 67_000_000

D = 2048
S = 256
R = 64
NQ = 1536
NO = 512
NF = 2048
HEADS = 4
LAYERS = 3

HR = R // 2
HS = S // 2


def dot(a, b):
    return jnp.dot(a, b, preferred_element_type=F32)


def dot_nt(a, b):
    return lax.dot_general(a, b, (((1,), (1,)), ((), ())), preferred_element_type=F32)


def dot_tn(a, b):
    return lax.dot_general(a, b, (((0,), (0,)), ((), ())), preferred_element_type=F32)


def ds(i, n):
    return pl.ds(i * n if isinstance(i, int) else pl.multiple_of(i * n, n), n)


def short(n, body):
    if n > 2:
        return loop(n, body)
    for i in range(n):
        body(i)


def loop(n, body):
    lax.fori_loop(0, n, lambda i, c: (body(i), c)[1], 0)


class Peers:
    def __init__(self):
        self.me = lax.axis_index("tp")
        core, chip = lax.rem(self.me, 2), self.me // 2
        self.sib = chip * 2 + (1 - core)
        self.cross = (1 - chip) * 2 + core
        self.diag = (1 - chip) * 2 + (1 - core)

    def here(self, *more):
        self.partners = 2 + len(more)
        for peer in (self.sib, self.cross, *more):
            pl.semaphore_signal(pltpu.get_barrier_semaphore(), inc=1, device_id={"tp": peer}, device_id_type=MESH)

    def ready(self):
        pl.semaphore_wait(pltpu.get_barrier_semaphore(), self.partners)


def remote(src, dst, send, recv, peer):
    return pltpu.make_async_remote_copy(
        src_ref=src, dst_ref=dst, send_sem=send, recv_sem=recv, device_id={"tp": peer}, device_id_type=MESH
    )


def owned(owner, half):
    return ds(half * 4 + owner, HR)


def true_position(row):
    return lax.rem(row, HS) // HR * R + row // HS * HR + lax.rem(row, HR)


class Gather:
    def __init__(self, p, buf, send, recv, which):
        self.p, self.buf, self.send, self.recv, self.which = p, buf, send, recv, which

    def _copy(self, kind, half, chunk, owner, peer):
        part = self.buf.at[owned(owner, half), ds(chunk, D // 2)]
        sems = (self.which, kind, half, chunk)
        return remote(part, part, self.send.at[sems], self.recv.at[sems], peer)

    def start(self, half):
        for chunk in range(2):
            self._copy(0, half, chunk, self.p.me, self.p.cross).start()
        for chunk in range(2):
            self._copy(1, half, chunk, self.p.me, self.p.sib).start()

    def relay(self, half, chunk):
        self._copy(0, half, chunk, self.p.cross, self.p.cross).wait_recv()
        self._copy(2, half, chunk, self.p.cross, self.p.sib).start()

    def arrived(self, half, chunk):
        self._copy(1, half, chunk, self.p.sib, self.p.sib).wait_recv()
        self._copy(2, half, chunk, self.p.diag, self.p.sib).wait_recv()

    def each(self, bodies, middle=None, after=None):
        self.relay(0, 0)

        def one(half):
            @pl.when(half == 0)
            def _():
                self.relay(0, 1)

            self.arrived(half, 0)
            bodies[0](half)

            @pl.when(half == 0)
            def _():
                self.relay(1, 0)

            if middle is not None:
                middle(half)
            self.arrived(half, 1)
            bodies[1](half)

            @pl.when(half == 0)
            def _():
                self.relay(1, 1)

            if after is not None:
                after(half)

        loop(2, one)

    def all(self):
        for half in range(2):
            for chunk in range(2):
                self.relay(half, chunk)
        for half in range(2):
            for chunk in range(2):
                self.arrived(half, chunk)

    def finish(self):
        def one(half):
            for chunk in range(2):
                self._copy(0, half, chunk, self.p.me, self.p.cross).wait_send()
                self._copy(1, half, chunk, self.p.me, self.p.sib).wait_send()
                self._copy(2, half, chunk, self.p.cross, self.p.sib).wait_send()

        loop(2, one)


class Scatter:
    def __init__(self, p, part, near, out, far, send, recv, chunks):
        self.p, self.part, self.near, self.out, self.far, self.send, self.recv = p, part, near, out, far, send, recv
        self.chunks, self.width = chunks, D // chunks

    def _near(self, kind, half, chunk):
        owner = self.p.diag if kind == 0 else self.p.sib
        cols = ds(chunk, self.width)
        return remote(
            self.part.at[owned(owner, half), cols],
            self.near.at[kind, ds(half, HR), cols],
            self.send.at[kind, half, chunk],
            self.recv.at[kind, half, chunk],
            self.p.sib,
        )

    def _far(self, half, chunk):
        cols = ds(chunk, self.width)
        return remote(
            self.out.at[ds(half, HR), cols],
            self.far.at[ds(half, HR), cols],
            self.send.at[2, half, chunk],
            self.recv.at[2, half, chunk],
            self.p.cross,
        )

    def _mid(self, half, chunk, send=True):
        self._near(0, half, chunk).wait_recv()
        cols = ds(chunk, self.width)
        total = self.part[owned(self.p.cross, half), cols] + self.near[0, ds(half, HR), cols]
        self.out[ds(half, HR), cols] = total.astype(BF16)
        if send:
            self._far(half, chunk).start()

    def mids(self, half):
        short(self.chunks, lambda chunk: self._mid(half, chunk))

    def run(self, half, compute, unrolled=False):
        def step(chunk):
            cols = ds(chunk, self.width)
            self.part[ds(half, HS), cols] = compute(ds(half, HS), cols)
            self._near(0, half, chunk).start()
            self._near(1, half, chunk).start()

        if unrolled:
            for chunk in range(self.chunks):
                step(chunk)
        else:
            loop(self.chunks, step)

    def run_full(self, compute, send=True):
        def mids(chunk):
            self._mid(0, chunk, send)
            self._mid(1, chunk, send)

        def step(chunk):
            cols = ds(chunk, self.width)
            self.part[:, cols] = compute(cols)
            for kind in range(2):
                for half in range(2):
                    self._near(kind, half, chunk).start()

            @pl.when(chunk > 0)
            def _():
                mids(chunk - 1)

        loop(self.chunks, step)
        mids(self.chunks - 1)

    def result(self, half):
        def waits(chunk):
            self._near(1, half, chunk).wait_recv()
            self._far(half, chunk).wait_recv()

        def sent(chunk):
            self._near(0, half, chunk).wait_send()
            self._near(1, half, chunk).wait_send()
            self._far(half, chunk).wait_send()

        short(self.chunks, waits)
        rows = ds(half, HR)
        total = self.part[owned(self.p.me, half), :] + self.near[1, rows, :] + self.far[rows, :].astype(F32)
        short(self.chunks, sent)
        return total.astype(BF16)


    def own_sum(self, own):
        for half in range(2):
            for chunk in range(self.chunks):
                self._near(1, half, chunk).wait_recv()
            own[ds(half, HR), :] = self.part[owned(self.p.me, half), :] + self.near[1, ds(half, HR), :]
        for half in range(2):
            for chunk in range(self.chunks):
                for kind in range(2):
                    self._near(kind, half, chunk).wait_send()


def norm(h, gain):
    hf = h.astype(F32)
    inv = lax.rsqrt(jnp.mean(hf * hf, axis=-1, keepdims=True) + EPS)
    return (hf * inv * gain).astype(BF16)


def norm_back(h, gain, dy):
    hf, dyf = h.astype(F32), dy.astype(F32)
    inv = lax.rsqrt(jnp.mean(hf * hf, axis=-1, keepdims=True) + EPS)
    dgain = jnp.sum(dyf * (hf * inv), axis=0, keepdims=True)
    dn = dyf * gain
    slope = jnp.sum(dn * hf, axis=-1, keepdims=True) * (inv * inv * inv) / D
    return (dn * inv - hf * slope).astype(BF16), dgain


def softmax_scores(q, k):
    scores = dot_nt(q, k) * HEAD**-0.5
    rows = true_position(lax.broadcasted_iota(jnp.int32, (S, 1), 0))
    cols = true_position(lax.broadcasted_iota(jnp.int32, (1, S), 1))
    scores = jnp.where(rows >= cols, scores, -1e30)
    e = jnp.exp(scores - jnp.max(scores, axis=-1, keepdims=True))
    return e / jnp.sum(e, axis=-1, keepdims=True)


def head_cols(head, which):
    return ds(head * 3 + which, HEAD)


def per_head(one, together):
    def step(j):
        for i in range(together):
            one(j * together + i)

    loop(HEADS // together, step)


def attention(qkv, o, together, probs=None):
    def one(head):
        prob = softmax_scores(qkv[:, head_cols(head, 0)], qkv[:, head_cols(head, 1)])
        if probs is not None:
            probs[head] = prob
        o[:, ds(head, HEAD)] = dot(prob.astype(BF16), qkv[:, head_cols(head, 2)]).astype(BF16)

    per_head(one, together)


def half_qkv(u, wq, acc, qkv):
    def body(chunk, half):
        rows, deep = ds(half, HS), ds(chunk, D // 2)
        for j in range(NQ // 512):
            cols = ds(j, 512)
            part = dot(u[rows, deep], wq[deep, cols])
            if chunk == 0:
                acc[:, cols] = part
            else:
                qkv[rows, cols] = (acc[:, cols] + part).astype(BF16)

    return [functools.partial(body, chunk) for chunk in range(2)]


def half_mlp(n, wg, wu, acc1, acc3, last, tile):
    def body(chunk, half):
        rows, deep = ds(half, HS), ds(chunk, D // 2)

        def one(j):
            for k in range(tile // 512):
                cols = ds(j * (tile // 512) + k, 512)
                z1 = dot(n[rows, deep], wg[deep, cols])
                z3 = dot(n[rows, deep], wu[deep, cols])
                if chunk == 0:
                    acc1[:, cols] = z1
                    acc3[:, cols] = z3
                else:
                    z1 = (acc1[:, cols] + z1).astype(BF16).astype(F32)
                    z3 = (acc3[:, cols] + z3).astype(BF16).astype(F32)
                    last(rows, cols, z1, z3)

        if tile == NF:
            one(0)
        else:
            loop(NF // tile, one)

    return [functools.partial(body, chunk) for chunk in range(2)]


def forward_kernel(x, ga, gm, wq_h, wo_h, wg_h, wu_h, wd_h, h1, h2, y,
                   wq, wo, wg, wu, wd, h, u, n, acc1, acc3, qkv, o, m, part, near, out, far,
                   wsem, gsend, grecv, ssend, srecv):
    p = Peers()
    pairs = ((wq_h, wq), (wo_h, wo), (wg_h, wg), (wu_h, wu), (wd_h, wd))

    def load(i, layer):
        return pltpu.make_async_copy(pairs[i][0].at[layer], pairs[i][1], wsem.at[i])

    p.here()
    for i in range(5):
        load(i, 0).start()
    h[...] = x[...]
    gu = Gather(p, u, gsend, grecv, 0)
    gn = Gather(p, n, gsend, grecv, 1)
    scatter = Scatter(p, part, near, out, far, ssend, srecv, 2)

    def enter(half, layer):
        u[owned(p.me, half), :] = norm(h[ds(half, HR), :], ga[pl.ds(layer, 1), :])

    def add(half):
        rows = ds(half, HR)
        total = h[rows, :] + scatter.result(half)
        h[rows, :] = total
        return total

    loop(2, lambda half: enter(half, 0))
    p.ready()
    loop(2, gu.start)

    def layer_step(layer):
        more = layer < LAYERS - 1

        def refill(i):
            @pl.when(more)
            def _():
                load(i, layer + 1).start()

        load(0, layer).wait()
        gu.each(half_qkv(u, wq, acc1, qkv))
        refill(0)
        attention(qkv, o, 4)
        load(1, layer).wait()

        def project(half):
            scatter.run(half, lambda rows, cols: dot(o[rows, :], wo[:, cols]), True)
            scatter.mids(half)

        loop(2, project)
        refill(1)
        gu.finish()

        def between(half):
            n[owned(p.me, half), :] = norm(add(half), gm[pl.ds(layer, 1), :])
            gn.start(half)

        loop(2, between)

        def last(rows, cols, z1, z3):
            m[rows, cols] = (z1 * jax.nn.sigmoid(z1) * z3).astype(BF16)

        for i in (2, 3, 4):
            load(i, layer).wait()

        def send_first(half):
            @pl.when(half == 1)
            def _():
                scatter.mids(0)

        gn.each(
            half_mlp(n, wg, wu, acc1, acc3, last, NF),
            send_first,
            lambda half: scatter.run(half, lambda rows, cols: dot(m[rows, :], wd[:, cols]), True),
        )
        scatter.mids(1)
        refill(2)
        refill(3)
        refill(4)
        gn.finish()

        def leave(half):
            total = add(half)

            for i, kept in enumerate((h1, h2, y)):
                @pl.when(layer == i)
                def _():
                    kept[ds(half, HR), :] = total

            @pl.when(more)
            def _():
                enter(half, layer + 1)
                gu.start(half)

        loop(2, leave)

    loop(LAYERS, layer_step)


def finish_layer(h, gain, own, far, d_mid, rows):
    d_in = (own[rows, :] + far[rows, :].astype(F32)).astype(BF16)
    d_norm, dgain = norm_back(h[rows, :], gain, d_in)
    return d_mid[rows, :] + d_norm, dgain


def backward_kernel(layer, hin, *refs):
    first_call, last_call = layer == LAYERS - 1, layer == 0
    refs = list(refs)
    take = lambda k: [refs.pop(0) for _ in range(k)]
    if first_call:
        (dy,) = take(1)
    else:
        h_above, above_own, above_far, above_mid, gin = take(5)
    ga, gm, wq_h, wo_h, wg_h, wu_h, wd_h = take(7)
    own_out, far_out, mid_out, gout = take(4)
    saved_h = take(9)
    u, dqkv, o, da, n, dg, du, m, dd = saved = take(9)
    wq, wo, wg, wu, wd = take(5)
    hm, acc1, acc3, qkv, probs, dgated, dh, part, near, out, far, gbuf, gmid, gfar, dy_buf = take(15)
    wsem, osem, gsend, grecv, ssend, srecv, rsend, rrecv = take(8)

    p = Peers()
    pairs = ((wq_h, wq), (wo_h, wo), (wg_h, wg), (wu_h, wu), (wd_h, wd))
    loads = [pltpu.make_async_copy(src.at[layer], dst, wsem.at[i]) for i, (src, dst) in enumerate(pairs)]
    saves = [pltpu.make_async_copy(src, dst, osem.at[i]) for i, (src, dst) in enumerate(zip(saved, saved_h))]
    p.here()
    for i in (0, 1, 4, 2, 3):
        loads[i].start()
    h = hin
    gain_a, gain_m = ga[pl.ds(layer, 1), :], gm[pl.ds(layer, 1), :]
    gu, gd, gn, gda = (Gather(p, buf, gsend, grecv, i) for i, buf in enumerate((u, dd, n, da)))
    two = Scatter(p, part, near, out, far, ssend, srecv, 2)
    four = Scatter(p, part, near, out, far, ssend, srecv, 4)

    def enter(half):
        u[owned(p.me, half), :] = norm(h[ds(half, HR), :], gain_a)

    if first_call:
        gbuf[...] = jnp.zeros_like(gbuf)
    else:
        dy = dy_buf
        gbuf[...] = gin[...]

    def enter_d(half):
        rows = ds(half, HR)
        if not first_call:
            above = layer + 1
            total, dgain = finish_layer(h_above, ga[above : above + 1, :], above_own, above_far, above_mid, rows)
            dy[rows, :] = total
            gbuf[above : above + 1, :] = gbuf[above : above + 1, :] + dgain
        dd[owned(p.me, half), :] = dy[rows, :]
        gd.start(half)

    loop(2, enter)
    p.ready()
    loop(2, gu.start)
    loop(2, enter_d)

    loads[0].wait()
    gu.each(half_qkv(u, wq, acc1, qkv))
    saves[0].start()
    attention(qkv, o, 2, probs)
    saves[2].start()
    loads[1].wait()

    def project(half):
        two.run(half, lambda rows, cols: dot(o[rows, :], wo[:, cols]))
        two.mids(half)

    loop(2, project)

    gd.all()
    saves[8].start()
    loads[4].wait()

    def gated(j):
        dgated[:, ds(j, 512)] = dot_nt(dd[...], wd[ds(j, 512), :]).astype(BF16)

    loop(NF // 512, gated)

    def between(half):
        rows = ds(half, HR)
        h_mid = h[rows, :] + two.result(half)
        hm[rows, :] = h_mid
        n[owned(p.me, half), :] = norm(h_mid, gain_m)
        gn.start(half)

    loop(2, between)
    loads[2].wait()
    loads[3].wait()

    def last(rows, cols, z1, z3):
        sig = jax.nn.sigmoid(z1)
        silu = z1 * sig
        dm = dgated[rows, cols].astype(F32)
        m[rows, cols] = (silu * z3).astype(BF16)
        du[rows, cols] = (dm * silu).astype(BF16)
        dg[rows, cols] = (dm * z3 * (sig + silu * (1.0 - sig))).astype(BF16)

    gn.each(half_mlp(n, wg, wu, acc1, acc3, last, 1024))
    for i in (4, 5, 6, 7):
        saves[i].start()

    four.run_full(lambda cols: dot_nt(dg[...], wg[cols, :]) + dot_nt(du[...], wu[cols, :]))

    def mid_back(half):
        rows = ds(half, HR)
        d_norm, dgain = norm_back(hm[rows, :], gain_m, four.result(half))
        da[owned(p.me, half), :] = dy[rows, :] + d_norm
        gda.start(half)
        row = pl.ds(LAYERS + layer, 1)
        gbuf[row, :] = gbuf[row, :] + dgain

    loop(2, mid_back)
    if last_call:
        near_g = remote(gbuf, gmid, rsend.at[0], rrecv.at[0], p.sib)
        near_g.start()

    def heads(chunk, half):
        rows, deep = ds(half, HS), ds(chunk, D // 2)
        part_h = dot_nt(da[rows, deep], wo[:, deep])
        if chunk == 0:
            acc1[:, :NO] = part_h
        else:
            dh[rows, :] = (acc1[:, :NO] + part_h).astype(BF16)

    gda.each([functools.partial(heads, chunk) for chunk in range(2)])
    saves[3].start()

    def back(head):
        prob = probs[head]
        d_o = dh[:, ds(head, HEAD)]
        q, k, v = (qkv[:, head_cols(head, i)] for i in range(3))
        d_prob = dot_nt(d_o, v)
        d_scores = (prob * (d_prob - jnp.sum(d_prob * prob, axis=-1, keepdims=True)) * HEAD**-0.5).astype(BF16)
        dqkv[:, head_cols(head, 0)] = dot(d_scores, k).astype(BF16)
        dqkv[:, head_cols(head, 1)] = dot_tn(d_scores, q).astype(BF16)
        dqkv[:, head_cols(head, 2)] = dot_tn(prob.astype(BF16), d_o).astype(BF16)

    per_head(back, 4)
    saves[1].start()
    if last_call:
        near_g.wait()
        gbuf[...] = gbuf[...] + gmid[...]
        far_g = remote(gbuf, gfar, rsend.at[1], rrecv.at[1], p.cross)
        far_g.start()
    last_sum = Scatter(p, part, near, far_out, None, ssend, srecv, 4)
    last_sum.run_full(lambda cols: dot_nt(dqkv[...], wq[cols, :]), send=False)
    for half in range(2):
        mid_out[ds(half, HR), :] = da[owned(p.me, half), :]
    last_sum.own_sum(own_out)
    if last_call:
        far_g.wait()
        gout[...] = gbuf[...] + gfar[...]
    else:
        gout[...] = gbuf[...]
    for g in (gu, gd, gn, gda):
        g.finish()
    for save in saves:
        save.wait()


def closing_kernel(x, own, far, d_mid, gin, ga, dx, ga_out, gm_out, mine, others, send, recv):
    p = Peers()
    p.here(p.diag)
    mine[...] = jnp.zeros_like(mine)

    def finish(half):
        rows = ds(half, HR)
        total, dgain = finish_layer(x, ga[0:1, :], own, far, d_mid, rows)
        dx[rows, :] = total
        mine[0:1, :] = mine[0:1, :] + dgain

    loop(2, finish)
    p.ready()
    copies = [
        remote(mine, others.at[i], send.at[i], recv.at[i], peer) for i, peer in enumerate((p.cross, p.diag, p.sib))
    ]
    for copy in copies:
        copy.start()
    ga_out[1:LAYERS, :] = gin[1:LAYERS, :]
    gm_out[...] = gin[LAYERS : 2 * LAYERS, :]
    for copy in copies:
        copy.wait()
    ga_out[0:1, :] = ((mine[...] + others[2]) + (others[0] + others[1]))[0:1, :]


def wgrad_kernel(layer, n_alias, u_h, dqkv_h, o_h, da_h, n_h, dg_h, du_h, m_h, dd_h, *refs):
    refs = list(refs)
    take = lambda k: [refs.pop(0) for _ in range(k)]
    take(n_alias)
    passed = n_alias == 0
    y_in = take(1) if passed else ()
    gqkv_h, gout_h, ggate_h, gup_h, gdown_h = take(5)
    y_out = take(1) if passed else ()
    u, dqkv, lhs, rhs, gqkv, gwide, y_buf, turned = take(8)
    isem, osem, ysem = take(3)
    y_load = [pltpu.make_async_copy(y, y_buf, ysem.at[0]) for y in y_in]
    y_save = [pltpu.make_async_copy(y_buf, y, ysem.at[1]) for y in y_out]
    sources = (n_h, dg_h, du_h, m_h, dd_h, o_h, da_h, u_h, dqkv_h)
    targets = (lhs.at[0], rhs.at[0], rhs.at[1], lhs.at[1], rhs.at[2], lhs.at[2, :, :NO], rhs.at[3], u, dqkv)
    loads = [pltpu.make_async_copy(src, dst, isem.at[i]) for i, (src, dst) in enumerate(zip(sources, targets))]
    for load in loads + y_load:
        load.start()

    def pair(a, b, stage, i, following, j):
        for k in range(2):
            for c in range(b.shape[1] // 512):
                stage[ds(2 * i + k, S), ds(c, 512)] = dot(turned[k], b[:, ds(c, 512)]).astype(BF16)
            if k == 0:
                turned[1] = a[:, ds(2 * i + 1, S)].T
            else:
                turned[0] = following[:, ds(2 * j, S)].T

    def copy(stage, out, i, sem):
        return pltpu.make_async_copy(stage.at[ds(i, 2 * S), :], out.at[layer, ds(i, 2 * S), :], sem)

    wide_outs = (ggate_h, gup_h, gdown_h, gout_h)
    loads[0].wait()
    loads[1].wait()

    turned[0] = lhs[0, :, :S].T

    def wide(step):
        which, i = step // 4, lax.rem(step, 4)
        after = jnp.minimum(step + 1, 12)
        for at, needed in ((3, loads[2:3]), (7, loads[3:5]), (11, loads[5:7])):
            @pl.when(step == at)
            def _():
                for load in needed:
                    load.wait()

        stage = gwide.at[which]
        left = lhs.at[jnp.maximum(which - 1, 0)]
        pair(left, rhs.at[which], stage, i, lhs.at[jnp.maximum(after // 4 - 1, 0)], lax.rem(after, 4))
        for k, out in enumerate(wide_outs):
            @pl.when(which == k)
            def _():
                copy(stage, out, i if k < 3 else 0, osem.at[k, i]).start()

    loop(13, wide)
    for load in loads[7:] + y_load:
        load.wait()
    for save in y_save:
        save.start()

    turned[0] = u[:, :S].T

    def qkv(i):
        pair(u, dqkv, gqkv, i, u, jnp.minimum(i + 1, 3))
        copy(gqkv, gqkv_h, i, osem.at[4, i]).start()

    loop(4, qkv)
    for i in range(4):
        for k, out in enumerate(wide_outs[:3]):
            copy(gwide.at[k], out, i, osem.at[k, i]).wait()
        copy(gqkv, gqkv_h, i, osem.at[4, i]).wait()
    copy(gwide.at[3], gout_h, 0, osem.at[3, 0]).wait()
    for save in y_save:
        save.wait()


def vmem():
    return pl.BlockSpec(memory_space=pltpu.VMEM)


def hbm():
    return pl.BlockSpec(memory_space=pltpu.HBM)


WEIGHT_SCRATCH = [
    pltpu.VMEM((D, NQ), BF16),
    pltpu.VMEM((NO, D), BF16),
    pltpu.VMEM((D, NF), BF16),
    pltpu.VMEM((D, NF), BF16),
    pltpu.VMEM((NF, D), BF16),
]
SCATTER_SCRATCH = [
    pltpu.VMEM((S, D), F32),
    pltpu.VMEM((2, R, D), F32),
    pltpu.VMEM((R, D), BF16),
    pltpu.VMEM((R, D), BF16),
]
SAVED = [(S, D), (S, NQ), (S, NO), (S, D), (S, D), (S, NF), (S, NF), (S, NF), (S, D)]
GRADS = [(D, NQ), (NO, D), (D, NF), (D, NF), (NF, D)]


def run_forward(x, ga, gm, weights):
    dma = pltpu.SemaphoreType.DMA
    return pl.pallas_call(
        forward_kernel,
        name="forward",
        out_shape=[jax.ShapeDtypeStruct((R, D), BF16)] * 3,
        in_specs=[vmem()] * 3 + [hbm()] * 5,
        out_specs=[vmem()] * 3,
        scratch_shapes=WEIGHT_SCRATCH
        + [
            pltpu.VMEM((R, D), BF16),
            pltpu.VMEM((S, D), BF16),
            pltpu.VMEM((S, D), BF16),
            pltpu.VMEM((HS, NF), F32),
            pltpu.VMEM((HS, NF), F32),
            pltpu.VMEM((S, NQ), BF16),
            pltpu.VMEM((S, NO), BF16),
            pltpu.VMEM((S, NF), BF16),
        ]
        + SCATTER_SCRATCH
        + [dma((5,)), dma((2, 3, 2, 2)), dma((2, 3, 2, 2)), dma((3, 2, 2)), dma((3, 2, 2))],
        compiler_params=pltpu.CompilerParams(collective_id=0, has_side_effects=True, vmem_limit_bytes=VMEM_LIMIT),
    )(x, ga, gm, *weights)


def run_backward(layer, hin, above, ga, gm, weights):
    dma = pltpu.SemaphoreType.DMA
    results = [((R, D), F32), ((R, D), BF16), ((R, D), BF16), ((8, D), F32)] + [(shape, BF16) for shape in SAVED]
    outs = pl.pallas_call(
        functools.partial(backward_kernel, layer),
        name=f"backward{layer}",
        out_shape=[jax.ShapeDtypeStruct(*result) for result in results],
        in_specs=[vmem()] * (3 + len(above)) + [hbm()] * 5,
        out_specs=[vmem()] * 4 + [hbm()] * 9,
        scratch_shapes=[pltpu.VMEM(shape, BF16) for shape in SAVED]
        + WEIGHT_SCRATCH
        + [
            pltpu.VMEM((R, D), BF16),
            pltpu.VMEM((HS, NF), F32),
            pltpu.VMEM((HS, NF), F32),
            pltpu.VMEM((S, NQ), BF16),
            pltpu.VMEM((HEADS, S, S), F32),
            pltpu.VMEM((S, NF), BF16),
            pltpu.VMEM((S, NO), BF16),
        ]
        + SCATTER_SCRATCH
        + [pltpu.VMEM((8, D), F32)] * 3
        + [pltpu.VMEM((R, D), BF16)]
        + [dma((5,)), dma((9,)), dma((4, 3, 2, 2)), dma((4, 3, 2, 2)), dma((3, 2, 4)), dma((3, 2, 4)), dma((2,)), dma((2,))],
        compiler_params=pltpu.CompilerParams(
            collective_id=1 + layer, has_side_effects=True, vmem_limit_bytes=VMEM_LIMIT
        ),
    )(hin, *above, ga, gm, *weights)
    return outs[:4], outs[4:]


def run_closing(above, ga):
    dma = pltpu.SemaphoreType.DMA
    return pl.pallas_call(
        closing_kernel,
        name="closing",
        out_shape=[jax.ShapeDtypeStruct((R, D), BF16)] + [jax.ShapeDtypeStruct((LAYERS, D), F32)] * 2,
        in_specs=[vmem()] * 6,
        out_specs=[vmem()] * 3,
        scratch_shapes=[pltpu.VMEM((8, D), F32), pltpu.VMEM((3, 8, D), F32), dma((3,)), dma((3,))],
        compiler_params=pltpu.CompilerParams(
            collective_id=1 + LAYERS, has_side_effects=True, vmem_limit_bytes=8_000_000
        ),
    )(*above, ga)


def run_wgrad(layer, saved, grads, y):
    dma = pltpu.SemaphoreType.DMA
    n_alias = len(grads)
    return pl.pallas_call(
        functools.partial(wgrad_kernel, layer, n_alias),
        name=f"wgrad{layer}",
        out_shape=[jax.ShapeDtypeStruct((LAYERS, *shape), BF16) for shape in GRADS]
        + [jax.ShapeDtypeStruct((R, D), BF16)] * len(y),
        in_specs=[hbm()] * (9 + n_alias + len(y)),
        out_specs=[hbm()] * (5 + len(y)),
        input_output_aliases={9 + i: i for i in range(n_alias)},
        scratch_shapes=[pltpu.VMEM(shape, BF16) for shape in SAVED[:2]]
        + [pltpu.VMEM(shape, BF16) for shape in ((3, S, D), (4, S, D), GRADS[0], (4, D, D), (R, D), (2, S, S))]
        + [dma((9,)), dma((5, 4)), dma((2,))],
        compiler_params=pltpu.CompilerParams(vmem_limit_bytes=VMEM_LIMIT if layer > 0 else 65_600_000),
        cost_estimate=pl.CostEstimate(flops=8_600_000_000, bytes_accessed=42_000_000, transcendentals=0),
    )(*saved, *grads, *y)


def solution(mesh):
    row_spec = P(("dp", "tp"), None)
    col_spec = P(None, None, "tp")
    mid_spec = P(None, "tp", None)
    in_specs = (row_spec, row_spec, P(None, None), P(None, None), col_spec, mid_spec, col_spec, col_spec, mid_spec)
    out_specs = (
        row_spec, row_spec, P("dp", None, "tp"), P("dp", "tp", None), P("dp", None, "tp"), P("dp", None, "tp"),
        P("dp", "tp", None), P("dp", None), P("dp", None),
    )

    def device_step(x, grad_y, gain_attn, gain_mlp, w_qkv, w_out, w_gate, w_up, w_down):
        weights = (w_qkv, w_out, w_gate, w_up, w_down)
        h1, h2, y = run_forward(x, gain_attn, gain_mlp, weights)
        kept, above = (x, h1, h2), (grad_y,)
        grads = ()
        for layer in reversed(range(LAYERS)):
            (own, chip_sum, d_mid, gains), saved = run_backward(
                layer, kept[layer], above, gain_attn, gain_mlp, weights
            )
            far = lax.ppermute(chip_sum, "tp", [(0, 2), (1, 3), (2, 0), (3, 1)])
            grads = run_wgrad(layer, saved, grads, () if grads else (y,))
            if len(grads) > len(GRADS):
                *grads, y = grads
            far, grads = lax.optimization_barrier((far, tuple(grads)))
            above = (kept[layer], own, far, d_mid, gains)
        grad_x, *gains = run_closing(above, gain_attn)
        return (y, grad_x, *grads, *gains)

    return jax.shard_map(device_step, mesh=mesh, in_specs=in_specs, out_specs=out_specs, check_vma=False)
```
